16 devices in a mesh: data: 16 (over z, y, x, core).
Axes of the slice: x: 2, y: 2, z: 2, core: 2. Of those that a mesh axis runs over, the one named last changes fastest.
Arguments:
- act_in: bfloat16 [65536, 896], P('data')
- grad_out: bfloat16 [65536, 896], P('data')
- w_up1: bfloat16 [896, 4864], replicated
- w_down1: bfloat16 [4864, 896], replicated
- w_up2: bfloat16 [896, 4864], replicated
- w_down2: bfloat16 [4864, 896], replicated
- master_up1: float32 [896, 4864], P('data')
- master_down1: float32 [4864, 896], P('data')
- master_up2: float32 [896, 4864], P('data')
- master_down2: float32 [4864, 896], P('data')
- mom_up1: float32 [896, 4864], P('data')
- mom_down1: float32 [4864, 896], P('data')
- mom_up2: float32 [896, 4864], P('data')
- mom_down2: float32 [4864, 896], P('data')
- vel_up1: float32 [896, 4864], P('data')
- vel_down1: float32 [4864, 896], P('data')
- vel_up2: float32 [896, 4864], P('data')
- vel_down2: float32 [4864, 896], P('data')
- learn_rate: float32 [], replicated
- clip_norm: float32 [], replicated
Outputs:
- output 1: bfloat16 [896, 4864], replicated
- output 2: bfloat16 [4864, 896], replicated
- output 3: bfloat16 [896, 4864], replicated
- output 4: bfloat16 [4864, 896], replicated
- output 5: float32 [896, 4864], P('data')
- output 6: float32 [4864, 896], P('data')
- output 7: float32 [896, 4864], P('data')
- output 8: float32 [4864, 896], P('data')
- output 9: float32 [896, 4864], P('data')
- output 10: float32 [4864, 896], P('data')
- output 11: float32 [896, 4864], P('data')
- output 12: float32 [4864, 896], P('data')
- output 13: float32 [896, 4864], P('data')
- output 14: float32 [4864, 896], P('data')
- output 15: float32 [896, 4864], P('data')
- output 16: float32 [4864, 896], P('data')
- output 17: float32 [], replicated
All inputs are finite; a program needn't handle non-finite values.
Results may differ from the reference program's by a relative error of at most 0.010218.
Values are sent between devices in bfloat16 or wider.
A program may use at most 1 GiB of HBM per device.

```python
import math
import jax
import jax.numpy as jnp
from jax import lax

D = 896
FF = 4864
ROWS = 65536
GROUP = 16
STEP = 20
SAMPLE = 256

BETA_ONE = 0.9
BETA_TWO = 0.95
EPSILON = 1e-8
NORM_EPS = 1e-6
CORR_ONE = 1.0 - BETA_ONE ** STEP
CORR_TWO = 1.0 - BETA_TWO ** STEP
ROOT_HALF = math.sqrt(0.5)
INV_ROOT_TAU = 1.0 / math.sqrt(2.0 * math.pi)
LAYER_GAINS = (1.0, 1.5, 1.0, 2.0)
LAYER_NAMES = ("up1", "down1", "up2", "down2")


def gelu_pair(pre):
    normal_cdf = 0.5 * (1.0 + lax.erf(pre * ROOT_HALF))
    density = jnp.exp(-0.5 * pre * pre) * INV_ROOT_TAU
    return pre * normal_cdf, normal_cdf + pre * density


def fwd_bwd(rows_in, rows_grad, w_up1, w_down1, w_up2, w_down2):
    pre_up1 = jnp.dot(rows_in, w_up1, preferred_element_type=jnp.float32)
    gel_up1, der_up1 = gelu_pair(pre_up1)
    act_up1 = gel_up1.astype(jnp.bfloat16)
    mid_act = jnp.dot(act_up1, w_down1, preferred_element_type=jnp.float32).astype(jnp.bfloat16)
    pre_up2 = jnp.dot(mid_act, w_up2, preferred_element_type=jnp.float32)
    gel_up2, der_up2 = gelu_pair(pre_up2)
    act_up2 = gel_up2.astype(jnp.bfloat16)
    grad_act2 = jnp.dot(rows_grad, w_down2.T, preferred_element_type=jnp.float32).astype(jnp.bfloat16)
    grad_pre2 = (grad_act2.astype(jnp.float32) * der_up2).astype(jnp.bfloat16)
    grad_mid = jnp.dot(grad_pre2, w_up2.T, preferred_element_type=jnp.float32).astype(jnp.bfloat16)
    grad_act1 = jnp.dot(grad_mid, w_down1.T, preferred_element_type=jnp.float32).astype(jnp.bfloat16)
    grad_pre1 = (grad_act1.astype(jnp.float32) * der_up1).astype(jnp.bfloat16)
    return ((act_up2, rows_grad), (mid_act, grad_pre2), (act_up1, grad_mid), (rows_in, grad_pre1))


def adam_step(grad_rows, master_old, mom_old, vel_old, clip_scale, learn_rate):
    scaled = clip_scale * grad_rows
    mom_new = BETA_ONE * mom_old + (1.0 - BETA_ONE) * scaled
    vel_new = BETA_TWO * vel_old + (1.0 - BETA_TWO) * scaled * scaled
    master_new = master_old - learn_rate * (mom_new / CORR_ONE) / (jnp.sqrt(vel_new / CORR_TWO) + EPSILON)
    return master_new.astype(jnp.bfloat16), master_new, mom_new, vel_new


def norm_estimate(act_in, grad_out, weights):
    stride = ROWS // SAMPLE
    grad_pairs = fwd_bwd(act_in[::stride], grad_out[::stride], weights[0], weights[1], weights[2], weights[3])
    row_total = 0.0
    for layer_in, layer_delta in grad_pairs:
        in_sq = jnp.sum(jnp.square(layer_in.astype(jnp.float32)), axis=1)
        delta_sq = jnp.sum(jnp.square(layer_delta.astype(jnp.float32)), axis=1)
        row_total = row_total + jnp.sum(in_sq * delta_sq)
    return jnp.sqrt(row_total * stride) / GROUP


def setup_inputs(seed: int = 0) -> dict:
    key_list = jax.random.split(jax.random.key(seed), 20)
    act_in = jax.random.normal(key_list[0], (ROWS, D), jnp.float32).astype(jnp.bfloat16)
    grad_scale = 2.0 * GROUP / math.sqrt(ROWS * D * FF)
    grad_out = (grad_scale * jax.random.normal(key_list[1], (ROWS, D), jnp.float32)).astype(jnp.bfloat16)
    shapes = ((D, FF), (FF, D), (D, FF), (FF, D))
    weights = []
    masters = []
    for layer_idx in range(4):
        init_scale = LAYER_GAINS[layer_idx] / math.sqrt(shapes[layer_idx][0])
        weight = init_scale * jax.random.normal(key_list[2 + layer_idx], shapes[layer_idx], jnp.float32)
        weights.append(weight.astype(jnp.bfloat16))
        masters.append(weight + 0.01 * init_scale * jax.random.normal(key_list[6 + layer_idx], shapes[layer_idx], jnp.float32))
    clip_norm = norm_estimate(act_in, grad_out, weights) * jax.random.uniform(key_list[10], (), jnp.float32, 0.3, 0.6)
    unit_size = clip_norm / math.sqrt(4 * D * FF)
    inputs = {"act_in": act_in, "grad_out": grad_out}
    for layer_idx in range(4):
        inputs["w_" + LAYER_NAMES[layer_idx]] = weights[layer_idx]
    for layer_idx in range(4):
        inputs["master_" + LAYER_NAMES[layer_idx]] = masters[layer_idx]
    for layer_idx in range(4):
        inputs["mom_" + LAYER_NAMES[layer_idx]] = 0.1 * unit_size * jax.random.normal(key_list[11 + layer_idx], shapes[layer_idx], jnp.float32)
    for layer_idx in range(4):
        inputs["vel_" + LAYER_NAMES[layer_idx]] = 0.05 * unit_size * unit_size * jax.random.uniform(key_list[15 + layer_idx], shapes[layer_idx], jnp.float32, 0.5, 1.5)
    inputs["learn_rate"] = 0.5 / math.sqrt(D) * jax.random.uniform(key_list[19], (), jnp.float32, 0.2, 1.0)
    inputs["clip_norm"] = clip_norm
    return inputs


def reference(act_in, grad_out, w_up1, w_down1, w_up2, w_down2, master_up1, master_down1, master_up2, master_down2, mom_up1, mom_down1, mom_up2, mom_down2, vel_up1, vel_down1, vel_up2, vel_down2, learn_rate, clip_norm):
    rows_dev = ROWS // GROUP
    dev_in = act_in.reshape(GROUP, rows_dev, D)
    dev_grad = grad_out.reshape(GROUP, rows_dev, D)

    def accumulate(carry, block):
        grad_pairs = fwd_bwd(block[0], block[1], w_up1, w_down1, w_up2, w_down2)
        summed = tuple(carry[layer_idx] + jnp.dot(grad_pairs[layer_idx][0].T, grad_pairs[layer_idx][1], preferred_element_type=jnp.float32) for layer_idx in range(4))
        return summed, None

    start_sums = (jnp.zeros((FF, D), jnp.float32), jnp.zeros((D, FF), jnp.float32), jnp.zeros((FF, D), jnp.float32), jnp.zeros((D, FF), jnp.float32))
    totals = lax.scan(accumulate, start_sums, (dev_in, dev_grad))[0]
    grad_list = [totals[3] / GROUP, totals[2] / GROUP, totals[1] / GROUP, totals[0] / GROUP]
    grad_norm = jnp.sqrt(sum(jnp.sum(grad_rows * grad_rows) for grad_rows in grad_list))
    clip_scale = jnp.minimum(1.0, clip_norm / (grad_norm + NORM_EPS))
    state_up1 = adam_step(grad_list[0], master_up1, mom_up1, vel_up1, clip_scale, learn_rate)
    state_down1 = adam_step(grad_list[1], master_down1, mom_down1, vel_down1, clip_scale, learn_rate)
    state_up2 = adam_step(grad_list[2], master_up2, mom_up2, vel_up2, clip_scale, learn_rate)
    state_down2 = adam_step(grad_list[3], master_down2, mom_down2, vel_down2, clip_scale, learn_rate)
    return (state_up1[0], state_down1[0], state_up2[0], state_down2[0], state_up1[1], state_down1[1], state_up2[1], state_down2[1], state_up1[2], state_down1[2], state_up2[2], state_down2[2], state_up1[3], state_down1[3], state_up2[3], state_down2[3], grad_norm)
```

```python
import functools
import math
import jax
import jax.numpy as jnp
from jax import lax
from jax.experimental import pallas as pl
from jax.experimental.pallas import tpu as pltpu
from jax.sharding import PartitionSpec as P

ROOT_HALF = math.sqrt(0.5)
INV_ROOT_TAU = 1.0 / math.sqrt(2.0 * math.pi)
F32, BF16 = jnp.float32, jnp.bfloat16
ANY = pl.BlockSpec(memory_space=pl.ANY)
HBM = pl.BlockSpec(memory_space=pltpu.HBM)

def dot_nn(a, b):
    return lax.dot_general(a, b, (((1,), (0,)), ((), ())), preferred_element_type=F32)
def dot_nt(a, b):
    return lax.dot_general(a, b, (((1,), (1,)), ((), ())), preferred_element_type=F32)

def gelu(z):
    return z * (0.5 * (1.0 + lax.erf(z * ROOT_HALF)))

def kernel_a(cfg, x_hbm, w1_hbm, w2_hbm, z_hbm, u_hbm, ut_hbm, xt_hbm,
             x_v, uacc, zout, w1, w2, h0, h1, sq, sqt, xsem, wsem, zsem, osem):
    nt, nr, rb, ft, d, nd = cfg
    hb = (h0, h1)
    xc = pltpu.make_async_copy(x_hbm, x_v, xsem.at[0])
    xc.start()

    def wcopies(j, slot):
        return (pltpu.make_async_copy(w1_hbm.at[j], w1.at[slot], wsem.at[slot]),
                pltpu.make_async_copy(w2_hbm.at[:, j], w2.at[slot], wsem.at[2 + slot]))
    for c in wcopies(0, 0):
        c.start()
    h1[...] = jnp.zeros_like(h1)
    def zero(r, _):
        uacc[pl.ds(pl.multiple_of(r * rb, rb), rb), :] = jnp.zeros((rb, d), F32)
        return 0
    lax.fori_loop(0, nr, zero, 0)
    xc.wait()
    for c in wcopies(0, 0):
        c.wait()
    zout[0, 0:rb, :] = dot_nn(x_v[0:rb, :], w1[0])

    def tile(j, _):
        slot = lax.rem(j, 2)
        nslot = lax.rem(j + 1, 2)
        pslot = lax.rem(jnp.maximum(j - 1, 0), 2)
        jn = jnp.minimum(j + 1, nt - 1)
        for r in range(nr):
            rows = pl.ds(r * rb, rb)
            pr = (r - 1) % nr
            prow = pl.ds(pr * rb, rb)
            w2p = w2[pslot if r == 0 else slot].reshape(ft, d)
            uacc[prow, :] += dot_nn(hb[(r + 1) % 2][...], w2p)
            if r == 0:
                for c in wcopies(jn, nslot):
                    c.start()
            if r == nr - 1:
                for c in wcopies(jn, nslot):
                    c.wait()
                @pl.when(j >= 1)
                def _():
                    pltpu.make_async_copy(zout.at[nslot], z_hbm.at[jn], zsem.at[nslot]).wait()
            hb[r % 2][...] = gelu(zout[slot, rows, :]).astype(BF16)
            if r < nr - 1:
                zout[slot, pl.ds((r + 1) * rb, rb), :] = dot_nn(x_v[pl.ds((r + 1) * rb, rb), :], w1[slot])
            else:
                zout[nslot, 0:rb, :] = dot_nn(x_v[0:rb, :], w1[nslot])
        pltpu.make_async_copy(zout.at[slot], z_hbm.at[j], zsem.at[slot]).start()
        return 0
    lax.fori_loop(0, nt, tile, 0)
    last = (nt - 1) % 2
    prow = pl.ds((nr - 1) * rb, rb)
    uacc[prow, :] += dot_nn(hb[(nr - 1) % 2][...], w2[last].reshape(ft, d))
    pltpu.make_async_copy(zout.at[last], z_hbm.at[nt - 1], zsem.at[last]).wait()
    def fin(r, _):
        rows = pl.ds(pl.multiple_of(r * rb, rb), rb)
        s = lax.rem(r, 2)
        cps = lambda: (pltpu.make_async_copy(sq.at[s], u_hbm.at[rows, :], osem.at[s]),
               pltpu.make_async_copy(sqt.at[s, 0], ut_hbm.at[:, rows], osem.at[2 + s]),
               pltpu.make_async_copy(sqt.at[s, 1], xt_hbm.at[:, rows], osem.at[4 + s]))
        @pl.when(r >= 2)
        def _():
            for c in cps():
                c.wait()
        v = uacc[rows, :].astype(BF16)
        sq[s] = v
        sqt[s, 0] = v.T
        sqt[s, 1] = x_v[rows, :].T
        for c in cps():
            c.start()
        return 0
    lax.fori_loop(0, nr, fin, 0)
    for s in range(2):
        rows = pl.ds((nr - 2 + s) * rb, rb)
        for c in (pltpu.make_async_copy(sq.at[s], u_hbm.at[rows, :], osem.at[s]),
               pltpu.make_async_copy(sqt.at[s, 0], ut_hbm.at[:, rows], osem.at[2 + s]),
               pltpu.make_async_copy(sqt.at[s, 1], xt_hbm.at[:, rows], osem.at[4 + s])):
            c.wait()

def forward_one(x, w1p, w2r):
    t, d = x.shape
    nt, _, ft = w1p.shape
    nd = w2r.shape[0]
    nr = 8
    rb = t // nr
    cfg = (nt, nr, rb, ft, d, nd)
    return pl.pallas_call(
        functools.partial(kernel_a, cfg),
        out_shape=(jax.ShapeDtypeStruct((nt, t, ft), F32), jax.ShapeDtypeStruct((t, d), BF16),
                   jax.ShapeDtypeStruct((d, t), BF16), jax.ShapeDtypeStruct((d, t), BF16)),
        in_specs=[HBM] * 3, out_specs=(HBM,) * 4,
        scratch_shapes=[
            pltpu.VMEM((t, d), BF16), pltpu.VMEM((t, d), F32), pltpu.VMEM((2, t, ft), F32),
            pltpu.VMEM((2, d, ft), BF16), pltpu.VMEM((2, nd, ft // nd, d), BF16),
            pltpu.VMEM((rb, ft), BF16), pltpu.VMEM((rb, ft), BF16),
            pltpu.VMEM((2, rb, d), BF16), pltpu.VMEM((2, 2, d, rb), BF16),
            pltpu.SemaphoreType.DMA((1,)), pltpu.SemaphoreType.DMA((4,)),
            pltpu.SemaphoreType.DMA((2,)), pltpu.SemaphoreType.DMA((6,))],
        compiler_params=pltpu.CompilerParams(vmem_limit_bytes=64 * 1024 * 1024 - 65536),
        name="forward_one",
    )(x, w1p, w2r)


MESH = pl.DeviceIdType.MESH

def gelu_pair(pre):
    normal_cdf = 0.5 * (1.0 + lax.erf(pre * ROOT_HALF))
    density = jnp.exp(-0.5 * pre * pre) * INV_ROOT_TAU
    return pre * normal_cdf, normal_cdf + pre * density

def flip(value, step):
    return value + step * (1 - 2 * lax.rem(lax.div(value, step), 2))

ORDERS = ((0, 2, 1), (1, 2, 0))

def kernel_bc(cfg, u_hbm, ut_hbm, e_hbm, xt_hbm, z_hbm, w3_hbm, w4_hbm, w2_hbm,
              gu_hbm, gd_hbm, nrm_ref,
              act, actt, e_v, euacc, wa, wb, zb0, zb1, eb0, eb1, ht0, ht1, q0, q1,
              gu, gd, r0u, r0d, au, ad, r1u, r1d, r2u, r2d, r3u, r3d, fu, fd, nu, nd_acc, nsend, nrecv,
              insem, wsem, zsem, ssem, rsem, fsem, nsem):
    nt, nr, rb, ft, d, nd = cfg
    total = 2 * nt
    me = lax.axis_index("data")
    core = lax.rem(me, 2)
    chip = lax.div(me, 2)
    bits = [lax.rem(lax.div(chip, 1 << k), 2) for k in range(3)]
    partner = flip(me, 1)
    zb, eb, htb, qb = (zb0, zb1), (eb0, eb1), (ht0, ht1), (q0, q1)
    G, R, ACC, FIN, NRM, OUT = (gu, gd), ((r0u, r1u, r2u, r3u), (r0d, r1d, r2d, r3d)), (au, ad), (fu, fd), (nu, nd_acc), (gu_hbm, gd_hbm)

    loads = [pltpu.make_async_copy(u_hbm, act, insem.at[0]), pltpu.make_async_copy(ut_hbm, actt, insem.at[1]),
             pltpu.make_async_copy(e_hbm, e_v, insem.at[2])]
    for c in loads:
        c.start()

    def wcopies(j, slot, back):
        second = w2_hbm if back else w4_hbm
        cps = [pltpu.make_async_copy(second.at[:, j], wb.at[slot], wsem.at[2 + slot])]
        if not back:
            cps.append(pltpu.make_async_copy(w3_hbm.at[j], wa.at[slot], wsem.at[slot]))
        return cps
    for c in wcopies(0, 0, False):
        c.start()

    barrier = pltpu.get_barrier_semaphore()
    for k in range(1, nd):
        pl.semaphore_signal(barrier, inc=1, device_id=(lax.rem(me + k, nd),), device_id_type=MESH)
    pl.semaphore_wait(barrier, nd - 1)

    nu[...] = jnp.zeros_like(nu)
    nd_acc[...] = jnp.zeros_like(nd_acc)
    def zero(r, _):
        euacc[pl.ds(pl.multiple_of(r * rb, rb), rb), :] = jnp.zeros((rb, d), F32)
        return 0
    lax.fori_loop(0, nr, zero, 0)

    def owner_chip(kind, p):
        out = 0
        for place, axis in enumerate(ORDERS[kind]):
            bit = bits[axis] if not (p >> (2 - place)) & 1 else 1 - bits[axis]
            out = out + bit * (1 << axis)
        return out

    def send(kind, stage, j):
        two = lax.rem(j, 2)
        four = lax.rem(j, 4)
        sem = (kind * 4 + stage) * 2 + two
        if stage == 0:
            src, dst, dev = G[kind].at[two, :, 1 - core], R[kind][0].at[two], partner
        else:
            lo = 8 >> stage
            src, dst = ACC[kind].at[four, pl.ds(lo, lo)], R[kind][stage].at[two]
            dev = flip(me, 2 << ORDERS[kind][stage - 1])
        return pltpu.make_async_remote_copy(src_ref=src, dst_ref=dst, send_sem=ssem.at[sem], recv_sem=rsem.at[sem],
                                            device_id=(dev,), device_id_type=MESH)

    def final_copy(kind, j):
        two = lax.rem(j, 2)
        return pltpu.make_async_copy(FIN[kind].at[two], OUT[kind].at[j], fsem.at[kind * 2 + two])

    def when_valid(j, fn):
        @pl.when(jnp.logical_and(j >= 0, j < total))
        def _():
            fn(j)

    def comm(step):
        def stage3(j):
            two, four = lax.rem(j, 2), lax.rem(j, 4)
            for kind in range(2):
                @pl.when(j >= 2)
                def _():
                    final_copy(kind, j - 2).wait()
                send(kind, 3, j).wait()
                f = (ACC[kind][four, 0] + R[kind][3][two, 0]) * (1.0 / nd)
                FIN[kind][two] = f
                NRM[kind][...] += f * f
            for kind in range(2):
                final_copy(kind, j).start()
        def stage2(j):
            two, four = lax.rem(j, 2), lax.rem(j, 4)
            for kind in range(2):
                send(kind, 2, j).wait()
                ACC[kind][four, 0:2] += R[kind][2][two]
            for kind in range(2):
                send(kind, 3, j).start()
        def stage1(j):
            two, four = lax.rem(j, 2), lax.rem(j, 4)
            for kind in range(2):
                send(kind, 1, j).wait()
                ACC[kind][four, 0:4] += R[kind][1][two]
            for kind in range(2):
                send(kind, 2, j).start()
        def stage0(j):
            two, four = lax.rem(j, 2), lax.rem(j, 4)
            for kind in range(2):
                send(kind, 0, j).wait()
                for p in range(8):
                    oc = owner_chip(kind, p)
                    ACC[kind][four, p] = G[kind][two, oc, core] + R[kind][0][two, oc]
            for kind in range(2):
                send(kind, 1, j).start()
        def start(j):
            for kind in range(2):
                send(kind, 0, j).start()
        when_valid(step - 5, stage3)
        when_valid(step - 4, stage2)
        when_valid(step - 3, stage1)
        when_valid(step - 2, stage0)
        when_valid(step - 1, start)

    def add_grads(slot, first, upd_u, upd_d):
        bu, bd = upd_u.reshape(gu.shape[1:]), upd_d.reshape(gd.shape[1:])
        gu[slot] = bu if first else gu[slot] + bu
        gd[slot] = bd if first else gd[slot] + bd

    for c in loads:
        c.wait()

    def tile_b(j, _):
        slot = lax.rem(j, 2)
        comm(j)
        for c in wcopies(j, slot, False):
            c.wait()
        @pl.when(j + 1 < nt)
        def _():
            for c in wcopies(j + 1, 1 - slot, False):
                c.start()
        def front(r):
            rows = pl.ds(r * rb, rb)
            zb[r % 2][...] = dot_nn(act[rows, :], wa[slot])
            eb[r % 2][...] = dot_nt(e_v[rows, :], wb[slot].reshape(ft, d)).astype(BF16)
        def middle(r):
            h, der = gelu_pair(zb[r % 2][...])
            htb[r % 2][...] = h.astype(BF16).T
            qb[r % 2][...] = (eb[r % 2][...].astype(F32) * der).astype(BF16)
        def back(r):
            rows = pl.ds(r * rb, rb)
            q = qb[r % 2][...]
            euacc[rows, :] += dot_nt(q, wa[slot])
            add_grads(slot, r == 0, dot_nn(actt[:, rows], q), dot_nn(htb[r % 2][...], e_v[rows, :]))
        front(0)
        for r in range(nr):
            middle(r)
            if r + 1 < nr:
                front(r + 1)
            if r >= 1:
                back(r - 1)
        back(nr - 1)
        return 0
    lax.fori_loop(0, nt, tile_b, 0)

    xt_in = pltpu.make_async_copy(xt_hbm, actt, insem.at[1])
    xt_in.start()
    for c in wcopies(0, nt % 2, True):
        c.start()
    def cast(r, _):
        rows = pl.ds(pl.multiple_of(r * rb, rb), rb)
        act[rows, :] = euacc[rows, :].astype(BF16)
        return 0
    lax.fori_loop(0, nr, cast, 0)
    def zcopy(j, slot):
        return pltpu.make_async_copy(z_hbm.at[j], euacc.at[:, pl.ds(pl.multiple_of(slot * ft, ft), ft)], zsem.at[slot])
    zcopy(0, nt % 2).start()
    xt_in.wait()

    def tile_c(step, _):
        j = step - nt
        slot = lax.rem(step, 2)
        comm(step)
        for c in wcopies(j, slot, True):
            c.wait()
        zcopy(j, slot).wait()
        @pl.when(j + 1 < nt)
        def _():
            for c in wcopies(j + 1, 1 - slot, True):
                c.start()
            zcopy(j + 1, 1 - slot).start()
        def front(r):
            rows = pl.ds(r * rb, rb)
            eb[r % 2][...] = dot_nt(act[rows, :], wb[slot].reshape(ft, d)).astype(BF16)
        def middle(r):
            rows = pl.ds(r * rb, rb)
            h, der = gelu_pair(euacc[rows, pl.ds(pl.multiple_of(slot * ft, ft), ft)])
            htb[r % 2][...] = h.astype(BF16).T
            qb[r % 2][...] = (eb[r % 2][...].astype(F32) * der).astype(BF16)
        def back(r):
            rows = pl.ds(r * rb, rb)
            add_grads(slot, r == 0, dot_nn(actt[:, rows], qb[r % 2][...]), dot_nn(htb[r % 2][...], act[rows, :]))
        front(0)
        for r in range(nr):
            middle(r)
            if r + 1 < nr:
                front(r + 1)
            if r >= 1:
                back(r - 1)
        back(nr - 1)
        return 0
    lax.fori_loop(nt, total, tile_c, 0)

    def drain(step, _):
        comm(step)
        return 0
    lax.fori_loop(total, total + 5, drain, 0)
    for kind in range(2):
        for j in (total - 2, total - 1):
            final_copy(kind, j).wait()

    part = jnp.zeros((8, 128), F32)
    for ref in (nu, nd_acc):
        rows, cols = ref.shape
        for a in range(rows // 8):
            for b in range(cols // 128):
                part = part + ref[8 * a:8 * a + 8, 128 * b:128 * b + 128]
    nsend[...] = part
    nrecv[me] = part
    for k in range(1, nd):
        pltpu.make_async_remote_copy(src_ref=nsend, dst_ref=nrecv.at[me], send_sem=nsem.at[0], recv_sem=nsem.at[1],
                                     device_id=(lax.rem(me + k, nd),), device_id_type=MESH).start()
    others = nrecv.at[pl.ds(0, nd - 1)]
    pltpu.make_async_remote_copy(src_ref=others, dst_ref=others, send_sem=nsem.at[0], recv_sem=nsem.at[1],
                                 device_id=(me,), device_id_type=MESH).wait()
    total_sq = nrecv[0]
    for k in range(1, nd):
        total_sq = total_sq + nrecv[k]
    nrm_ref[...] = total_sq

def backward(u, ut, e, xt, z, w3p, w4r, w2r):
    t, d = u.shape
    nt, _, ft = w3p.shape
    nd = w4r.shape[0]
    nr = 8
    rb = t // nr
    bu, bd = (d // nd, ft), (ft // nd, d)
    cfg = (nt, nr, rb, ft, d, nd)
    V = pltpu.VMEM
    scratch = [V((t, d), BF16), V((d, t), BF16), V((t, d), BF16), V((t, d), F32),
               V((2, d, ft), BF16), V((2, nd, ft // nd, d), BF16),
               V((rb, ft), F32), V((rb, ft), F32), V((rb, ft), BF16), V((rb, ft), BF16),
               V((ft, rb), BF16), V((ft, rb), BF16), V((rb, ft), BF16), V((rb, ft), BF16),
               V((2, 8, 2) + bu, F32), V((2, 8, 2) + bd, F32)]
    for n, c in ((2, 8), (4, 8), (2, 4), (2, 2), (2, 1)):
        scratch += [V((n, c) + bu, F32), V((n, c) + bd, F32)]
    scratch += [V((2,) + bu, F32), V((2,) + bd, F32), V(bu, F32), V(bd, F32), V((8, 128), F32), V((nd, 8, 128), F32)]
    D = pltpu.SemaphoreType.DMA
    scratch += [D((3,)), D((4,)), D((2,)), D((16,)), D((16,)), D((4,)), D((2,))]
    return pl.pallas_call(
        functools.partial(kernel_bc, cfg),
        out_shape=(jax.ShapeDtypeStruct((2 * nt,) + bu, F32), jax.ShapeDtypeStruct((2 * nt,) + bd, F32),
                   jax.ShapeDtypeStruct((8, 128), F32)),
        in_specs=[HBM] * 8, out_specs=(HBM, HBM, pl.BlockSpec(memory_space=pltpu.VMEM)),
        scratch_shapes=scratch,
        compiler_params=pltpu.CompilerParams(collective_id=0, has_side_effects=True, vmem_limit_bytes=64 * 1024 * 1024 - 65536),
        name="backward",
    )(u, ut, e, xt, z, w3p, w4r, w2r)

def kernel_permute(nd, nt, w1_ref, w3_ref, o1_ref, o3_ref):
    w = 16
    for src, dst in ((w1_ref, o1_ref), (w3_ref, o3_ref)):
        for j in range(nt):
            dst[j] = jnp.concatenate([src[:, (d * nt + j) * w:(d * nt + j + 1) * w] for d in range(nd)], axis=1)

def permute(w1, w3, nd, rows):
    d, f = w1.shape
    nt = f // (nd * 16)
    ft = nd * 16
    return pl.pallas_call(functools.partial(kernel_permute, nd, nt),
        grid=(d // rows,),
        in_specs=[pl.BlockSpec((rows, f), lambda i: (i, 0))] * 2,
        out_specs=[pl.BlockSpec((nt, rows, ft), lambda i: (0, i, 0))] * 2,
        out_shape=[jax.ShapeDtypeStruct((nt, d, ft), BF16)] * 2, name="permute")(w1, w3)


STEP = 20
BETA_ONE = 0.9
BETA_TWO = 0.95
EPSILON = 1e-8
NORM_EPS = 1e-6
CORR_ONE = 1.0 - BETA_ONE ** STEP
CORR_TWO = 1.0 - BETA_TWO ** STEP


def adam_step(grad_rows, master_old, mom_old, vel_old, clip_scale, learn_rate):
    scaled = clip_scale * grad_rows
    mom_new = BETA_ONE * mom_old + (1.0 - BETA_ONE) * scaled
    vel_new = BETA_TWO * vel_old + (1.0 - BETA_TWO) * scaled * scaled
    master_new = master_old - learn_rate * (mom_new / CORR_ONE) / (jnp.sqrt(vel_new / CORR_TWO) + EPSILON)
    return master_new.astype(jnp.bfloat16), master_new, mom_new, vel_new


def solution(mesh):
    groups = mesh.shape["data"]
    rows_spec = P("data", None)
    full_spec = P(None, None)
    scalar_spec = P()

    def shard_body(act_in, grad_out, w_up1, w_down1, w_up2, w_down2, master_up1, master_down1, master_up2, master_down2, mom_up1, mom_down1, mom_up2, mom_down2, vel_up1, vel_down1, vel_up2, vel_down2, learn_rate, clip_norm):
        ff, d = w_down1.shape
        nt = ff // (groups * 16)
        up1_tiles, up2_tiles = permute(w_up1, w_up2, groups, 64)
        down1_tiles = w_down1.reshape(groups, nt, 16, d)
        down2_tiles = w_down2.reshape(groups, nt, 16, d)
        pre1, mid, mid_t, in_t = forward_one(act_in, up1_tiles, down1_tiles)
        grads_up, grads_down, sq = backward(mid, mid_t, grad_out, in_t, pre1, up2_tiles, down2_tiles, down1_tiles)
        grad_norm = jnp.sqrt(jnp.sum(sq))
        clip_scale = jnp.minimum(1.0, clip_norm / (grad_norm + NORM_EPS))

        def up_rows(tiles):
            rows = tiles.shape[1]
            return tiles.reshape(nt, rows, groups, 16).transpose(1, 2, 0, 3).reshape(rows, ff)

        grad_list = (up_rows(grads_up[nt:]), grads_down[nt:].reshape(ff // groups, d), up_rows(grads_up[:nt]), grads_down[:nt].reshape(ff // groups, d))
        master_list = (master_up1, master_down1, master_up2, master_down2)
        mom_list = (mom_up1, mom_down1, mom_up2, mom_down2)
        vel_list = (vel_up1, vel_down1, vel_up2, vel_down2)
        layer_states = [adam_step(grad_list[layer_idx], master_list[layer_idx], mom_list[layer_idx], vel_list[layer_idx], clip_scale, learn_rate) for layer_idx in range(4)]
        new_weights = [lax.all_gather(layer_state[0], "data", axis=0, tiled=True) for layer_state in layer_states]
        results = new_weights
        for field_idx in range(1, 4):
            results = results + [layer_state[field_idx] for layer_state in layer_states]
        return tuple(results + [grad_norm])

    in_specs = (rows_spec, rows_spec) + (full_spec,) * 4 + (rows_spec,) * 12 + (scalar_spec, scalar_spec)
    out_specs = (full_spec,) * 4 + (rows_spec,) * 12 + (scalar_spec,)
    return jax.shard_map(shard_body, mesh=mesh, in_specs=in_specs, out_specs=out_specs, check_vma=False)
```

```python
import functools
import math
import jax
import jax.numpy as jnp
from jax import lax
from jax.experimental import pallas as pl
from jax.experimental.pallas import tpu as pltpu
from jax.sharding import PartitionSpec as P

ROOT_HALF = math.sqrt(0.5)
INV_ROOT_TAU = 1.0 / math.sqrt(2.0 * math.pi)
F32, BF16 = jnp.float32, jnp.bfloat16
HBM = pl.BlockSpec(memory_space=pltpu.HBM)
VMEM_MAX = 64 * 1024 * 1024 - 65536
BLOCKS = 8


def dot_nn(a, b):
    return lax.dot_general(a, b, (((1,), (0,)), ((), ())), preferred_element_type=F32)


def dot_nt(a, b):
    return lax.dot_general(a, b, (((1,), (1,)), ((), ())), preferred_element_type=F32)


def gelu(z):
    return z * (0.5 * (1.0 + lax.erf(z * ROOT_HALF)))


def kernel_a(cfg, x_hbm, w1_hbm, w3_hbm, w2_hbm, z_hbm, u_hbm, ut_hbm, xt_hbm, w3p_hbm,
             x_v, uacc, zout, w1_v, w3_v, w1, w3, w2, h0, h1, sq, sqt, xsem, wsem, zsem, osem):
    nt, nr, rb, ft, d, nd = cfg
    hb = (h0, h1)
    step16 = ft // nd
    loads = [pltpu.make_async_copy(w1_hbm, w1_v, xsem.at[0]), pltpu.make_async_copy(x_hbm, x_v, xsem.at[1]),
             pltpu.make_async_copy(w3_hbm, w3_v, xsem.at[2])]
    for c in loads:
        c.start()

    def w2copy(j, slot):
        return pltpu.make_async_copy(w2_hbm.at[:, j], w2.at[slot], wsem.at[slot])

    def w3copy(j, slot):
        return pltpu.make_async_copy(w3.at[slot], w3p_hbm.at[j], wsem.at[2 + slot])

    def zcopy(j, slot):
        return pltpu.make_async_copy(zout.at[slot], z_hbm.at[j], zsem.at[slot])

    def xtcopy(r):
        return pltpu.make_async_copy(sqt, xt_hbm.at[:, pl.ds(pl.multiple_of(r * rb, rb), rb)], osem.at[0])
    w2copy(0, 0).start()

    lanes = 128
    per = lanes // step16
    group = lax.broadcasted_iota(jnp.int32, (d, lanes), 1) // step16

    def permute(src, dst, j, slot):
        for half in range(nd // per):
            acc = None
            for k in range(per // 2):
                pair = []
                for q in (k, k + per // 2):
                    place = nt * (half * per + q) + j
                    col = pl.multiple_of(lax.div(place, per) * lanes, lanes)
                    pair.append((src[:, pl.ds(col, lanes)], lax.rem(place, per)))
                mixed = jnp.where(group == pair[0][1], pair[0][0], pair[1][0])
                shift = lax.rem(k - pair[0][1] + per, per) * step16
                turned = pltpu.roll(mixed, shift, 1)
                acc = turned if acc is None else jnp.where(lax.rem(group, per // 2) == k, turned, acc)
            dst[slot, :, half * lanes:(half + 1) * lanes] = acc

    def zero(r, _):
        uacc[pl.ds(pl.multiple_of(r * rb, rb), rb), :] = jnp.zeros((rb, d), F32)
        return 0
    lax.fori_loop(0, nr, zero, 0)
    loads[0].wait()
    permute(w1_v, w1, 0, 0)
    loads[1].wait()
    loads[2].wait()

    def tile(j, _):
        slot = lax.rem(j, 2)
        nslot = 1 - slot
        xr = lax.rem(j, nr)
        @pl.when(j >= 2)
        def _():
            zcopy(j - 2, slot).wait()
            w3copy(j - 2, slot).wait()
        @pl.when(jnp.logical_and(j >= 1, j <= nr))
        def _():
            xtcopy(j - 1).wait()
        w2copy(j, slot).wait()
        @pl.when(j + 1 < nt)
        def _():
            w2copy(j + 1, nslot).start()
        def front(r):
            rows = pl.ds(r * rb, rb)
            zout[slot, rows, :] = dot_nn(x_v[rows, :], w1[slot])
        def middle(r):
            hb[r % 2][...] = gelu(zout[slot, pl.ds(r * rb, rb), :]).astype(BF16)
        def back(r):
            uacc[pl.ds(r * rb, rb), :] += dot_nn(hb[r % 2][...], w2[slot].reshape(ft, d))
        front(0)
        for r in range(nr):
            middle(r)
            if r + 1 < nr:
                front(r + 1)
            if r >= 1:
                back(r - 1)
            if r == 1:
                permute(w1_v, w1, jnp.minimum(j + 1, nt - 1), nslot)
            if r == 3:
                permute(w3_v, w3, j, slot)
            if r == 5:
                sqt[...] = x_v[pl.ds(pl.multiple_of(xr * rb, rb), rb), :].T
        back(nr - 1)
        zcopy(j, slot).start()
        w3copy(j, slot).start()
        @pl.when(j < nr)
        def _():
            xtcopy(j).start()
        return 0
    lax.fori_loop(0, nt, tile, 0)
    if nt <= nr:
        xtcopy(nt - 1).wait()
        for r in range(nt, nr):
            sqt[...] = x_v[pl.ds(r * rb, rb), :].T
            xtcopy(r).start()
            xtcopy(r).wait()

    def fin(r, _):
        rows = pl.ds(pl.multiple_of(r * rb, rb), rb)
        x_v[rows, :] = uacc[rows, :].astype(BF16)
        pltpu.make_async_copy(x_v.at[rows, :], u_hbm.at[rows, :], osem.at[1]).start()
        return 0
    lax.fori_loop(0, nr, fin, 0)
    def fin_t(r, _):
        rows = pl.ds(pl.multiple_of(r * rb, rb), rb)
        sq[r] = x_v[rows, :].T
        pltpu.make_async_copy(sq.at[r], ut_hbm.at[:, rows], osem.at[2]).start()
        return 0
    lax.fori_loop(0, nr, fin_t, 0)
    pltpu.make_async_copy(x_v, u_hbm, osem.at[1]).wait()
    pltpu.make_async_copy(ut_hbm, ut_hbm, osem.at[2]).wait()
    for j in (nt - 2, nt - 1):
        zcopy(j, j % 2).wait()
        w3copy(j, j % 2).wait()


def forward_one(x, w1, w3, w2r):
    t, d = x.shape
    nd, nt, rows2, _ = w2r.shape
    ft, nr = nd * rows2, BLOCKS
    rb = t // nr
    V, D = pltpu.VMEM, pltpu.SemaphoreType.DMA
    S = jax.ShapeDtypeStruct
    return pl.pallas_call(
        functools.partial(kernel_a, (nt, nr, rb, ft, d, nd)),
        out_shape=(S((nt, t, ft), F32), S((t, d), BF16), S((d, t), BF16), S((d, t), BF16), S((nt, d, ft), BF16)),
        in_specs=[HBM] * 4, out_specs=(HBM,) * 5,
        scratch_shapes=[
            V((t, d), BF16), V((t, d), F32), V((2, t, ft), F32), V(w1.shape, BF16), V(w3.shape, BF16),
            V((2, d, ft), BF16), V((2, d, ft), BF16), V((2, nd, rows2, d), BF16),
            V((rb, ft), BF16), V((rb, ft), BF16), V((nr, d, rb), BF16), V((d, rb), BF16),
            D((3,)), D((4,)), D((2,)), D((3,))],
        compiler_params=pltpu.CompilerParams(vmem_limit_bytes=VMEM_MAX),
        name="forward_one",
    )(x, w1, w3, w2r)


MESH = pl.DeviceIdType.MESH

def gelu_pair(pre):
    normal_cdf = 0.5 * (1.0 + lax.erf(pre * ROOT_HALF))
    density = jnp.exp(-0.5 * pre * pre) * INV_ROOT_TAU
    return pre * normal_cdf, normal_cdf + pre * density

def flip(value, step):
    return value + step * (1 - 2 * lax.rem(lax.div(value, step), 2))

def relative(kind, p, bits):
    out = 0
    for place, axis in enumerate(reversed(ORDERS[kind])):
        out = out + (1 - bits[axis] if (p >> place) & 1 else bits[axis]) * (1 << axis)
    return out


def position():
    me = lax.axis_index("data")
    chip = lax.div(me, 2)
    return me, lax.rem(me, 2), [lax.rem(lax.div(chip, 1 << k), 2) for k in range(3)]


ORDERS = ((0, 2, 1), (1, 2, 0))
PARTS = 8
SEEN = (2, 4, 6, 7)
DEPTH = (2, 4, 4, 2)
LAST = len(SEEN) - 1
ACCS = 5

def kernel_bc(cfg, u_hbm, ut_hbm, e_hbm, xt_hbm, z_hbm, w3_hbm, w4_hbm, w2_hbm,
              gu_hbm, gd_hbm, nrm_ref,
              act, actt, e_v, euacc, wa, wb, zb0, zb1, eb0, eb1, ht0, ht1, q0, q1,
              gu, gd, r0u, r0d, au, ad, r1u, r1d, r2u, r2d, r3u, r3d, fu, fd, nu, nd_acc, nsend, nrecv,
              insem, wsem, zsem, ssem, rsem, fsem, nsem):
    nt, nr, rb, ft, d, nd = cfg
    total = 2 * nt
    me, core, bits = position()
    partner = flip(me, 1)
    zb, eb, htb, qb = (zb0, zb1), (eb0, eb1), (ht0, ht1), (q0, q1)
    G, R, ACC, FIN, NRM, OUT = (gu, gd), ((r0u, r1u, r2u, r3u), (r0d, r1d, r2d, r3d)), (au, ad), (fu, fd), (nu, nd_acc), (gu_hbm, gd_hbm)

    loads = [pltpu.make_async_copy(u_hbm, act, insem.at[0]), pltpu.make_async_copy(ut_hbm, actt, insem.at[1]),
             pltpu.make_async_copy(e_hbm, e_v, insem.at[2])]
    for c in loads:
        c.start()

    def wcopies(j, slot, back):
        second = w2_hbm if back else w4_hbm
        cps = [pltpu.make_async_copy(second.at[:, j], wb.at[slot], wsem.at[1, slot])]
        if not back:
            cps.append(pltpu.make_async_copy(w3_hbm.at[j], wa.at[slot], wsem.at[0, slot]))
        return cps
    for c in wcopies(0, 0, False):
        c.start()

    barrier = pltpu.get_barrier_semaphore()
    for k in range(1, nd):
        pl.semaphore_signal(barrier, inc=1, device_id=(lax.rem(me + k, nd),), device_id_type=MESH)
    pl.semaphore_wait(barrier, nd - 1)

    nu[...] = jnp.zeros_like(nu)
    nd_acc[...] = jnp.zeros_like(nd_acc)
    def zero(r, _):
        euacc[pl.ds(pl.multiple_of(r * rb, rb), rb), :] = jnp.zeros((rb, d), F32)
        return 0
    lax.fori_loop(0, nr, zero, 0)

    def owner_chip(kind, p):
        return relative(kind, p, bits)

    def send(kind, stage, j):
        depth = R[kind][stage].shape[0]
        slot = lax.rem(j, depth)
        sem = (kind * len(SEEN) + stage) * max(DEPTH) + slot
        dst = R[kind][stage].at[slot]
        if stage == 0:
            src, dev = G[kind].at[slot, :, 1 - core], partner
        else:
            lo = PARTS >> stage
            src, dev = ACC[kind].at[lax.rem(j, ACCS), pl.ds(lo, lo)], flip(me, 2 << ORDERS[kind][stage - 1])
        return pltpu.make_async_remote_copy(src_ref=src, dst_ref=dst, send_sem=ssem.at[sem], recv_sem=rsem.at[sem],
                                            device_id=(dev,), device_id_type=MESH)

    def final_copy(kind, j):
        slot = lax.rem(j, 2)
        return pltpu.make_async_copy(FIN[kind].at[slot], OUT[kind].at[j], fsem.at[kind, slot])

    def absorb(stage, j):
        place = lax.rem(j, ACCS)
        for kind in range(2):
            send(kind, stage, j).wait()
            slot = lax.rem(j, R[kind][stage].shape[0])
            got, acc = R[kind][stage], ACC[kind]
            if stage == 0:
                for p in range(PARTS):
                    oc = owner_chip(kind, p)
                    acc[place, p] = G[kind][slot, oc, core] + got[slot, oc]
            elif stage < LAST:
                keep = pl.ds(0, PARTS >> stage)
                acc[place, keep] += got[slot]
            else:
                @pl.when(j >= 2)
                def _():
                    final_copy(kind, j - 2).wait()
                f = (acc[place, 0] + got[slot, 0]) * (1.0 / nd)
                FIN[kind][lax.rem(j, 2)] = f
                NRM[kind][...] += f * f
        for kind in range(2):
            (send(kind, stage + 1, j) if stage < LAST else final_copy(kind, j)).start()

    def comm(step):
        def when_valid(j, fn):
            @pl.when(jnp.logical_and(j >= 0, j < total))
            def _():
                fn()
        for stage in reversed(range(len(SEEN))):
            when_valid(step - SEEN[stage], functools.partial(absorb, stage, step - SEEN[stage]))
        def start():
            for kind in range(2):
                send(kind, 0, step - 1).start()
        when_valid(step - 1, start)

    def add_grads(slot, first, upd_u, upd_d):
        bu, bd = upd_u.reshape(gu.shape[1:]), upd_d.reshape(gd.shape[1:])
        gu[slot] = bu if first else gu[slot] + bu
        gd[slot] = bd if first else gd[slot] + bd

    for c in loads:
        c.wait()

    def tile_b(j, _):
        slot = lax.rem(j, 2)
        comm(j)
        for c in wcopies(j, slot, False):
            c.wait()
        @pl.when(j + 1 < nt)
        def _():
            for c in wcopies(j + 1, 1 - slot, False):
                c.start()
        def front(r):
            rows = pl.ds(r * rb, rb)
            zb[r % 2][...] = dot_nn(act[rows, :], wa[slot])
            eb[r % 2][...] = dot_nt(e_v[rows, :], wb[slot].reshape(ft, d)).astype(BF16)
        def middle(r):
            h, der = gelu_pair(zb[r % 2][...])
            htb[r % 2][...] = h.astype(BF16).T
            qb[r % 2][...] = (eb[r % 2][...].astype(F32) * der).astype(BF16)
        def back(r):
            rows = pl.ds(r * rb, rb)
            q = qb[r % 2][...]
            euacc[rows, :] += dot_nt(q, wa[slot])
            add_grads(slot, r == 0, dot_nn(actt[:, rows], q), dot_nn(htb[r % 2][...], e_v[rows, :]))
        front(0)
        for r in range(nr):
            middle(r)
            if r + 1 < nr:
                front(r + 1)
            if r >= 1:
                back(r - 1)
        back(nr - 1)
        return 0
    lax.fori_loop(0, nt, tile_b, 0)

    xt_in = pltpu.make_async_copy(xt_hbm, actt, insem.at[1])
    xt_in.start()
    for c in wcopies(0, nt % 2, True):
        c.start()
    def cast(r, _):
        rows = pl.ds(pl.multiple_of(r * rb, rb), rb)
        act[rows, :] = euacc[rows, :].astype(BF16)
        return 0
    lax.fori_loop(0, nr, cast, 0)
    def zcopy(j, slot):
        return pltpu.make_async_copy(z_hbm.at[j], euacc.at[:, pl.ds(pl.multiple_of(slot * ft, ft), ft)], zsem.at[slot])
    zcopy(0, nt % 2).start()
    xt_in.wait()

    def tile_c(step, _):
        j = step - nt
        slot = lax.rem(step, 2)
        comm(step)
        for c in wcopies(j, slot, True):
            c.wait()
        zcopy(j, slot).wait()
        @pl.when(j + 1 < nt)
        def _():
            for c in wcopies(j + 1, 1 - slot, True):
                c.start()
            zcopy(j + 1, 1 - slot).start()
        def front(r):
            rows = pl.ds(r * rb, rb)
            eb[r % 2][...] = dot_nt(act[rows, :], wb[slot].reshape(ft, d)).astype(BF16)
        def middle(r):
            rows = pl.ds(r * rb, rb)
            h, der = gelu_pair(euacc[rows, pl.ds(pl.multiple_of(slot * ft, ft), ft)])
            htb[r % 2][...] = h.astype(BF16).T
            qb[r % 2][...] = (eb[r % 2][...].astype(F32) * der).astype(BF16)
        def back(r):
            rows = pl.ds(r * rb, rb)
            add_grads(slot, r == 0, dot_nn(actt[:, rows], qb[r % 2][...]), dot_nn(htb[r % 2][...], act[rows, :]))
        front(0)
        for r in range(nr):
            middle(r)
            if r + 1 < nr:
                front(r + 1)
            if r >= 1:
                back(r - 1)
        back(nr - 1)
        return 0
    lax.fori_loop(nt, total, tile_c, 0)

    def drain(step, _):
        comm(step)
        return 0
    lax.fori_loop(total, total + SEEN[LAST], drain, 0)
    for kind in range(2):
        for j in (total - 2, total - 1):
            final_copy(kind, j).wait()

    part = jnp.zeros((8, 128), F32)
    for ref in (nu, nd_acc):
        rows, cols = ref.shape
        for a in range(rows // 8):
            for b in range(cols // 128):
                part = part + ref[8 * a:8 * a + 8, 128 * b:128 * b + 128]
    nsend[...] = part
    nrecv[me] = part
    for k in range(1, nd):
        pltpu.make_async_remote_copy(src_ref=nsend, dst_ref=nrecv.at[me], send_sem=nsem.at[0], recv_sem=nsem.at[1],
                                     device_id=(lax.rem(me + k, nd),), device_id_type=MESH).start()
    others = nrecv.at[pl.ds(0, nd - 1)]
    pltpu.make_async_remote_copy(src_ref=others, dst_ref=others, send_sem=nsem.at[0], recv_sem=nsem.at[1],
                                 device_id=(me,), device_id_type=MESH).wait()
    total_sq = nrecv[0]
    for k in range(1, nd):
        total_sq = total_sq + nrecv[k]
    nrm_ref[...] = total_sq

def backward(u, ut, e, xt, z, w3p, w4r, w2r):
    t, d = u.shape
    nt, _, ft = w3p.shape
    nd = w4r.shape[0]
    nr = 8
    rb = t // nr
    bu, bd = (d // nd, ft), (ft // nd, d)
    cfg = (nt, nr, rb, ft, d, nd)
    V = pltpu.VMEM
    scratch = [V((t, d), BF16), V((d, t), BF16), V((t, d), BF16), V((t, d), F32),
               V((2, d, ft), BF16), V((2, nd, ft // nd, d), BF16),
               V((rb, ft), F32), V((rb, ft), F32), V((rb, ft), BF16), V((rb, ft), BF16),
               V((ft, rb), BF16), V((ft, rb), BF16), V((rb, ft), BF16), V((rb, ft), BF16),
               V((2, 8, 2) + bu, F32), V((2, 8, 2) + bd, F32)]
    for n, c in ((DEPTH[0], PARTS), (ACCS, PARTS)) + tuple((DEPTH[k], PARTS >> k) for k in range(1, LAST + 1)):
        scratch += [V((n, c) + bu, F32), V((n, c) + bd, F32)]
    scratch += [V((2,) + bu, F32), V((2,) + bd, F32), V(bu, F32), V(bd, F32), V((8, 128), F32), V((nd, 8, 128), F32)]
    D = pltpu.SemaphoreType.DMA
    scratch += [D((3,)), D((2, 2)), D((2,)), D((2 * len(SEEN) * max(DEPTH),)), D((2 * len(SEEN) * max(DEPTH),)), D((2, 2)), D((2,))]
    return pl.pallas_call(
        functools.partial(kernel_bc, cfg),
        out_shape=(jax.ShapeDtypeStruct((2 * nt,) + bu, F32), jax.ShapeDtypeStruct((2 * nt,) + bd, F32),
                   jax.ShapeDtypeStruct((8, 128), F32)),
        in_specs=[HBM] * 8, out_specs=(HBM, HBM, pl.BlockSpec(memory_space=pltpu.VMEM)),
        scratch_shapes=scratch,
        compiler_params=pltpu.CompilerParams(collective_id=0, has_side_effects=True, vmem_limit_bytes=VMEM_MAX),
        name="backward",
    )(u, ut, e, xt, z, w3p, w4r, w2r)


LAG = 2

def kernel_gather(cfg, su, sd, ou, od, lsem, rsem, ssem, dsem):
    nd, np_, ru, cu, rd = cfg
    pieces = 2 * np_
    me, core, bits = position()
    partner = flip(me, 1)
    barrier = pltpu.get_barrier_semaphore()
    for peer in (partner, flip(me, 2), flip(me, 4), flip(me, 8)):
        pl.semaphore_signal(barrier, inc=1, device_id=(peer,), device_id_type=MESH)
    pl.semaphore_wait(barrier, 4)

    def owner(kind, p):
        return 2 * relative(kind, p, bits) + core

    def block(kind, who, j, ref, local=False):
        w, k = lax.div(j, np_), lax.rem(j, np_)
        if kind == 0:
            row = 0 if local else pl.multiple_of(who * ru, 8)
            return ref.at[w, pl.ds(row, ru), pl.ds(pl.multiple_of(k * cu, 128), cu)]
        row = k * rd if local else who * (rd * np_) + k * rd
        return ref.at[w, pl.ds(pl.multiple_of(row, 8), rd), :]

    IN, O = (su, sd), (ou, od)
    own = [pltpu.make_async_copy(su, ou.at[:, pl.ds(pl.multiple_of(me * ru, 8), ru), :], lsem.at[0]),
           pltpu.make_async_copy(sd, od.at[:, pl.ds(pl.multiple_of(me * (rd * np_), 8), rd * np_), :], lsem.at[1])]

    def push(kind, p, j, dev, send, recv):
        who = owner(kind, p)
        src = block(kind, who, j, IN[kind], True) if p == 0 else block(kind, who, j, O[kind])
        pltpu.make_async_remote_copy(src_ref=src, dst_ref=block(kind, who, j, O[kind]), send_sem=send, recv_sem=recv,
                                     device_id=(dev,), device_id_type=MESH).start()

    def spread(kind, stage, j):
        dev = flip(me, 2 << ORDERS[kind][2 - stage])
        slot = lax.rem(j, 2 * LAG)
        for p in range(1 << stage):
            push(kind, p, j, dev, ssem.at[kind * 3 + stage], rsem.at[(kind * 3 + stage) * 2 * LAG + slot])

    def local(kind, ps, j):
        for p in ps:
            push(kind, p, j, partner, dsem.at[kind], dsem.at[2 + kind])

    def arrived(kind, stage, j):
        n = 1 << stage
        slot = lax.rem(j, 2 * LAG)
        size = O[kind].at[0, pl.ds(0, n * ru), pl.ds(0, cu)] if kind == 0 else O[kind].at[0, pl.ds(0, n * rd), :]
        sem = rsem.at[(kind * 3 + stage) * 2 * LAG + slot]
        pltpu.make_async_remote_copy(src_ref=size, dst_ref=size, send_sem=sem, recv_sem=sem, device_id=(me,), device_id_type=MESH).wait_recv()

    def step(s, _):
        for stage in (3, 2, 1, 0):
            j = s - stage * LAG
            @pl.when(jnp.logical_and(j >= 0, j < pieces))
            def _():
                for kind in range(2):
                    if stage:
                        arrived(kind, stage - 1, j)
                    if stage < 3:
                        spread(kind, stage, j)
                    local(kind, range((1 << stage) >> 1, 1 << stage), j)
        return 0
    for c in own:
        c.start()
    lax.fori_loop(0, pieces + 3 * LAG, step, 0)
    for c in own:
        c.wait()
    for kind in range(2):
        full = O[kind].at[0]
        rows = O[kind].shape[1] // 8
        pltpu.make_async_remote_copy(src_ref=full, dst_ref=full, send_sem=dsem.at[kind], recv_sem=dsem.at[2 + kind], device_id=(me,), device_id_type=MESH).wait()
        for stage in range(3):
            part = O[kind].at[0, pl.ds(0, rows << stage)]
            pltpu.make_async_remote_copy(src_ref=part, dst_ref=part, send_sem=ssem.at[kind * 3 + stage], recv_sem=dsem.at[2 + kind], device_id=(me,), device_id_type=MESH).wait_send()

def gather(su, sd, nd):
    _, ru, f = su.shape
    _, rf, d = sd.shape
    np_ = rf // 16
    cfg = (nd, np_, ru, f // np_, 16)
    D = pltpu.SemaphoreType.DMA
    anyspec = pl.BlockSpec(memory_space=pl.ANY)
    return pl.pallas_call(functools.partial(kernel_gather, cfg),
        out_shape=(jax.ShapeDtypeStruct((2, ru * nd, f), BF16), jax.ShapeDtypeStruct((2, rf * nd, d), BF16)),
        in_specs=[anyspec] * 2, out_specs=(anyspec,) * 2,
        scratch_shapes=[D((2,)), D((12 * LAG,)), D((6,)), D((4,))],
        compiler_params=pltpu.CompilerParams(collective_id=1, has_side_effects=True, vmem_limit_bytes=1024 * 1024),
        name="gather")(su, sd)


STEP = 20
BETA_ONE = 0.9
BETA_TWO = 0.95
EPSILON = 1e-8
NORM_EPS = 1e-6
CORR_ONE = 1.0 - BETA_ONE ** STEP
CORR_TWO = 1.0 - BETA_TWO ** STEP


def kernel_adam(cfg, sq_ref, hyper_ref, gu_hbm, gd_hbm, *refs):
    nd, nt = cfg
    states, outs, (nu_ref, nd_ref, norm_ref), (gbuf_u, gbuf_d, sbuf_u, sbuf_d, obuf_u, obuf_d, lsem, osem) = refs[:12], refs[12:24], refs[24:27], refs[27:]
    lanes, width = 128, 16
    per = lanes // width
    gbuf, sbuf, obuf, half = (gbuf_u, gbuf_d), (sbuf_u, sbuf_d), (obuf_u, obuf_d), (nu_ref, nd_ref)
    order = (2, 3, 1, 0)

    def loads(k):
        kind, layer = k % 2, k // 2
        src = (gu_hbm, gd_hbm)[kind].at[pl.ds((1 - layer) * nt, nt)]
        return [pltpu.make_async_copy(src, gbuf[kind].at[layer], lsem.at[k])] + [
            pltpu.make_async_copy(states[4 * f + k], sbuf[kind].at[layer, f], lsem.at[k]) for f in range(3)]

    def stores(k):
        kind, layer = k % 2, k // 2
        return [pltpu.make_async_copy(obuf[kind].at[layer, f], outs[4 * f + k], osem.at[k]) for f in range(3)]
    for k in order:
        for c in loads(k):
            c.start()
    norm = jnp.sqrt(jnp.sum(sq_ref[...], keepdims=True))
    norm_ref[...] = norm
    rate, clip = hyper_ref[0], hyper_ref[1]
    scale = jnp.minimum(1.0, clip / (norm + NORM_EPS))
    group = lax.broadcasted_iota(jnp.int32, (8, lanes), 1) // width

    def update(kind, layer, rows, grad):
        master, mom, vel = [sbuf[kind][layer, f, rows, :] for f in range(3)]
        scaled = scale * grad
        mom = BETA_ONE * mom + (1.0 - BETA_ONE) * scaled
        vel = BETA_TWO * vel + (1.0 - BETA_TWO) * scaled * scaled
        master = master - rate * (mom * (1.0 / CORR_ONE)) / (jnp.sqrt(vel * (1.0 / CORR_TWO)) + EPSILON)
        half[kind][layer, rows, :] = master.astype(BF16)
        for f, value in enumerate((master, mom, vel)):
            obuf[kind][layer, f, rows, :] = value

    for k in order:
        kind, layer = k % 2, k // 2
        for c in loads(k):
            c.wait()
        if kind == 0:
            def body(r, _):
                rows = pl.ds(pl.multiple_of(r * 8, 8), 8)
                cols = []
                for t in range(nd * nt // per):
                    acc = None
                    for s in range(per):
                        k_owner, j = divmod(per * t + s, nt)
                        src = gbuf_u[layer, j, rows, (k_owner // per) * lanes:(k_owner // per + 1) * lanes]
                        shift = (s - k_owner) % per * width
                        turned = pltpu.roll(src, shift, 1) if shift else src
                        acc = turned if acc is None else jnp.where(group == s, turned, acc)
                    cols.append(acc)
                update(0, layer, rows, jnp.concatenate(cols, axis=1))
                return 0
            lax.fori_loop(0, sbuf_u.shape[2] // 8, body, 0)
        else:
            def body(j, _):
                n = gbuf_d.shape[2]
                update(1, layer, pl.ds(pl.multiple_of(j * n, n), n), gbuf_d[layer, j])
                return 0
            lax.fori_loop(0, nt, body, 0)
        for c in stores(k):
            c.start()
    for k in order:
        for c in stores(k):
            c.wait()


def adam(sq, hyper, gu, gd, states, nd):
    nt = gu.shape[0] // 2
    up, down = states[0].shape, states[1].shape
    S, V, D = jax.ShapeDtypeStruct, pltpu.VMEM, pltpu.SemaphoreType.DMA
    vm = pl.BlockSpec(memory_space=pltpu.VMEM)
    return pl.pallas_call(
        functools.partial(kernel_adam, (nd, nt)),
        out_shape=tuple(S(s.shape, F32) for s in states) + (S((2,) + up, BF16), S((2,) + down, BF16), S((1, 1), F32)),
        in_specs=[vm, pl.BlockSpec(memory_space=pltpu.SMEM)] + [HBM] * 14, out_specs=(HBM,) * 12 + (vm,) * 3,
        scratch_shapes=[V((2, nt) + gu.shape[1:], F32), V((2, nt) + gd.shape[1:], F32), V((2, 3) + up, F32), V((2, 3) + down, F32),
                        V((2, 3) + up, F32), V((2, 3) + down, F32), D((4,)), D((4,))],
        compiler_params=pltpu.CompilerParams(vmem_limit_bytes=VMEM_MAX),
        name="adam")(sq, hyper, gu, gd, *states)


def solution(mesh):
    groups = mesh.shape["data"]
    rows_spec = P("data", None)
    full_spec = P(None, None)
    scalar_spec = P()

    def shard_body(act_in, grad_out, w_up1, w_down1, w_up2, w_down2, *rest):
        states, learn_rate, clip_norm = rest[:12], rest[12], rest[13]
        ff, d = w_down1.shape
        down1_tiles = w_down1.reshape(groups, -1, 16, d)
        down2_tiles = w_down2.reshape(groups, -1, 16, d)
        pre1, mid, mid_t, in_t, up2_tiles = forward_one(act_in, w_up1, w_up2, down1_tiles)
        grads_up, grads_down, sq = backward(mid, mid_t, grad_out, in_t, pre1, up2_tiles, down2_tiles, down1_tiles)
        *new_states, up_half, down_half, norm = adam(sq, jnp.stack([learn_rate, clip_norm]), grads_up, grads_down, states, groups)
        up_full, down_full = gather(up_half, down_half, groups)
        return (up_full[0], down_full[0], up_full[1], down_full[1], *new_states, norm.reshape(()))

    in_specs = (rows_spec, rows_spec) + (full_spec,) * 4 + (rows_spec,) * 12 + (scalar_spec, scalar_spec)
    out_specs = (full_spec,) * 4 + (rows_spec,) * 12 + (scalar_spec,)
    return jax.shard_map(shard_body, mesh=mesh, in_specs=in_specs, out_specs=out_specs, check_vma=False)
```

```python
import functools
import math
import jax
import jax.numpy as jnp
from jax import lax
from jax.experimental import pallas as pl
from jax.experimental.pallas import tpu as pltpu
from jax.sharding import PartitionSpec as P

ROOT_HALF = math.sqrt(0.5)
INV_ROOT_TAU = 1.0 / math.sqrt(2.0 * math.pi)
F32, BF16 = jnp.float32, jnp.bfloat16
HBM = pl.BlockSpec(memory_space=pltpu.HBM)
VMEM_MAX = 64 * 1024 * 1024 - 65536
BLOCKS = 8
RING = 6


def dot_nn(a, b):
    return lax.dot_general(a, b, (((1,), (0,)), ((), ())), preferred_element_type=F32)


def dot_nt(a, b):
    return lax.dot_general(a, b, (((1,), (1,)), ((), ())), preferred_element_type=F32)


def gelu(z):
    return z * (0.5 * (1.0 + lax.erf(z * ROOT_HALF)))


def at_most(j, bound):
    return jnp.minimum(j, bound)


def aligned(j, size):
    return pl.ds(pl.multiple_of(j * size, size), size)


def kernel_a(cfg, x_hbm, e_hbm, w1_hbm, w3_hbm, w2_hbm, z_hbm, ut_hbm, xt_hbm, et_hbm, w3t_hbm,
             xt, uacc, zout, w1t_v, w1_in, x_in, w1, w2, w2t, w3_in, w3_out, e_in, e_out, h0, h1,
             wsem, xsem, esem, vsem, zsem, osem):
    nt, nr, rb, ft, d, nd = cfg
    hb = (h0, h1)
    width = ft // nd

    def w1copy(q):
        slot = lax.rem(q, RING)
        return pltpu.make_async_copy(w1_hbm.at[:, aligned(q, ft)], w1_in.at[slot], wsem.at[slot])

    def xcopy(r):
        slot = lax.rem(r, RING)
        return pltpu.make_async_copy(x_hbm.at[aligned(r, rb), :], x_in.at[slot], xsem.at[slot])

    def w2copy(j):
        slot = lax.rem(j, 2)
        return pltpu.make_async_copy(w2_hbm.at[:, j], w2.at[slot], vsem.at[0, slot])

    def w3copy(j):
        slot = lax.rem(j, 2)
        return pltpu.make_async_copy(w3_hbm.at[:, aligned(j, ft)], w3_in.at[slot], vsem.at[1, slot])

    def w3store(j):
        slot = lax.rem(j, 2)
        return pltpu.make_async_copy(w3_out.at[slot], w3t_hbm.at[aligned(j, ft), :], osem.at[0, slot])

    def ecopy(r):
        slot = lax.rem(r, 2)
        return pltpu.make_async_copy(e_hbm.at[aligned(r, rb), :], e_in.at[slot], esem.at[slot])

    def estore(r):
        slot = lax.rem(r, 2)
        return pltpu.make_async_copy(e_out.at[slot], et_hbm.at[:, aligned(r, rb)], osem.at[1, slot])

    def zstore(j):
        slot = lax.rem(j, 2)
        return pltpu.make_async_copy(zout.at[slot], z_hbm.at[j], zsem.at[slot])

    for q in range(min(RING, nt)):
        w1copy(q).start()
    for r in range(min(RING, nr)):
        xcopy(r).start()
    for c in (w2copy(0), w3copy(0), ecopy(0)):
        c.start()

    def zero(r, _):
        uacc[:, aligned(r, rb)] = jnp.zeros((d, rb), F32)
        return 0
    lax.fori_loop(0, nr, zero, 0)

    def turn_w1(q, _):
        w1copy(q).wait()
        w1t_v[aligned(q, ft), :] = w1_in[lax.rem(q, RING)].T
        @pl.when(q + RING < nt)
        def _():
            w1copy(q + RING).start()
        return 0
    lax.fori_loop(0, nt, turn_w1, 0)

    def turn_x(r, _):
        xcopy(r).wait()
        xt[:, aligned(r, rb)] = x_in[lax.rem(r, RING)].T
        @pl.when(r + RING < nr)
        def _():
            xcopy(r + RING).start()
        return 0
    lax.fori_loop(0, nr, turn_x, 0)
    xt_store = pltpu.make_async_copy(xt, xt_hbm, osem.at[2, 0])
    xt_store.start()

    def pick_w1(j, slot):
        for k in range(nd):
            w1[slot, k * width:(k + 1) * width, :] = w1t_v[aligned(k * nt + j, width), :]
    pick_w1(0, 0)

    def tile(j, _):
        slot = lax.rem(j, 2)
        nslot = 1 - slot
        @pl.when(j >= 2)
        def _():
            zstore(j - 2).wait()
            w3store(j - 2).wait()
        @pl.when(jnp.logical_and(j >= 2, j < nr + 2))
        def _():
            estore(j - 2).wait()
        w2copy(j).wait()
        w3copy(j).wait()
        @pl.when(j < nr)
        def _():
            ecopy(j).wait()
        @pl.when(j + 1 < nt)
        def _():
            w2copy(j + 1).start()
            w3copy(j + 1).start()
        @pl.when(j + 1 < min(nr, nt))
        def _():
            ecopy(j + 1).start()

        def cols(r):
            return pl.ds(r * rb, rb)
        def front(r):
            zout[slot, :, cols(r)] = dot_nn(w1[slot], xt[:, cols(r)])
        def middle(r):
            hb[r % 2][...] = gelu(zout[slot, :, cols(r)]).astype(BF16)
        def back(r):
            uacc[:, cols(r)] += dot_nn(w2t[...], hb[r % 2][...])
        front(0)
        w2t[...] = w2[slot].reshape(ft, d).T
        for r in range(nr):
            middle(r)
            if r + 1 < nr:
                front(r + 1)
            if r >= 1:
                back(r - 1)
            if r == 1:
                pick_w1(at_most(j + 1, nt - 1), nslot)
            if r == 3:
                w3_out[slot] = w3_in[slot].T
            if r == 5:
                e_out[slot] = e_in[slot].T
        back(nr - 1)
        zstore(j).start()
        w3store(j).start()
        @pl.when(j < nr)
        def _():
            estore(j).start()
        return 0
    lax.fori_loop(0, nt, tile, 0)
    xt_store.wait()

    def finish(r, _):
        xt[:, aligned(r, rb)] = uacc[:, aligned(r, rb)].astype(BF16)
        return 0
    lax.fori_loop(0, nr, finish, 0)
    ut_store = pltpu.make_async_copy(xt, ut_hbm, osem.at[2, 1])
    ut_store.start()
    for j in (nt - 2, nt - 1):
        zstore(j).wait()
        w3store(j).wait()
        if j < nr:
            estore(j).wait()
    for r in range(nt, nr):
        ecopy(r).start()
        ecopy(r).wait()
        e_out[r % 2] = e_in[r % 2].T
        estore(r).start()
        estore(r).wait()
    ut_store.wait()


def forward_one(x, e, w1, w3, w2r):
    t, d = x.shape
    nd, nt, rows2, _ = w2r.shape
    ft, nr = nd * rows2, BLOCKS
    rb = t // nr
    V, D = pltpu.VMEM, pltpu.SemaphoreType.DMA
    S = jax.ShapeDtypeStruct
    return pl.pallas_call(
        functools.partial(kernel_a, (nt, nr, rb, ft, d, nd)),
        out_shape=(S((nt, ft, t), F32), S((d, t), BF16), S((d, t), BF16), S((d, t), BF16), S((nt * ft, d), BF16)),
        in_specs=[HBM] * 5, out_specs=(HBM,) * 5,
        scratch_shapes=[
            V((d, t), BF16), V((d, t), F32), V((2, ft, t), F32), V((nt * ft, d), BF16), V((RING, d, ft), BF16), V((RING, rb, d), BF16),
            V((2, ft, d), BF16), V((2, nd, rows2, d), BF16), V((d, ft), BF16), V((2, d, ft), BF16), V((2, ft, d), BF16),
            V((2, rb, d), BF16), V((2, d, rb), BF16), V((ft, rb), BF16), V((ft, rb), BF16),
            D((RING,)), D((RING,)), D((2,)), D((2, 2)), D((2,)), D((3, 2))],
        compiler_params=pltpu.CompilerParams(vmem_limit_bytes=VMEM_MAX),
        name="forward_one",
    )(x, e, w1, w3, w2r)


MESH = pl.DeviceIdType.MESH

def gelu_pair(pre):
    normal_cdf = 0.5 * (1.0 + lax.erf(pre * ROOT_HALF))
    density = jnp.exp(-0.5 * pre * pre) * INV_ROOT_TAU
    return pre * normal_cdf, normal_cdf + pre * density

def flip(value, step):
    return value + step * (1 - 2 * lax.rem(lax.div(value, step), 2))

def relative(kind, p, bits):
    out = 0
    for place, axis in enumerate(reversed(ORDERS[kind])):
        out = out + (1 - bits[axis] if (p >> place) & 1 else bits[axis]) * (1 << axis)
    return out


def position():
    me = lax.axis_index("data")
    chip = lax.div(me, 2)
    return me, lax.rem(me, 2), [lax.rem(lax.div(chip, 1 << k), 2) for k in range(3)]


ORDERS = ((0, 2, 1), (1, 2, 0))
PARTS = 8
BEGUN = 2
TURN = 128
SEEN = (3, 5, 7, 8)
DEPTH = (2, 4, 4, 2)
LAST = len(SEEN) - 1
ACCS = 5

def kernel_bc(cfg, ut_hbm, et_hbm, xt_hbm, z_hbm, w3_hbm, w4_hbm, w2_hbm,
              gu_hbm, gd_hbm, nrm_ref,
              act, side, euacc, wa, wb, wat, zb0, zb1, eb0, eb1, hb0, hb1, qb0, qb1,
              gu, gt, gd, r0u, r0d, au, ad, r1u, r1d, r2u, r2d, r3u, r3d, fu, fd, nu, nd_acc, nsend, nrecv,
              insem, wsem, zsem, ssem, rsem, fsem, nsem):
    nt, nr, rb, ft, d, nd = cfg
    total = 2 * nt
    me, core, bits = position()
    partner = flip(me, 1)
    zb, eb, hb, qb = (zb0, zb1), (eb0, eb1), (hb0, hb1), (qb0, qb1)
    G, R, ACC, FIN, NRM, OUT = (gu, gd), ((r0u, r1u, r2u, r3u), (r0d, r1d, r2d, r3d)), (au, ad), (fu, fd), (nu, nd_acc), (gu_hbm, gd_hbm)

    loads = [pltpu.make_async_copy(ut_hbm, act, insem.at[0]), pltpu.make_async_copy(et_hbm, side, insem.at[1])]
    for c in loads:
        c.start()

    def wcopies(j, slot, back):
        second = w2_hbm if back else w4_hbm
        cps = [pltpu.make_async_copy(second.at[:, j], wb.at[slot], wsem.at[1, slot])]
        if not back:
            cps.append(pltpu.make_async_copy(w3_hbm.at[:, j], wa.at[slot], wsem.at[0, slot]))
        return cps
    for c in wcopies(0, 0, False):
        c.start()

    barrier = pltpu.get_barrier_semaphore()
    for k in range(1, nd):
        pl.semaphore_signal(barrier, inc=1, device_id=(lax.rem(me + k, nd),), device_id_type=MESH)
    pl.semaphore_wait(barrier, nd - 1)

    nu[...] = jnp.zeros_like(nu)
    nd_acc[...] = jnp.zeros_like(nd_acc)
    gt[1] = jnp.zeros_like(gt[1])
    def zero(r, _):
        euacc[:, aligned(r, rb)] = jnp.zeros((d, rb), F32)
        return 0
    lax.fori_loop(0, nr, zero, 0)

    def owner_chip(kind, p):
        return relative(kind, p, bits)

    def send(kind, stage, j):
        depth = R[kind][stage].shape[0]
        slot = lax.rem(j, depth)
        sem = (kind * len(SEEN) + stage) * max(DEPTH) + slot
        dst = R[kind][stage].at[slot]
        if stage == 0:
            src, dev = G[kind].at[lax.rem(j, G[kind].shape[0]), :, 1 - core], partner
        else:
            lo = PARTS >> stage
            src, dev = ACC[kind].at[lax.rem(j, ACCS), pl.ds(lo, lo)], flip(me, 2 << ORDERS[kind][stage - 1])
        return pltpu.make_async_remote_copy(src_ref=src, dst_ref=dst, send_sem=ssem.at[sem], recv_sem=rsem.at[sem],
                                            device_id=(dev,), device_id_type=MESH)

    def final_copy(kind, j):
        slot = lax.rem(j, 2)
        return pltpu.make_async_copy(FIN[kind].at[slot], OUT[kind].at[j], fsem.at[kind, slot])

    def absorb(stage, j):
        place = lax.rem(j, ACCS)
        for kind in range(2):
            send(kind, stage, j).wait()
            slot = lax.rem(j, R[kind][stage].shape[0])
            got, acc = R[kind][stage], ACC[kind]
            if stage == 0:
                for p in range(PARTS):
                    oc = owner_chip(kind, p)
                    acc[place, p] = G[kind][lax.rem(j, G[kind].shape[0]), oc, core] + got[slot, oc]
            elif stage < LAST:
                keep = pl.ds(0, PARTS >> stage)
                acc[place, keep] += got[slot]
            else:
                @pl.when(j >= 2)
                def _():
                    final_copy(kind, j - 2).wait()
                f = (acc[place, 0] + got[slot, 0]) * (1.0 / nd)
                FIN[kind][lax.rem(j, 2)] = f
                NRM[kind][...] += f * f
        for kind in range(2):
            (send(kind, stage + 1, j) if stage < LAST else final_copy(kind, j)).start()

    def comm(step):
        def when_valid(j, fn):
            @pl.when(jnp.logical_and(j >= 0, j < total))
            def _():
                fn()
        for stage in reversed(range(len(SEEN))):
            when_valid(step - SEEN[stage], functools.partial(absorb, stage, step - SEEN[stage]))
        def start():
            for kind in range(2):
                send(kind, 0, step - BEGUN).start()
        when_valid(step - BEGUN, start)

    def cols(r):
        return pl.ds(r * rb, rb)

    def turn(step, part):
        slot = lax.rem(step + 1, 2)
        lanes = pl.ds(part * TURN, TURN)
        gd[slot, :, :, :, lanes] = gt[slot, lanes, :].T.reshape(gd.shape[1:-1] + (TURN,))

    def add_grads(step, r, up, down_t):
        up = up.reshape(gu.shape[1:])
        three, two = lax.rem(step, gu.shape[0]), lax.rem(step, 2)
        gu[three] = up if r == 0 else gu[three] + up
        gt[two] = down_t if r == 0 else gt[two] + down_t

    def gates(r, pre):
        h, der = gelu_pair(pre)
        hb[r % 2][...] = h.astype(BF16)
        qb[r % 2][...] = (eb[r % 2][...].astype(F32) * der).astype(BF16)

    def pipeline(step, front, middle, back):
        front(0)
        for r in range(nr):
            middle(r)
            if r + 1 < nr:
                front(r + 1)
            if r >= 1:
                back(r - 1)
            if r < d // TURN:
                turn(step, r)
        back(nr - 1)

    for c in loads:
        c.wait()

    def tile_b(j, _):
        slot = lax.rem(j, 2)
        comm(j)
        for c in wcopies(j, slot, False):
            c.wait()
        @pl.when(j + 1 < nt)
        def _():
            for c in wcopies(j + 1, 1 - slot, False):
                c.start()
        def front(r):
            zb[r % 2][...] = dot_nn(wa[slot].reshape(ft, d), act[:, cols(r)])
            eb[r % 2][...] = dot_nn(wb[slot].reshape(ft, d), side[:, cols(r)]).astype(BF16)
            if r == 0:
                wat[...] = wa[slot].reshape(ft, d).T
        def middle(r):
            gates(r, zb[r % 2][...])
        def back(r):
            q = qb[r % 2][...]
            euacc[:, cols(r)] += dot_nn(wat[...], q)
            add_grads(j, r, dot_nt(act[:, cols(r)], q), dot_nt(side[:, cols(r)], hb[r % 2][...]))
        pipeline(j, front, middle, back)
        return 0
    lax.fori_loop(0, nt, tile_b, 0)

    xt_in = pltpu.make_async_copy(xt_hbm, side, insem.at[1])
    xt_in.start()
    for c in wcopies(0, nt % 2, True):
        c.start()
    def cast(r, _):
        act[:, aligned(r, rb)] = euacc[:, aligned(r, rb)].astype(BF16)
        return 0
    lax.fori_loop(0, nr, cast, 0)
    def zcopy(j, slot):
        return pltpu.make_async_copy(z_hbm.at[j], euacc.at[aligned(slot, ft), :], zsem.at[slot])
    zcopy(0, nt % 2).start()
    xt_in.wait()

    def tile_c(step, _):
        j = step - nt
        slot = lax.rem(step, 2)
        comm(step)
        for c in wcopies(j, slot, True):
            c.wait()
        zcopy(j, slot).wait()
        @pl.when(j + 1 < nt)
        def _():
            for c in wcopies(j + 1, 1 - slot, True):
                c.start()
            zcopy(j + 1, 1 - slot).start()
        def front(r):
            eb[r % 2][...] = dot_nn(wb[slot].reshape(ft, d), act[:, cols(r)]).astype(BF16)
        def middle(r):
            gates(r, euacc[aligned(slot, ft), cols(r)])
        def back(r):
            add_grads(step, r, dot_nt(side[:, cols(r)], qb[r % 2][...]), dot_nt(act[:, cols(r)], hb[r % 2][...]))
        pipeline(step, front, middle, back)
        return 0
    lax.fori_loop(nt, total, tile_c, 0)

    def drain(step, _):
        comm(step)
        @pl.when(step == total)
        def _():
            for part in range(d // TURN):
                turn(step, part)
        return 0
    lax.fori_loop(total, total + SEEN[LAST], drain, 0)
    for kind in range(2):
        for j in (total - 2, total - 1):
            final_copy(kind, j).wait()

    part = jnp.zeros((8, 128), F32)
    for ref in (nu, nd_acc):
        rows, cols = ref.shape
        for a in range(rows // 8):
            for b in range(cols // 128):
                part = part + ref[8 * a:8 * a + 8, 128 * b:128 * b + 128]
    nsend[...] = part
    nrecv[me] = part
    for k in range(1, nd):
        pltpu.make_async_remote_copy(src_ref=nsend, dst_ref=nrecv.at[me], send_sem=nsem.at[0], recv_sem=nsem.at[1],
                                     device_id=(lax.rem(me + k, nd),), device_id_type=MESH).start()
    others = nrecv.at[pl.ds(0, nd - 1)]
    pltpu.make_async_remote_copy(src_ref=others, dst_ref=others, send_sem=nsem.at[0], recv_sem=nsem.at[1],
                                 device_id=(me,), device_id_type=MESH).wait()
    total_sq = nrecv[0]
    for k in range(1, nd):
        total_sq = total_sq + nrecv[k]
    nrm_ref[...] = total_sq

def backward(ut, et, xt, z, w3r, w4r, w2r):
    d, t = ut.shape
    nd, nt, rows2, _ = w4r.shape
    ft, nr = nd * rows2, BLOCKS
    rb = t // nr
    bu, bd = (d // nd, ft), (rows2, d)
    V, D = pltpu.VMEM, pltpu.SemaphoreType.DMA
    S = jax.ShapeDtypeStruct
    scratch = [V((d, t), BF16)] * 2 + [V((d, t), F32)] + [V((2, nd, rows2, d), BF16)] * 2 + [V((d, ft), BF16)]
    scratch += [V((ft, rb), F32)] * 2 + [V((ft, rb), BF16)] * 6
    scratch += [V((3, PARTS, 2) + bu, F32), V((2, d, ft), F32), V((2, PARTS, 2) + bd, F32)]
    for n, c in ((DEPTH[0], PARTS), (ACCS, PARTS)) + tuple((DEPTH[k], PARTS >> k) for k in range(1, LAST + 1)):
        scratch += [V((n, c) + bu, F32), V((n, c) + bd, F32)]
    scratch += [V((2,) + bu, F32), V((2,) + bd, F32), V(bu, F32), V(bd, F32), V((8, 128), F32), V((nd, 8, 128), F32)]
    flags = 2 * len(SEEN) * max(DEPTH)
    scratch += [D((2,)), D((2, 2)), D((2,)), D((flags,)), D((flags,)), D((2, 2)), D((2,))]
    return pl.pallas_call(
        functools.partial(kernel_bc, (nt, nr, rb, ft, d, nd)),
        out_shape=(S((2 * nt,) + bu, F32), S((2 * nt,) + bd, F32), S((8, 128), F32)),
        in_specs=[HBM] * 7, out_specs=(HBM, HBM, pl.BlockSpec(memory_space=pltpu.VMEM)),
        scratch_shapes=scratch,
        compiler_params=pltpu.CompilerParams(collective_id=0, has_side_effects=True, vmem_limit_bytes=VMEM_MAX),
        name="backward",
    )(ut, et, xt, z, w3r, w4r, w2r)


LAG = 2

def kernel_gather(cfg, su, sd, ou, od, lsem, rsem, ssem, dsem):
    nd, np_, ru, cu, rd = cfg
    pieces = 2 * np_
    me, core, bits = position()
    partner = flip(me, 1)
    barrier = pltpu.get_barrier_semaphore()
    for peer in (partner, flip(me, 2), flip(me, 4), flip(me, 8)):
        pl.semaphore_signal(barrier, inc=1, device_id=(peer,), device_id_type=MESH)
    pl.semaphore_wait(barrier, 4)

    def owner(kind, p):
        return 2 * relative(kind, p, bits) + core

    def block(kind, who, j, ref, local=False):
        w, k = lax.div(j, np_), lax.rem(j, np_)
        if kind == 0:
            row = 0 if local else pl.multiple_of(who * ru, 8)
            return ref.at[w, pl.ds(row, ru), pl.ds(pl.multiple_of(k * cu, 128), cu)]
        row = k * rd if local else who * (rd * np_) + k * rd
        return ref.at[w, pl.ds(pl.multiple_of(row, 8), rd), :]

    IN, O = (su, sd), (ou, od)
    own = [pltpu.make_async_copy(su, ou.at[:, pl.ds(pl.multiple_of(me * ru, 8), ru), :], lsem.at[0]),
           pltpu.make_async_copy(sd, od.at[:, pl.ds(pl.multiple_of(me * (rd * np_), 8), rd * np_), :], lsem.at[1])]

    def push(kind, p, j, dev, send, recv):
        who = owner(kind, p)
        src = block(kind, who, j, IN[kind], True) if p == 0 else block(kind, who, j, O[kind])
        pltpu.make_async_remote_copy(src_ref=src, dst_ref=block(kind, who, j, O[kind]), send_sem=send, recv_sem=recv,
                                     device_id=(dev,), device_id_type=MESH).start()

    def spread(kind, stage, j):
        dev = flip(me, 2 << ORDERS[kind][2 - stage])
        slot = lax.rem(j, 2 * LAG)
        for p in range(1 << stage):
            push(kind, p, j, dev, ssem.at[kind * 3 + stage], rsem.at[(kind * 3 + stage) * 2 * LAG + slot])

    def local(kind, ps, j):
        for p in ps:
            push(kind, p, j, partner, dsem.at[kind], dsem.at[2 + kind])

    def arrived(kind, stage, j):
        n = 1 << stage
        slot = lax.rem(j, 2 * LAG)
        size = O[kind].at[0, pl.ds(0, n * ru), pl.ds(0, cu)] if kind == 0 else O[kind].at[0, pl.ds(0, n * rd), :]
        sem = rsem.at[(kind * 3 + stage) * 2 * LAG + slot]
        pltpu.make_async_remote_copy(src_ref=size, dst_ref=size, send_sem=sem, recv_sem=sem, device_id=(me,), device_id_type=MESH).wait_recv()

    def step(s, _):
        for stage in (3, 2, 1, 0):
            j = s - stage * LAG
            @pl.when(jnp.logical_and(j >= 0, j < pieces))
            def _():
                for kind in range(2):
                    if stage:
                        arrived(kind, stage - 1, j)
                    if stage < 3:
                        spread(kind, stage, j)
                    local(kind, range((1 << stage) >> 1, 1 << stage), j)
        return 0
    for c in own:
        c.start()
    lax.fori_loop(0, pieces + 3 * LAG, step, 0)
    for c in own:
        c.wait()
    for kind in range(2):
        full = O[kind].at[0]
        rows = O[kind].shape[1] // 8
        pltpu.make_async_remote_copy(src_ref=full, dst_ref=full, send_sem=dsem.at[kind], recv_sem=dsem.at[2 + kind], device_id=(me,), device_id_type=MESH).wait()
        for stage in range(3):
            part = O[kind].at[0, pl.ds(0, rows << stage)]
            pltpu.make_async_remote_copy(src_ref=part, dst_ref=part, send_sem=ssem.at[kind * 3 + stage], recv_sem=dsem.at[2 + kind], device_id=(me,), device_id_type=MESH).wait_send()

def gather(su, sd, nd):
    _, ru, f = su.shape
    _, rf, d = sd.shape
    np_ = rf // 16
    cfg = (nd, np_, ru, f // np_, 16)
    D = pltpu.SemaphoreType.DMA
    anyspec = pl.BlockSpec(memory_space=pl.ANY)
    return pl.pallas_call(functools.partial(kernel_gather, cfg),
        out_shape=(jax.ShapeDtypeStruct((2, ru * nd, f), BF16), jax.ShapeDtypeStruct((2, rf * nd, d), BF16)),
        in_specs=[anyspec] * 2, out_specs=(anyspec,) * 2,
        scratch_shapes=[D((2,)), D((12 * LAG,)), D((6,)), D((4,))],
        compiler_params=pltpu.CompilerParams(collective_id=1, has_side_effects=True, vmem_limit_bytes=1024 * 1024),
        name="gather")(su, sd)


STEP = 20
BETA_ONE = 0.9
BETA_TWO = 0.95
EPSILON = 1e-8
NORM_EPS = 1e-6
CORR_ONE = 1.0 - BETA_ONE ** STEP
CORR_TWO = 1.0 - BETA_TWO ** STEP


def kernel_adam(cfg, sq_ref, hyper_ref, gu_hbm, gd_hbm, *refs):
    nd, nt = cfg
    states, outs, (nu_ref, nd_ref, norm_ref), (gbuf_u, gbuf_d, sbuf_u, sbuf_d, obuf_u, obuf_d, lsem, osem) = refs[:12], refs[12:24], refs[24:27], refs[27:]
    lanes, width = 128, 16
    per = lanes // width
    gbuf, sbuf, obuf, half = (gbuf_u, gbuf_d), (sbuf_u, sbuf_d), (obuf_u, obuf_d), (nu_ref, nd_ref)
    order = (2, 3, 1, 0)

    def loads(k):
        kind, layer = k % 2, k // 2
        src = (gu_hbm, gd_hbm)[kind].at[pl.ds((1 - layer) * nt, nt)]
        return [pltpu.make_async_copy(src, gbuf[kind].at[layer], lsem.at[k])] + [
            pltpu.make_async_copy(states[4 * f + k], sbuf[kind].at[layer, f], lsem.at[k]) for f in range(3)]

    def stores(k):
        kind, layer = k % 2, k // 2
        return [pltpu.make_async_copy(obuf[kind].at[layer, f], outs[4 * f + k], osem.at[k]) for f in range(3)]
    for k in order:
        for c in loads(k):
            c.start()
    norm = jnp.sqrt(jnp.sum(sq_ref[...], keepdims=True))
    norm_ref[...] = norm
    rate, clip = hyper_ref[0], hyper_ref[1]
    scale = jnp.minimum(1.0, clip / (norm + NORM_EPS))
    group = lax.broadcasted_iota(jnp.int32, (8, lanes), 1) // width

    def update(kind, layer, rows, grad):
        master, mom, vel = [sbuf[kind][layer, f, rows, :] for f in range(3)]
        scaled = scale * grad
        mom = BETA_ONE * mom + (1.0 - BETA_ONE) * scaled
        vel = BETA_TWO * vel + (1.0 - BETA_TWO) * scaled * scaled
        master = master - rate * (mom * (1.0 / CORR_ONE)) / (jnp.sqrt(vel * (1.0 / CORR_TWO)) + EPSILON)
        half[kind][layer, rows, :] = master.astype(BF16)
        for f, value in enumerate((master, mom, vel)):
            obuf[kind][layer, f, rows, :] = value

    for k in order:
        kind, layer = k % 2, k // 2
        for c in loads(k):
            c.wait()
        if kind == 0:
            def body(r, _):
                rows = pl.ds(pl.multiple_of(r * 8, 8), 8)
                cols = []
                for t in range(nd * nt // per):
                    acc = None
                    for s in range(per):
                        k_owner, j = divmod(per * t + s, nt)
                        src = gbuf_u[layer, j, rows, (k_owner // per) * lanes:(k_owner // per + 1) * lanes]
                        shift = (s - k_owner) % per * width
                        turned = pltpu.roll(src, shift, 1) if shift else src
                        acc = turned if acc is None else jnp.where(group == s, turned, acc)
                    cols.append(acc)
                update(0, layer, rows, jnp.concatenate(cols, axis=1))
                return 0
            lax.fori_loop(0, sbuf_u.shape[2] // 8, body, 0)
        else:
            def body(j, _):
                n = gbuf_d.shape[2]
                update(1, layer, pl.ds(pl.multiple_of(j * n, n), n), gbuf_d[layer, j])
                return 0
            lax.fori_loop(0, nt, body, 0)
        for c in stores(k):
            c.start()
    for k in order:
        for c in stores(k):
            c.wait()


def adam(sq, hyper, gu, gd, states, nd):
    nt = gu.shape[0] // 2
    up, down = states[0].shape, states[1].shape
    S, V, D = jax.ShapeDtypeStruct, pltpu.VMEM, pltpu.SemaphoreType.DMA
    vm = pl.BlockSpec(memory_space=pltpu.VMEM)
    return pl.pallas_call(
        functools.partial(kernel_adam, (nd, nt)),
        out_shape=tuple(S(s.shape, F32) for s in states) + (S((2,) + up, BF16), S((2,) + down, BF16), S((1, 1), F32)),
        in_specs=[vm, pl.BlockSpec(memory_space=pltpu.SMEM)] + [HBM] * 14, out_specs=(HBM,) * 12 + (vm,) * 3,
        scratch_shapes=[V((2, nt) + gu.shape[1:], F32), V((2, nt) + gd.shape[1:], F32), V((2, 3) + up, F32), V((2, 3) + down, F32),
                        V((2, 3) + up, F32), V((2, 3) + down, F32), D((4,)), D((4,))],
        compiler_params=pltpu.CompilerParams(vmem_limit_bytes=VMEM_MAX),
        name="adam")(sq, hyper, gu, gd, *states)


def solution(mesh):
    groups = mesh.shape["data"]
    rows_spec = P("data", None)
    full_spec = P(None, None)
    scalar_spec = P()

    def shard_body(act_in, grad_out, w_up1, w_down1, w_up2, w_down2, *rest):
        states, learn_rate, clip_norm = rest[:12], rest[12], rest[13]
        ff, d = w_down1.shape
        down1_tiles = w_down1.reshape(groups, -1, 16, d)
        down2_tiles = w_down2.reshape(groups, -1, 16, d)
        pre1, mid_t, in_t, grad_t, up2_t = forward_one(act_in, grad_out, w_up1, w_up2, down1_tiles)
        up2_tiles = up2_t.reshape(down1_tiles.shape)
        grads_up, grads_down, sq = backward(mid_t, grad_t, in_t, pre1, up2_tiles, down2_tiles, down1_tiles)
        *new_states, up_half, down_half, norm = adam(sq, jnp.stack([learn_rate, clip_norm]), grads_up, grads_down, states, groups)
        up_full, down_full = gather(up_half, down_half, groups)
        return (up_full[0], down_full[0], up_full[1], down_full[1], *new_states, norm.reshape(()))

    in_specs = (rows_spec, rows_spec) + (full_spec,) * 4 + (rows_spec,) * 12 + (scalar_spec, scalar_spec)
    out_specs = (full_spec,) * 4 + (rows_spec,) * 12 + (scalar_spec,)
    return jax.shard_map(shard_body, mesh=mesh, in_specs=in_specs, out_specs=out_specs, check_vma=False)
```

```python
import functools
import math
import jax
import jax.numpy as jnp
from jax import lax
from jax.experimental import pallas as pl
from jax.experimental.pallas import tpu as pltpu
from jax.sharding import PartitionSpec as P

ROOT_HALF = math.sqrt(0.5)
INV_ROOT_TAU = 1.0 / math.sqrt(2.0 * math.pi)
F32, BF16 = jnp.float32, jnp.bfloat16
HBM = pl.BlockSpec(memory_space=pltpu.HBM)
VMEM_MAX = 64 * 1024 * 1024 - 65536
BLOCKS = 8
TURNS = 8
RING = 6


def dot_nn(a, b):
    return lax.dot_general(a, b, (((1,), (0,)), ((), ())), preferred_element_type=F32)


def dot_nt(a, b):
    return lax.dot_general(a, b, (((1,), (1,)), ((), ())), preferred_element_type=F32)


def gelu(z):
    return z * (0.5 * (1.0 + lax.erf(z * ROOT_HALF)))


def at_most(j, bound):
    return jnp.minimum(j, bound)


def aligned(j, size):
    return pl.ds(pl.multiple_of(j * size, size), size)


def kernel_a(cfg, x_hbm, e_hbm, w1_hbm, w3_hbm, w2_hbm, z_hbm, ut_hbm, xt_hbm, et_hbm, w3t_hbm,
             xt, uacc, zout, w1t_v, w1_in, x_in, w1, w2, w2t, w3_in, w3_out, e_in, e_out, h0, h1,
             wsem, xsem, esem, vsem, zsem, osem):
    nt, nr, rb, tr, tb, ft, d, nd = cfg
    hb = (h0, h1)
    width = ft // nd

    def w1copy(q):
        slot = lax.rem(q, RING)
        return pltpu.make_async_copy(w1_hbm.at[:, aligned(q, ft)], w1_in.at[slot], wsem.at[slot])

    def xcopy(r):
        slot = lax.rem(r, RING)
        return pltpu.make_async_copy(x_hbm.at[aligned(r, tb), :], x_in.at[slot], xsem.at[slot])

    def w2copy(j):
        slot = lax.rem(j, 2)
        return pltpu.make_async_copy(w2_hbm.at[:, j], w2.at[slot], vsem.at[0, slot])

    def w3copy(j):
        slot = lax.rem(j, 2)
        return pltpu.make_async_copy(w3_hbm.at[:, aligned(j, ft)], w3_in.at[slot], vsem.at[1, slot])

    def w3store(j):
        slot = lax.rem(j, 2)
        return pltpu.make_async_copy(w3_out.at[slot], w3t_hbm.at[aligned(j, ft), :], osem.at[0, slot])

    def ecopy(r):
        slot = lax.rem(r, 2)
        return pltpu.make_async_copy(e_hbm.at[aligned(r, tb), :], e_in.at[slot], esem.at[slot])

    def estore(r):
        slot = lax.rem(r, 2)
        return pltpu.make_async_copy(e_out.at[slot], et_hbm.at[:, aligned(r, tb)], osem.at[1, slot])

    def zstore(j):
        slot = lax.rem(j, 2)
        return pltpu.make_async_copy(zout.at[slot], z_hbm.at[j], zsem.at[slot])

    for q in range(min(RING, nt)):
        w1copy(q).start()
    for r in range(min(RING, tr)):
        xcopy(r).start()
    for c in (w2copy(0), w3copy(0), ecopy(0)):
        c.start()

    def zero(r, _):
        uacc[:, aligned(r, rb)] = jnp.zeros((d, rb), F32)
        return 0
    lax.fori_loop(0, nr, zero, 0)

    def turn_w1(q, _):
        w1copy(q).wait()
        w1t_v[aligned(q, ft), :] = w1_in[lax.rem(q, RING)].T
        @pl.when(q + RING < nt)
        def _():
            w1copy(q + RING).start()
        return 0
    lax.fori_loop(0, nt, turn_w1, 0)

    def turn_x(r, _):
        xcopy(r).wait()
        xt[:, aligned(r, tb)] = x_in[lax.rem(r, RING)].T
        @pl.when(r + RING < tr)
        def _():
            xcopy(r + RING).start()
        return 0
    lax.fori_loop(0, tr, turn_x, 0)
    xt_store = pltpu.make_async_copy(xt, xt_hbm, osem.at[2, 0])
    xt_store.start()

    def pick_w1(j, slot):
        for k in range(nd):
            w1[slot, k * width:(k + 1) * width, :] = w1t_v[aligned(k * nt + j, width), :]
    pick_w1(0, 0)

    def tile(j, _):
        slot = lax.rem(j, 2)
        nslot = 1 - slot
        @pl.when(j >= 2)
        def _():
            zstore(j - 2).wait()
            w3store(j - 2).wait()
        @pl.when(jnp.logical_and(j >= 2, j < tr + 2))
        def _():
            estore(j - 2).wait()
        w2copy(j).wait()
        w3copy(j).wait()
        @pl.when(j < tr)
        def _():
            ecopy(j).wait()
        @pl.when(j + 1 < nt)
        def _():
            w2copy(j + 1).start()
            w3copy(j + 1).start()
        @pl.when(j + 1 < min(tr, nt))
        def _():
            ecopy(j + 1).start()

        def cols(r):
            return pl.ds(r * rb, rb)
        def front(r):
            zout[slot, :, cols(r)] = dot_nn(w1[slot], xt[:, cols(r)])
        def middle(r):
            hb[r % 2][...] = gelu(zout[slot, :, cols(r)]).astype(BF16)
        def back(r):
            uacc[:, cols(r)] += dot_nn(w2t[...], hb[r % 2][...])
        front(0)
        w2t[...] = w2[slot].reshape(ft, d).T
        for r in range(nr):
            middle(r)
            if r + 1 < nr:
                front(r + 1)
            if r >= 1:
                back(r - 1)
            if r == 0:
                pick_w1(at_most(j + 1, nt - 1), nslot)
            if r == 1:
                w3_out[slot] = w3_in[slot].T
            if r == nr - 2:
                e_out[slot] = e_in[slot].T
        back(nr - 1)
        zstore(j).start()
        w3store(j).start()
        @pl.when(j < tr)
        def _():
            estore(j).start()
        return 0
    lax.fori_loop(0, nt, tile, 0)
    xt_store.wait()

    def finish(r, _):
        xt[:, aligned(r, rb)] = uacc[:, aligned(r, rb)].astype(BF16)
        return 0
    lax.fori_loop(0, nr, finish, 0)
    ut_store = pltpu.make_async_copy(xt, ut_hbm, osem.at[2, 1])
    ut_store.start()
    for j in (nt - 2, nt - 1):
        zstore(j).wait()
        w3store(j).wait()
        if j < tr:
            estore(j).wait()
    for r in range(nt, tr):
        ecopy(r).start()
        ecopy(r).wait()
        e_out[r % 2] = e_in[r % 2].T
        estore(r).start()
        estore(r).wait()
    ut_store.wait()


def forward_one(x, e, w1, w3, w2r):
    t, d = x.shape
    nd, nt, rows2, _ = w2r.shape
    ft, nr, tr = nd * rows2, BLOCKS, TURNS
    rb, tb = t // nr, t // tr
    V, D = pltpu.VMEM, pltpu.SemaphoreType.DMA
    S = jax.ShapeDtypeStruct
    return pl.pallas_call(
        functools.partial(kernel_a, (nt, nr, rb, tr, tb, ft, d, nd)),
        out_shape=(S((nt, ft, t), F32), S((d, t), BF16), S((d, t), BF16), S((d, t), BF16), S((nt * ft, d), BF16)),
        in_specs=[HBM] * 5, out_specs=(HBM,) * 5,
        scratch_shapes=[
            V((d, t), BF16), V((d, t), F32), V((2, ft, t), F32), V((nt * ft, d), BF16), V((RING, d, ft), BF16), V((RING, tb, d), BF16),
            V((2, ft, d), BF16), V((2, nd, rows2, d), BF16), V((d, ft), BF16), V((2, d, ft), BF16), V((2, ft, d), BF16),
            V((2, tb, d), BF16), V((2, d, tb), BF16), V((ft, rb), BF16), V((ft, rb), BF16),
            D((RING,)), D((RING,)), D((2,)), D((2, 2)), D((2,)), D((3, 2))],
        compiler_params=pltpu.CompilerParams(vmem_limit_bytes=VMEM_MAX),
        name="forward_one",
    )(x, e, w1, w3, w2r)


MESH = pl.DeviceIdType.MESH

def gelu_pair(pre):
    normal_cdf = 0.5 * (1.0 + lax.erf(pre * ROOT_HALF))
    density = jnp.exp(-0.5 * pre * pre) * INV_ROOT_TAU
    return pre * normal_cdf, normal_cdf + pre * density

def flip(value, step):
    return value + step * (1 - 2 * lax.rem(lax.div(value, step), 2))

def position():
    me = lax.axis_index("data")
    chip = lax.div(me, 2)
    steps = [(1 << k) * (1 - 2 * lax.rem(lax.div(chip, 1 << k), 2)) for k in range(AXES)]
    return me, lax.rem(me, 2), chip, steps


def hop(steps, kind, place, j):
    axis = lax.rem(j + ORDERS[kind][place], AXES)
    return steps[0] * lax.div((2 - axis) * (1 - axis), 2) + steps[1] * axis * (2 - axis) + steps[2] * lax.div(axis * (axis - 1), 2)


def relative(hops, p):
    return sum((hops[place] for place in range(AXES) if (p >> (AXES - 1 - place)) & 1), 0)


AXES = 3
ORDERS = ((0, 2, 1), (1, 2, 0))
PARTS = 8
BACK_BLOCKS = 4
BEGUN = 2
TURN = 128
SEEN = (3, 5, 7, 8)
DEPTH = (2, 6, 6, 6)
LAST = len(SEEN) - 1
ACCS = 5

def kernel_bc(cfg, ut_hbm, et_hbm, xt_hbm, z_hbm, w3_hbm, w4_hbm, w2_hbm,
              gu_hbm, gd_hbm, nrm_ref,
              act, side, euacc, wa, wb, wat, zb0, zb1, eb0, eb1, hb0, hb1, qb0, qb1,
              gu, gt, gd, r0u, r0d, au, ad, r1u, r1d, r2u, r2d, r3u, r3d, fu, fd, nu, nd_acc, nsend, nrecv,
              insem, wsem, zsem, ssem, rsem, fsem, nsem):
    nt, nr, nc, t, ft, d, nd = cfg
    rb, rc = t // nr, t // nc
    total = 2 * nt
    me, core, chip, steps = position()
    partner = flip(me, 1)
    zb, eb, hb, qb = (zb0, zb1), (eb0, eb1), (hb0, hb1), (qb0, qb1)
    G, R, ACC, FIN, NRM, OUT = (gu, gd), ((r0u, r1u, r2u, r3u), (r0d, r1d, r2d, r3d)), (au, ad), (fu, fd), (nu, nd_acc), (gu_hbm, gd_hbm)

    loads = [pltpu.make_async_copy(ut_hbm, act, insem.at[0]), pltpu.make_async_copy(et_hbm, side, insem.at[1])]
    for c in loads:
        c.start()

    def wcopies(j, slot, back):
        second = w2_hbm if back else w4_hbm
        cps = [pltpu.make_async_copy(second.at[:, j], wb.at[slot], wsem.at[1, slot])]
        if not back:
            cps.append(pltpu.make_async_copy(w3_hbm.at[:, j], wa.at[slot], wsem.at[0, slot]))
        return cps
    for c in wcopies(0, 0, False):
        c.start()

    barrier = pltpu.get_barrier_semaphore()
    for k in range(1, nd):
        pl.semaphore_signal(barrier, inc=1, device_id=(lax.rem(me + k, nd),), device_id_type=MESH)
    pl.semaphore_wait(barrier, nd - 1)

    nu[...] = jnp.zeros_like(nu)
    nd_acc[...] = jnp.zeros_like(nd_acc)
    gt[1] = jnp.zeros_like(gt[1])
    def zero(r, _):
        euacc[:, aligned(r, rb)] = jnp.zeros((d, rb), F32)
        return 0
    lax.fori_loop(0, nr, zero, 0)

    def send(kind, stage, j):
        depth = R[kind][stage].shape[0]
        slot = lax.rem(j, depth)
        sem = (kind * len(SEEN) + stage) * max(DEPTH) + slot
        dst = R[kind][stage].at[slot]
        if stage == 0:
            src, dev = G[kind].at[lax.rem(j, G[kind].shape[0]), :, 1 - core], partner
        else:
            lo = PARTS >> stage
            src, dev = ACC[kind].at[lax.rem(j, ACCS), pl.ds(lo, lo)], me + 2 * hop(steps, kind, stage - 1, j)
        return pltpu.make_async_remote_copy(src_ref=src, dst_ref=dst, send_sem=ssem.at[sem], recv_sem=rsem.at[sem],
                                            device_id=(dev,), device_id_type=MESH)

    def final_copy(kind, j):
        slot = lax.rem(j, 2)
        return pltpu.make_async_copy(FIN[kind].at[slot], OUT[kind].at[j], fsem.at[kind, slot])

    def absorb(stage, j):
        place = lax.rem(j, ACCS)
        for kind in range(2):
            send(kind, stage, j).wait()
            slot = lax.rem(j, R[kind][stage].shape[0])
            got, acc = R[kind][stage], ACC[kind]
            if stage == 0:
                hops = [hop(steps, kind, place, j) for place in range(AXES)]
                for p in range(PARTS):
                    oc = chip + relative(hops, p)
                    acc[place, p] = G[kind][lax.rem(j, G[kind].shape[0]), oc, core] + got[slot, oc]
            elif stage < LAST:
                keep = pl.ds(0, PARTS >> stage)
                acc[place, keep] += got[slot]
            else:
                @pl.when(j >= 2)
                def _():
                    final_copy(kind, j - 2).wait()
                f = (acc[place, 0] + got[slot, 0]) * (1.0 / nd)
                FIN[kind][lax.rem(j, 2)] = f
                NRM[kind][...] += f * f
        for kind in range(2):
            (send(kind, stage + 1, j) if stage < LAST else final_copy(kind, j)).start()

    def comm(step):
        def when_valid(j, fn):
            @pl.when(jnp.logical_and(j >= 0, j < total))
            def _():
                fn()
        for stage in reversed(range(len(SEEN))):
            when_valid(step - SEEN[stage], functools.partial(absorb, stage, step - SEEN[stage]))
        def start():
            for kind in range(2):
                send(kind, 0, step - BEGUN).start()
        when_valid(step - BEGUN, start)

    def turn(step, part):
        slot = lax.rem(step + 1, 2)
        lanes = pl.ds(part * TURN, TURN)
        gd[slot, :, :, :, lanes] = gt[slot, lanes, :].T.reshape(gd.shape[1:-1] + (TURN,))

    def add_up(step, r, value):
        slot, value = lax.rem(step, gu.shape[0]), value.reshape(gu.shape[1:])
        gu[slot] = value if r == 0 else gu[slot] + value

    def add_down(step, r, value):
        slot = lax.rem(step, 2)
        gt[slot] = value if r == 0 else gt[slot] + value

    def gates(r, width, pre):
        h, der = gelu_pair(pre)
        lanes = pl.ds(0, width)
        hb[r % 2][:, lanes] = h.astype(BF16)
        qb[r % 2][:, lanes] = (eb[r % 2][:, lanes].astype(F32) * der).astype(BF16)

    def pipeline(step, blocks, front, middle, back):
        front(0)
        for r in range(blocks):
            middle(r)
            if r + 1 < blocks:
                front(r + 1)
            if r >= 1:
                back(r - 1)
            for part in range(r, d // TURN, blocks):
                turn(step, part)
        back(blocks - 1)

    for c in loads:
        c.wait()

    def tile_b(j, _):
        slot = lax.rem(j, 2)
        comm(j)
        for c in wcopies(j, slot, False):
            c.wait()
        @pl.when(j + 1 < nt)
        def _():
            for c in wcopies(j + 1, 1 - slot, False):
                c.start()
        def cols(r):
            return pl.ds(r * rb, rb)
        mine = pl.ds(0, rb)
        def front(r):
            zb[r % 2][...] = dot_nn(wa[slot].reshape(ft, d), act[:, cols(r)])
            eb[r % 2][:, mine] = dot_nn(wb[slot].reshape(ft, d), side[:, cols(r)]).astype(BF16)
            if r == 0:
                wat[...] = wa[slot].reshape(ft, d).T
        def middle(r):
            gates(r, rb, zb[r % 2][...])
        def back(r):
            q = qb[r % 2][:, mine]
            euacc[:, cols(r)] += dot_nn(wat[...], q)
            add_up(j, r, dot_nt(act[:, cols(r)], q))
            add_down(j, r, dot_nt(side[:, cols(r)], hb[r % 2][:, mine]))
        pipeline(j, nr, front, middle, back)
        return 0
    lax.fori_loop(0, nt, tile_b, 0)

    xt_in = pltpu.make_async_copy(xt_hbm, side, insem.at[1])
    xt_in.start()
    for c in wcopies(0, nt % 2, True):
        c.start()
    def cast(r, _):
        act[:, aligned(r, rb)] = euacc[:, aligned(r, rb)].astype(BF16)
        return 0
    lax.fori_loop(0, nr, cast, 0)
    def zcopy(j, slot):
        return pltpu.make_async_copy(z_hbm.at[j], euacc.at[aligned(slot, ft), :], zsem.at[slot])
    zcopy(0, nt % 2).start()
    xt_in.wait()

    def tile_c(step, _):
        j = step - nt
        slot = lax.rem(step, 2)
        comm(step)
        for c in wcopies(j, slot, True):
            c.wait()
        zcopy(j, slot).wait()
        @pl.when(j + 1 < nt)
        def _():
            for c in wcopies(j + 1, 1 - slot, True):
                c.start()
            zcopy(j + 1, 1 - slot).start()
        def cols(r):
            return pl.ds(r * rc, rc)
        mine = pl.ds(0, rc)
        def front(r):
            eb[r % 2][:, mine] = dot_nn(wb[slot].reshape(ft, d), act[:, cols(r)]).astype(BF16)
        def middle(r):
            gates(r, rc, euacc[aligned(slot, ft), cols(r)])
        def back(r):
            add_up(step, r, dot_nt(side[:, cols(r)], qb[r % 2][:, mine]))
            add_down(step, r, dot_nt(act[:, cols(r)], hb[r % 2][:, mine]))
        pipeline(step, nc, front, middle, back)
        return 0
    lax.fori_loop(nt, total, tile_c, 0)

    def drain(step, _):
        comm(step)
        @pl.when(step == total)
        def _():
            for part in range(d // TURN):
                turn(step, part)
        return 0
    lax.fori_loop(total, total + SEEN[LAST], drain, 0)
    for kind in range(2):
        for j in (total - 2, total - 1):
            final_copy(kind, j).wait()

    part = jnp.zeros((8, 128), F32)
    for ref in (nu, nd_acc):
        rows, cols = ref.shape
        for a in range(rows // 8):
            for b in range(cols // 128):
                part = part + ref[8 * a:8 * a + 8, 128 * b:128 * b + 128]
    nsend[...] = part
    nrecv[me] = part
    for k in range(1, nd):
        pltpu.make_async_remote_copy(src_ref=nsend, dst_ref=nrecv.at[me], send_sem=nsem.at[0], recv_sem=nsem.at[1],
                                     device_id=(lax.rem(me + k, nd),), device_id_type=MESH).start()
    others = nrecv.at[pl.ds(0, nd - 1)]
    pltpu.make_async_remote_copy(src_ref=others, dst_ref=others, send_sem=nsem.at[0], recv_sem=nsem.at[1],
                                 device_id=(me,), device_id_type=MESH).wait()
    total_sq = nrecv[0]
    for k in range(1, nd):
        total_sq = total_sq + nrecv[k]
    nrm_ref[...] = total_sq

def backward(ut, et, xt, z, w3r, w4r, w2r):
    d, t = ut.shape
    nd, nt, rows2, _ = w4r.shape
    ft, nr, nc = nd * rows2, BACK_BLOCKS, BACK_BLOCKS // 2
    rb, rc = t // nr, t // nc
    bu, bd = (d // nd, ft), (rows2, d)
    V, D = pltpu.VMEM, pltpu.SemaphoreType.DMA
    S = jax.ShapeDtypeStruct
    scratch = [V((d, t), BF16)] * 2 + [V((d, t), F32)] + [V((2, nd, rows2, d), BF16)] * 2 + [V((d, ft), BF16)]
    scratch += [V((ft, rb), F32)] * 2 + [V((ft, rc), BF16)] * 6
    scratch += [V((3, PARTS, 2) + bu, F32), V((2, d, ft), F32), V((2, PARTS, 2) + bd, F32)]
    for n, c in ((DEPTH[0], PARTS), (ACCS, PARTS)) + tuple((DEPTH[k], PARTS >> k) for k in range(1, LAST + 1)):
        scratch += [V((n, c) + bu, F32), V((n, c) + bd, F32)]
    scratch += [V((2,) + bu, F32), V((2,) + bd, F32), V(bu, F32), V(bd, F32), V((8, 128), F32), V((nd, 8, 128), F32)]
    flags = 2 * len(SEEN) * max(DEPTH)
    scratch += [D((2,)), D((2, 2)), D((2,)), D((flags,)), D((flags,)), D((2, 2)), D((2,))]
    return pl.pallas_call(
        functools.partial(kernel_bc, (nt, nr, nc, t, ft, d, nd)),
        out_shape=(S((2 * nt,) + bu, F32), S((2 * nt,) + bd, F32), S((8, 128), F32)),
        in_specs=[HBM] * 7, out_specs=(HBM, HBM, pl.BlockSpec(memory_space=pltpu.VMEM)),
        scratch_shapes=scratch,
        compiler_params=pltpu.CompilerParams(collective_id=0, has_side_effects=True, vmem_limit_bytes=VMEM_MAX),
        name="backward",
    )(ut, et, xt, z, w3r, w4r, w2r)


LAG = 2
EMIT = 4

def kernel_gather(cfg, su1, su2, sd1, sd2, ou1, ou2, od1, od2, lsem, rsem, ssem, dsem):
    nd, pieces, ru, cu, rd = cfg
    me, core, chip, steps = position()
    partner = flip(me, 1)
    IN, O = ((su1, su2), (sd1, sd2)), ((ou1, ou2), (od1, od2))
    layers = range(len(O[0]))
    barrier = pltpu.get_barrier_semaphore()
    peers = [partner] + [me + 2 * s for s in steps]
    for peer in peers:
        pl.semaphore_signal(barrier, inc=1, device_id=(peer,), device_id_type=MESH)
    pl.semaphore_wait(barrier, len(peers))

    def block(kind, first, j, ref):
        if kind == 0:
            return ref.at[pl.ds(pl.multiple_of(first, 8), ru), aligned(j, cu)]
        return ref.at[pl.ds(pl.multiple_of(first + j * rd, 8), rd), :]

    height = (ru, rd * pieces)
    own = [pltpu.make_async_copy(IN[kind][w], O[kind][w].at[aligned(me, height[kind]), :], lsem.at[kind, w])
           for kind in range(2) for w in layers]

    def push(kind, p, j, hops, dev, send, recv):
        first = (2 * (chip + relative(hops, p)) + core) * height[kind]
        for w in layers:
            dst = block(kind, first, j, O[kind][w])
            src = dst if p else block(kind, 0, j, IN[kind][w])
            pltpu.make_async_remote_copy(src_ref=src, dst_ref=dst, send_sem=send, recv_sem=recv, device_id=(dev,), device_id_type=MESH).start()

    def flag(kind, stage, j):
        return rsem.at[kind, stage, lax.rem(j, AXES * LAG)]

    def spread(kind, stage, j, hops):
        dev = me + 2 * hops[AXES - 1 - stage]
        for p in range(1 << stage):
            push(kind, p, j, hops, dev, ssem.at[kind, stage], flag(kind, stage, j))

    def await_bytes(ref, sem, recv):
        cp = pltpu.make_async_remote_copy(src_ref=ref, dst_ref=ref, send_sem=sem, recv_sem=sem, device_id=(me,), device_id_type=MESH)
        if recv:
            cp.wait_recv()
        else:
            cp.wait_send()

    def arrived(kind, stage, j):
        n = 2 << stage
        part = O[kind][0].at[pl.ds(0, n * ru), pl.ds(0, cu)] if kind == 0 else O[kind][0].at[pl.ds(0, n * rd), :]
        await_bytes(part, flag(kind, stage, j), True)

    def step(s, _):
        for stage in reversed(range(AXES + 1)):
            j = s - stage * LAG
            @pl.when(jnp.logical_and(j >= 0, j < pieces))
            def _():
                for kind in range(2):
                    hops = [hop(steps, kind, place, j) for place in range(AXES)]
                    if stage:
                        arrived(kind, stage - 1, j)
                    if stage < AXES:
                        spread(kind, stage, j, hops)
                    for p in range((1 << stage) >> 1, 1 << stage):
                        push(kind, p, j, hops, partner, dsem.at[0, kind], dsem.at[1, kind])
        return 0
    for c in own:
        c.start()
    lax.fori_loop(0, pieces + AXES * LAG, step, 0)
    for c in own:
        c.wait()
    for kind in range(2):
        full = O[kind][0]
        await_bytes(full, dsem.at[0, kind], False)
        await_bytes(full, dsem.at[1, kind], True)
        for stage in range(AXES):
            await_bytes(full.at[pl.ds(0, (2 << stage) * height[kind]), :], ssem.at[kind, stage], False)


def gather(shards, nd):
    (ru, f), (rf, d) = shards[0].shape, shards[2].shape
    pieces = rf // 16
    D, S = pltpu.SemaphoreType.DMA, jax.ShapeDtypeStruct
    anyspec = pl.BlockSpec(memory_space=pl.ANY)
    return pl.pallas_call(
        functools.partial(kernel_gather, (nd, pieces, ru, f // pieces, rf // pieces)),
        out_shape=(S((ru * nd, f), BF16),) * 2 + (S((rf * nd, d), BF16),) * 2,
        in_specs=[anyspec] * 4, out_specs=(anyspec,) * 4,
        scratch_shapes=[D((2, 2)), D((2, 3, AXES * LAG)), D((2, 3)), D((2, 2))],
        compiler_params=pltpu.CompilerParams(collective_id=1, has_side_effects=True, vmem_limit_bytes=1024 * 1024),
        name="gather")(*shards)


def kernel_emit(*refs):
    count = (len(refs) - 1) // 2
    copies = []
    for k in range(count):
        rows = refs[k].shape[0] // EMIT
        for part in range(EMIT):
            piece = pl.ds(part * rows, rows)
            copies.append(pltpu.make_async_copy(refs[k].at[piece, :], refs[count + k].at[piece, :], refs[-1].at[k, part]))
    for c in copies:
        c.start()
    for c in copies:
        c.wait()


def emit(arrays):
    return pl.pallas_call(
        kernel_emit, out_shape=[jax.ShapeDtypeStruct(a.shape, a.dtype) for a in arrays],
        in_specs=[pl.BlockSpec(memory_space=pl.ANY)] * len(arrays), out_specs=[HBM] * len(arrays),
        scratch_shapes=[pltpu.SemaphoreType.DMA((len(arrays), EMIT))],
        compiler_params=pltpu.CompilerParams(vmem_limit_bytes=1024 * 1024), name="emit")(*arrays)


STEP = 20
BETA_ONE = 0.9
BETA_TWO = 0.95
EPSILON = 1e-8
NORM_EPS = 1e-6
CORR_ONE = 1.0 - BETA_ONE ** STEP
CORR_TWO = 1.0 - BETA_TWO ** STEP


def kernel_adam(cfg, sq_ref, rate_ref, clip_ref, gu_hbm, gd_hbm, *refs):
    nd, nt = cfg
    states, outs, half, norm_ref, (gbuf_u, gbuf_d, sbuf_u, sbuf_d, obuf_u, obuf_d, lsem, osem) = refs[:12], refs[12:24], refs[24:28], refs[28], refs[29:]
    lanes, width = 128, 16
    per = lanes // width
    gbuf, sbuf, obuf = (gbuf_u, gbuf_d), (sbuf_u, sbuf_d), (obuf_u, obuf_d)
    order = (2, 3, 1, 0)

    def loads(k):
        kind, layer = k % 2, k // 2
        src = (gu_hbm, gd_hbm)[kind].at[pl.ds((1 - layer) * nt, nt)]
        return [pltpu.make_async_copy(src, gbuf[kind].at[layer], lsem.at[k])] + [
            pltpu.make_async_copy(states[4 * f + k], sbuf[kind].at[layer, f], lsem.at[k]) for f in range(3)]

    def stores(k):
        kind, layer = k % 2, k // 2
        return [pltpu.make_async_copy(obuf[kind].at[layer, f], outs[4 * f + k], osem.at[k]) for f in range(3)]
    for k in order:
        for c in loads(k):
            c.start()
    norm = jnp.sqrt(jnp.sum(sq_ref[...], keepdims=True))
    norm_ref[...] = norm
    rate, clip = rate_ref[0], clip_ref[0]
    scale = jnp.minimum(1.0, clip / (norm + NORM_EPS))
    group = lax.broadcasted_iota(jnp.int32, (8, lanes), 1) // width

    def update(kind, layer, rows, grad):
        master, mom, vel = [sbuf[kind][layer, f, rows, :] for f in range(3)]
        scaled = scale * grad
        mom = BETA_ONE * mom + (1.0 - BETA_ONE) * scaled
        vel = BETA_TWO * vel + (1.0 - BETA_TWO) * scaled * scaled
        master = master - rate * (mom * (1.0 / CORR_ONE)) / (jnp.sqrt(vel * (1.0 / CORR_TWO)) + EPSILON)
        half[2 * kind + layer][rows, :] = master.astype(BF16)
        for f, value in enumerate((master, mom, vel)):
            obuf[kind][layer, f, rows, :] = value

    for k in order:
        kind, layer = k % 2, k // 2
        for c in loads(k):
            c.wait()
        if kind == 0:
            def body(r, _):
                rows = pl.ds(pl.multiple_of(r * 8, 8), 8)
                cols = []
                for t in range(nd * nt // per):
                    acc = None
                    for s in range(per):
                        k_owner, j = divmod(per * t + s, nt)
                        src = gbuf_u[layer, j, rows, (k_owner // per) * lanes:(k_owner // per + 1) * lanes]
                        shift = (s - k_owner) % per * width
                        turned = pltpu.roll(src, shift, 1) if shift else src
                        acc = turned if acc is None else jnp.where(group == s, turned, acc)
                    cols.append(acc)
                update(0, layer, rows, jnp.concatenate(cols, axis=1))
                return 0
            lax.fori_loop(0, sbuf_u.shape[2] // 8, body, 0)
        else:
            def body(j, _):
                n = gbuf_d.shape[2]
                update(1, layer, pl.ds(pl.multiple_of(j * n, n), n), gbuf_d[layer, j])
                return 0
            lax.fori_loop(0, nt, body, 0)
        for c in stores(k):
            c.start()
    for k in order:
        for c in stores(k):
            c.wait()


def adam(sq, rate, clip, gu, gd, states, nd):
    nt = gu.shape[0] // 2
    up, down = states[0].shape, states[1].shape
    S, V, D = jax.ShapeDtypeStruct, pltpu.VMEM, pltpu.SemaphoreType.DMA
    vm = pl.BlockSpec(memory_space=pltpu.VMEM)
    return pl.pallas_call(
        functools.partial(kernel_adam, (nd, nt)),
        out_shape=tuple(S(s.shape, F32) for s in states) + (S(up, BF16),) * 2 + (S(down, BF16),) * 2 + (S((1, 1), F32),),
        in_specs=[vm] + [pl.BlockSpec(memory_space=pltpu.SMEM)] * 2 + [HBM] * 14, out_specs=(HBM,) * 12 + (vm,) * 5,
        scratch_shapes=[V((2, nt) + gu.shape[1:], F32), V((2, nt) + gd.shape[1:], F32), V((2, 3) + up, F32), V((2, 3) + down, F32),
                        V((2, 3) + up, F32), V((2, 3) + down, F32), D((4,)), D((4,))],
        compiler_params=pltpu.CompilerParams(vmem_limit_bytes=VMEM_MAX),
        name="adam")(sq, rate.reshape(1), clip.reshape(1), gu, gd, *states)


def solution(mesh):
    groups = mesh.shape["data"]
    rows_spec = P("data", None)
    full_spec = P(None, None)
    scalar_spec = P()

    def shard_body(act_in, grad_out, w_up1, w_down1, w_up2, w_down2, *rest):
        states, learn_rate, clip_norm = rest[:12], rest[12], rest[13]
        ff, d = w_down1.shape
        down1_tiles = w_down1.reshape(groups, -1, 16, d)
        down2_tiles = w_down2.reshape(groups, -1, 16, d)
        pre1, mid_t, in_t, grad_t, up2_t = forward_one(act_in, grad_out, w_up1, w_up2, down1_tiles)
        up2_tiles = up2_t.reshape(down1_tiles.shape)
        grads_up, grads_down, sq = backward(mid_t, grad_t, in_t, pre1, up2_tiles, down2_tiles, down1_tiles)
        *new_states, up1, up2, down1, down2, norm = adam(sq, learn_rate, clip_norm, grads_up, grads_down, states, groups)
        up1, up2, down1, down2 = emit(gather((up1, up2, down1, down2), groups))
        return (up1, down1, up2, down2, *new_states, norm.reshape(()))

    in_specs = (rows_spec, rows_spec) + (full_spec,) * 4 + (rows_spec,) * 12 + (scalar_spec, scalar_spec)
    out_specs = (full_spec,) * 4 + (rows_spec,) * 12 + (scalar_spec,)
    return jax.shard_map(shard_body, mesh=mesh, in_specs=in_specs, out_specs=out_specs, check_vma=False)
```

```python
import functools
import math
import jax
import jax.numpy as jnp
from jax import lax
from jax.experimental import pallas as pl
from jax.experimental.pallas import tpu as pltpu
from jax.sharding import PartitionSpec as P

ROOT_HALF = math.sqrt(0.5)
INV_ROOT_TAU = 1.0 / math.sqrt(2.0 * math.pi)
F32, BF16 = jnp.float32, jnp.bfloat16
HBM = pl.BlockSpec(memory_space=pltpu.HBM)
VMEM_MAX = 64 * 1024 * 1024 - 65536
BLOCKS = 8
TURNS = 8
RING = 6


def dot_nn(a, b):
    return lax.dot_general(a, b, (((1,), (0,)), ((), ())), preferred_element_type=F32)


def dot_nt(a, b):
    return lax.dot_general(a, b, (((1,), (1,)), ((), ())), preferred_element_type=F32)


def gelu(z):
    return z * (0.5 * (1.0 + lax.erf(z * ROOT_HALF)))


def at_most(j, bound):
    return jnp.minimum(j, bound)


def aligned(j, size):
    return pl.ds(pl.multiple_of(j * size, size), size)


def kernel_a(cfg, x_hbm, e_hbm, w1_hbm, w3_hbm, w2_hbm, z_hbm, ut_hbm, xt_hbm, et_hbm, w3t_hbm,
             xt, uacc, zout, w1t_v, w1_in, x_in, w1, w2, w2t, w3_in, w3_out, e_in, e_out, h0, h1,
             wsem, xsem, esem, vsem, zsem, osem):
    nt, nr, rb, tr, tb, ft, d, nd = cfg
    hb = (h0, h1)
    width = ft // nd

    def w1copy(q):
        slot = lax.rem(q, RING)
        return pltpu.make_async_copy(w1_hbm.at[:, aligned(q, ft)], w1_in.at[slot], wsem.at[slot])

    def xcopy(r):
        slot = lax.rem(r, RING)
        return pltpu.make_async_copy(x_hbm.at[aligned(r, tb), :], x_in.at[slot], xsem.at[slot])

    def w2copy(j):
        slot = lax.rem(j, 2)
        return pltpu.make_async_copy(w2_hbm.at[:, j], w2.at[slot], vsem.at[0, slot])

    def w3copy(j):
        slot = lax.rem(j, 2)
        return pltpu.make_async_copy(w3_hbm.at[:, aligned(j, ft)], w3_in.at[slot], vsem.at[1, slot])

    def w3store(j):
        slot = lax.rem(j, 2)
        return pltpu.make_async_copy(w3_out.at[slot], w3t_hbm.at[aligned(j, ft), :], osem.at[0, slot])

    def ecopy(r):
        slot = lax.rem(r, 2)
        return pltpu.make_async_copy(e_hbm.at[aligned(r, tb), :], e_in.at[slot], esem.at[slot])

    def estore(r):
        slot = lax.rem(r, 2)
        return pltpu.make_async_copy(e_out.at[slot], et_hbm.at[:, aligned(r, tb)], osem.at[1, slot])

    def zstore(j):
        slot = lax.rem(j, 2)
        return pltpu.make_async_copy(zout.at[slot], z_hbm.at[j], zsem.at[slot])

    for q in range(min(RING, nt)):
        w1copy(q).start()
    for r in range(min(RING, tr)):
        xcopy(r).start()
    for c in (w2copy(0), w3copy(0), ecopy(0)):
        c.start()

    def zero(r, _):
        uacc[:, aligned(r, rb)] = jnp.zeros((d, rb), F32)
        return 0
    lax.fori_loop(0, nr, zero, 0)

    def turn_w1(q, _):
        w1copy(q).wait()
        w1t_v[aligned(q, ft), :] = w1_in[lax.rem(q, RING)].T
        @pl.when(q + RING < nt)
        def _():
            w1copy(q + RING).start()
        return 0
    lax.fori_loop(0, nt, turn_w1, 0)

    def turn_x(r, _):
        xcopy(r).wait()
        xt[:, aligned(r, tb)] = x_in[lax.rem(r, RING)].T
        @pl.when(r + RING < tr)
        def _():
            xcopy(r + RING).start()
        return 0
    lax.fori_loop(0, tr, turn_x, 0)
    xt_store = pltpu.make_async_copy(xt, xt_hbm, osem.at[2, 0])
    xt_store.start()

    def pick_w1(j, slot):
        for k in range(nd):
            w1[slot, k * width:(k + 1) * width, :] = w1t_v[aligned(k * nt + j, width), :]
    pick_w1(0, 0)

    def tile(j, _):
        slot = lax.rem(j, 2)
        nslot = 1 - slot
        @pl.when(j >= 2)
        def _():
            zstore(j - 2).wait()
            w3store(j - 2).wait()
        @pl.when(jnp.logical_and(j >= 2, j < tr + 2))
        def _():
            estore(j - 2).wait()
        w2copy(j).wait()
        w3copy(j).wait()
        @pl.when(j < tr)
        def _():
            ecopy(j).wait()
        @pl.when(j + 1 < nt)
        def _():
            w2copy(j + 1).start()
            w3copy(j + 1).start()
        @pl.when(j + 1 < min(tr, nt))
        def _():
            ecopy(j + 1).start()

        def cols(r):
            return pl.ds(r * rb, rb)
        def front(r):
            zout[slot, :, cols(r)] = dot_nn(w1[slot], xt[:, cols(r)])
        def middle(r):
            hb[r % 2][...] = gelu(zout[slot, :, cols(r)]).astype(BF16)
        def back(r):
            uacc[:, cols(r)] += dot_nn(w2t[...], hb[r % 2][...])
        front(0)
        w2t[...] = w2[slot].reshape(ft, d).T
        for r in range(nr):
            middle(r)
            if r + 1 < nr:
                front(r + 1)
            if r >= 1:
                back(r - 1)
            if r == 0:
                pick_w1(at_most(j + 1, nt - 1), nslot)
            if r == 1:
                w3_out[slot] = w3_in[slot].T
            if r == nr - 2:
                e_out[slot] = e_in[slot].T
        back(nr - 1)
        zstore(j).start()
        w3store(j).start()
        @pl.when(j < tr)
        def _():
            estore(j).start()
        return 0
    lax.fori_loop(0, nt, tile, 0)
    xt_store.wait()

    def finish(r, _):
        xt[:, aligned(r, rb)] = uacc[:, aligned(r, rb)].astype(BF16)
        return 0
    lax.fori_loop(0, nr, finish, 0)
    ut_store = pltpu.make_async_copy(xt, ut_hbm, osem.at[2, 1])
    ut_store.start()
    for j in (nt - 2, nt - 1):
        zstore(j).wait()
        w3store(j).wait()
        if j < tr:
            estore(j).wait()
    for r in range(nt, tr):
        ecopy(r).start()
        ecopy(r).wait()
        e_out[r % 2] = e_in[r % 2].T
        estore(r).start()
        estore(r).wait()
    ut_store.wait()


def forward_one(x, e, w1, w3, w2r):
    t, d = x.shape
    nd, nt, rows2, _ = w2r.shape
    ft, nr, tr = nd * rows2, BLOCKS, TURNS
    rb, tb = t // nr, t // tr
    V, D = pltpu.VMEM, pltpu.SemaphoreType.DMA
    S = jax.ShapeDtypeStruct
    return pl.pallas_call(
        functools.partial(kernel_a, (nt, nr, rb, tr, tb, ft, d, nd)),
        out_shape=(S((nt, ft, t), F32), S((d, t), BF16), S((d, t), BF16), S((d, t), BF16), S((nt * ft, d), BF16)),
        in_specs=[HBM] * 5, out_specs=(HBM,) * 5,
        scratch_shapes=[
            V((d, t), BF16), V((d, t), F32), V((2, ft, t), F32), V((nt * ft, d), BF16), V((RING, d, ft), BF16), V((RING, tb, d), BF16),
            V((2, ft, d), BF16), V((2, nd, rows2, d), BF16), V((d, ft), BF16), V((2, d, ft), BF16), V((2, ft, d), BF16),
            V((2, tb, d), BF16), V((2, d, tb), BF16), V((ft, rb), BF16), V((ft, rb), BF16),
            D((RING,)), D((RING,)), D((2,)), D((2, 2)), D((2,)), D((3, 2))],
        compiler_params=pltpu.CompilerParams(vmem_limit_bytes=VMEM_MAX),
        name="forward_one",
    )(x, e, w1, w3, w2r)


MESH = pl.DeviceIdType.MESH

def gelu_pair(pre):
    normal_cdf = 0.5 * (1.0 + lax.erf(pre * ROOT_HALF))
    density = jnp.exp(-0.5 * pre * pre) * INV_ROOT_TAU
    return pre * normal_cdf, normal_cdf + pre * density

def flip(value, step):
    return value + step * (1 - 2 * lax.rem(lax.div(value, step), 2))

def position():
    me = lax.axis_index("data")
    chip = lax.div(me, 2)
    steps = [(1 << k) * (1 - 2 * lax.rem(lax.div(chip, 1 << k), 2)) for k in range(AXES)]
    return me, lax.rem(me, 2), chip, steps


def hop(steps, kind, place, j):
    axis = lax.rem(j + ORDERS[kind][place], AXES)
    return steps[0] * lax.div((2 - axis) * (1 - axis), 2) + steps[1] * axis * (2 - axis) + steps[2] * lax.div(axis * (axis - 1), 2)


def relative(hops, p):
    return sum((hops[place] for place in range(AXES) if (p >> (AXES - 1 - place)) & 1), 0)


AXES = 3


def meet(peers):
    barrier = pltpu.get_barrier_semaphore()
    for peer in peers:
        pl.semaphore_signal(barrier, inc=1, device_id=(peer,), device_id_type=MESH)
    pl.semaphore_wait(barrier, len(peers))


ORDERS = ((0, 2, 1), (1, 2, 0))
PARTS = 8
BACK_BLOCKS = 4
BEGUN = 2
TURN = 128
SEEN = (3, 6, 9, 12)
DEPTH = (2, 6, 6, 6)
LAST = len(SEEN) - 1
HOLD = 3

def kernel_bc(cfg, ut_hbm, et_hbm, xt_hbm, z_hbm, w3_hbm, w4_hbm, w2_hbm,
              gu_hbm, gd_hbm, nrm_ref,
              act, side, euacc, wa, wb, wat, zb0, zb1, eb0, eb1, hb0, hb1, qb0, qb1,
              gu, gt, gd, r0u, r0d, a0u, a0d, a1u, a1d, a2u, a2d, r1u, r1d, r2u, r2d, r3u, r3d, fu, fd, nu, nd_acc,
              insem, wsem, zsem, ssem, rsem, fsem):
    nt, nr, nc, t, ft, d, nd = cfg
    rb, rc = t // nr, t // nc
    total = 2 * nt
    me, core, chip, steps = position()
    partner = flip(me, 1)
    zb, eb, hb, qb = (zb0, zb1), (eb0, eb1), (hb0, hb1), (qb0, qb1)
    G, R, ACC, FIN, NRM, OUT = (gu, gd), ((r0u, r1u, r2u, r3u), (r0d, r1d, r2d, r3d)), ((a0u, a1u, a2u), (a0d, a1d, a2d)), (fu, fd), (nu, nd_acc), (gu_hbm, gd_hbm)

    loads = [pltpu.make_async_copy(ut_hbm, act, insem.at[0]), pltpu.make_async_copy(et_hbm, side, insem.at[1])]
    for c in loads:
        c.start()

    def wcopies(j, slot, back):
        second = w2_hbm if back else w4_hbm
        cps = [pltpu.make_async_copy(second.at[:, j], wb.at[slot], wsem.at[1, slot])]
        if not back:
            cps.append(pltpu.make_async_copy(w3_hbm.at[:, j], wa.at[slot], wsem.at[0, slot]))
        return cps
    for c in wcopies(0, 0, False):
        c.start()

    meet([partner] + [me + 2 * s for s in steps])

    nu[...] = jnp.zeros_like(nu)
    nd_acc[...] = jnp.zeros_like(nd_acc)
    gt[1] = jnp.zeros_like(gt[1])
    def zero(r, _):
        euacc[:, aligned(r, rb)] = jnp.zeros((d, rb), F32)
        return 0
    lax.fori_loop(0, nr, zero, 0)

    def send(kind, stage, j):
        depth = R[kind][stage].shape[0]
        slot = lax.rem(j, depth)
        sem = (kind * len(SEEN) + stage) * max(DEPTH) + slot
        dst = R[kind][stage].at[slot]
        if stage == 0:
            src, dev = G[kind].at[lax.rem(j, G[kind].shape[0]), :, 1 - core], partner
        else:
            lo = PARTS >> stage
            src, dev = ACC[kind][stage - 1].at[lax.rem(j, HOLD), pl.ds(lo, lo)], me + 2 * hop(steps, kind, stage - 1, j)
        return pltpu.make_async_remote_copy(src_ref=src, dst_ref=dst, send_sem=ssem.at[sem], recv_sem=rsem.at[sem],
                                            device_id=(dev,), device_id_type=MESH)

    def final_copy(kind, j):
        slot = lax.rem(j, 2)
        return pltpu.make_async_copy(FIN[kind].at[slot], OUT[kind].at[j], fsem.at[kind, slot])

    def absorb(stage, j):
        place = lax.rem(j, HOLD)
        for kind in range(2):
            send(kind, stage, j).wait()
            slot = lax.rem(j, R[kind][stage].shape[0])
            got, acc = R[kind][stage], ACC[kind]
            if stage == 0:
                hops = [hop(steps, kind, place, j) for place in range(AXES)]
                for p in range(PARTS):
                    oc = chip + relative(hops, p)
                    acc[0][place, p] = G[kind][lax.rem(j, G[kind].shape[0]), oc, core] + got[slot, oc]
                continue
            kept = acc[stage - 1][place, 0:PARTS >> stage] + got[slot]
            if stage < LAST:
                acc[stage][place] = kept
            else:
                @pl.when(j >= 2)
                def _():
                    final_copy(kind, j - 2).wait()
                f = kept[0] * (1.0 / nd)
                FIN[kind][lax.rem(j, 2)] = f
                NRM[kind][...] += f * f
        for kind in range(2):
            (send(kind, stage + 1, j) if stage < LAST else final_copy(kind, j)).start()

    def comm(step):
        def when_valid(j, fn):
            @pl.when(jnp.logical_and(j >= 0, j < total))
            def _():
                fn()
        for stage in reversed(range(len(SEEN))):
            when_valid(step - SEEN[stage], functools.partial(absorb, stage, step - SEEN[stage]))
        def start():
            for kind in range(2):
                send(kind, 0, step - BEGUN).start()
        when_valid(step - BEGUN, start)

    def turn(step, part):
        slot = lax.rem(step + 1, 2)
        lanes = pl.ds(part * TURN, TURN)
        gd[slot, :, :, :, lanes] = gt[slot, lanes, :].T.reshape(gd.shape[1:-1] + (TURN,))

    def add_up(step, r, value):
        slot, value = lax.rem(step, gu.shape[0]), value.reshape(gu.shape[1:])
        gu[slot] = value if r == 0 else gu[slot] + value

    def add_down(step, r, value):
        slot = lax.rem(step, 2)
        gt[slot] = value if r == 0 else gt[slot] + value

    def gates(r, width, pre):
        h, der = gelu_pair(pre)
        lanes = pl.ds(0, width)
        hb[r % 2][:, lanes] = h.astype(BF16)
        qb[r % 2][:, lanes] = (eb[r % 2][:, lanes].astype(F32) * der).astype(BF16)

    def pipeline(step, blocks, front, middle, back):
        front(0)
        for r in range(blocks):
            middle(r)
            if r + 1 < blocks:
                front(r + 1)
            if r >= 1:
                back(r - 1)
            for part in range(r, d // TURN, blocks):
                turn(step, part)
        back(blocks - 1)

    for c in loads:
        c.wait()

    def tile_b(j, _):
        slot = lax.rem(j, 2)
        comm(j)
        for c in wcopies(j, slot, False):
            c.wait()
        @pl.when(j + 1 < nt)
        def _():
            for c in wcopies(j + 1, 1 - slot, False):
                c.start()
        def cols(r):
            return pl.ds(r * rb, rb)
        mine = pl.ds(0, rb)
        def front(r):
            zb[r % 2][...] = dot_nn(wa[slot].reshape(ft, d), act[:, cols(r)])
            eb[r % 2][:, mine] = dot_nn(wb[slot].reshape(ft, d), side[:, cols(r)]).astype(BF16)
            if r == 0:
                wat[...] = wa[slot].reshape(ft, d).T
        def middle(r):
            gates(r, rb, zb[r % 2][...])
        def back(r):
            q = qb[r % 2][:, mine]
            add_up(j, r, dot_nt(act[:, cols(r)], q))
            add_down(j, r, dot_nt(side[:, cols(r)], hb[r % 2][:, mine]))
            euacc[:, cols(r)] += dot_nn(wat[...], q)
        pipeline(j, nr, front, middle, back)
        return 0
    lax.fori_loop(0, nt, tile_b, 0)

    xt_in = pltpu.make_async_copy(xt_hbm, side, insem.at[1])
    xt_in.start()
    for c in wcopies(0, nt % 2, True):
        c.start()
    def cast(r, _):
        act[:, aligned(r, rb)] = euacc[:, aligned(r, rb)].astype(BF16)
        return 0
    lax.fori_loop(0, nr, cast, 0)
    def zcopy(j, slot):
        return pltpu.make_async_copy(z_hbm.at[j], euacc.at[aligned(slot, ft), :], zsem.at[slot])
    zcopy(0, nt % 2).start()
    xt_in.wait()

    def tile_c(step, _):
        j = step - nt
        slot = lax.rem(step, 2)
        comm(step)
        for c in wcopies(j, slot, True):
            c.wait()
        zcopy(j, slot).wait()
        @pl.when(j + 1 < nt)
        def _():
            for c in wcopies(j + 1, 1 - slot, True):
                c.start()
            zcopy(j + 1, 1 - slot).start()
        def cols(r):
            return pl.ds(r * rc, rc)
        mine = pl.ds(0, rc)
        def front(r):
            eb[r % 2][:, mine] = dot_nn(wb[slot].reshape(ft, d), act[:, cols(r)]).astype(BF16)
        def middle(r):
            gates(r, rc, euacc[aligned(slot, ft), cols(r)])
        def back(r):
            add_down(step, r, dot_nt(act[:, cols(r)], hb[r % 2][:, mine]))
            add_up(step, r, dot_nt(side[:, cols(r)], qb[r % 2][:, mine]))
        pipeline(step, nc, front, middle, back)
        return 0
    lax.fori_loop(nt, total, tile_c, 0)

    def drain(step, _):
        comm(step)
        @pl.when(step == total)
        def _():
            for part in range(d // TURN):
                turn(step, part)
        return 0
    lax.fori_loop(total, total + SEEN[LAST], drain, 0)
    for kind in range(2):
        for j in (total - 2, total - 1):
            final_copy(kind, j).wait()

    part = jnp.zeros((8, 128), F32)
    for ref in (nu, nd_acc):
        rows, cols = ref.shape
        for a in range(rows // 8):
            for b in range(cols // 128):
                part = part + ref[8 * a:8 * a + 8, 128 * b:128 * b + 128]
    nrm_ref[...] = part


def backward(ut, et, xt, z, w3r, w4r, w2r):
    d, t = ut.shape
    nd, nt, rows2, _ = w4r.shape
    ft, nr, nc = nd * rows2, BACK_BLOCKS, BACK_BLOCKS // 2
    rb, rc = t // nr, t // nc
    bu, bd = (d // nd, ft), (rows2, d)
    V, D = pltpu.VMEM, pltpu.SemaphoreType.DMA
    S = jax.ShapeDtypeStruct
    scratch = [V((d, t), BF16)] * 2 + [V((d, t), F32)] + [V((2, nd, rows2, d), BF16)] * 2 + [V((d, ft), BF16)]
    scratch += [V((ft, rb), F32)] * 2 + [V((ft, rc), BF16)] * 6
    scratch += [V((3, PARTS, 2) + bu, F32), V((2, d, ft), F32), V((2, PARTS, 2) + bd, F32)]
    for n, c in [(DEPTH[0], PARTS)] + [(HOLD, PARTS >> k) for k in range(LAST)] + [(DEPTH[k], PARTS >> k) for k in range(1, LAST + 1)]:
        scratch += [V((n, c) + bu, F32), V((n, c) + bd, F32)]
    scratch += [V((2,) + bu, F32), V((2,) + bd, F32), V(bu, F32), V(bd, F32)]
    flags = 2 * len(SEEN) * max(DEPTH)
    scratch += [D((2,)), D((2, 2)), D((2,)), D((flags,)), D((flags,)), D((2, 2))]
    return pl.pallas_call(
        functools.partial(kernel_bc, (nt, nr, nc, t, ft, d, nd)),
        out_shape=(S((2 * nt,) + bu, F32), S((2 * nt,) + bd, F32), S((8, 128), F32)),
        in_specs=[HBM] * 7, out_specs=(HBM, HBM, pl.BlockSpec(memory_space=pltpu.VMEM)),
        scratch_shapes=scratch,
        compiler_params=pltpu.CompilerParams(collective_id=0, has_side_effects=True, vmem_limit_bytes=VMEM_MAX),
        name="backward",
    )(ut, et, xt, z, w3r, w4r, w2r)


STEP = 20
BETA_ONE = 0.9
BETA_TWO = 0.95
EPSILON = 1e-8
NORM_EPS = 1e-6
CORR_ONE = 1.0 - BETA_ONE ** STEP
CORR_TWO = 1.0 - BETA_TWO ** STEP
LANES = 128
WIDTH = 16
LAG = 2
AHEAD = 2
EMIT = 4
UPDATE_VMEM = 19 * 1024 * 1024 + 256 * 1024
EMIT_VMEM = 17 * 1024 * 1024


def clip_scale(norm, clip):
    return jnp.minimum(1.0, clip / (norm + NORM_EPS))


def adam_rows(scale, rate, grad, master, mom, vel):
    scaled = scale * grad
    mom = BETA_ONE * mom + (1.0 - BETA_ONE) * scaled
    vel = BETA_TWO * vel + (1.0 - BETA_TWO) * scaled * scaled
    master = master - rate * (mom * (1.0 / CORR_ONE)) / (jnp.sqrt(vel * (1.0 / CORR_TWO)) + EPSILON)
    return master, mom, vel


def natural_columns(gbuf, layer, first, count, nd, nt):
    rows, per = gbuf.shape[2], LANES // WIDTH
    group = lax.broadcasted_iota(jnp.int32, (rows, LANES), 1) // WIDTH
    tiles = []
    for t in range(count):
        acc = None
        for s in range(per):
            place = per * (first + t) + s
            owner, j = lax.div(place, nt), lax.rem(place, nt)
            src = gbuf[layer, j, :, aligned(lax.div(owner, per), LANES)]
            turned = pltpu.roll(src, lax.rem(s - lax.rem(owner, per) + per, per) * WIDTH, 1)
            acc = turned if acc is None else jnp.where(group == s, turned, acc)
        tiles.append(acc)
    return jnp.concatenate(tiles, axis=1)


def state_loads(gu_hbm, gd_hbm, states, gbuf, sbuf, sem):
    loads = []
    for kind, src in enumerate((gu_hbm, gd_hbm)):
        nt = src.shape[0] // 2
        for layer in range(2):
            loads.append(pltpu.make_async_copy(src.at[pl.ds((1 - layer) * nt, nt)], gbuf[kind].at[layer], sem.at[kind, layer, 3]))
            for f in range(3):
                loads.append(pltpu.make_async_copy(states[4 * f + 2 * layer + kind], sbuf[kind].at[layer, f], sem.at[kind, layer, f]))
    return loads


def kernel_update(cfg, part_ref, rate_ref, clip_ref, gu_hbm, gd_hbm, *refs):
    nd, pieces, ru, cu, rd = cfg
    states, (ou1, ou2, od1, od2, norm_ref), (su, sd, gbuf_u, gbuf_d, sbuf_u, sbuf_d, nrecv, insem, nsem, lsem, rsem, ssem, dsem) = refs[:12], refs[12:17], refs[17:]
    me, core, chip, steps = position()
    partner = flip(me, 1)
    IN, O = (su, sd), ((ou1, ou2), (od1, od2))
    layers = range(len(O[0]))
    loads = state_loads(gu_hbm, gd_hbm, states, (gbuf_u, gbuf_d), (sbuf_u, sbuf_d), insem)
    for c in loads:
        c.start()
    meet([lax.rem(me + k, nd) for k in range(1, nd)])
    nrecv[me] = part_ref[...]
    for k in range(1, nd):
        pltpu.make_async_remote_copy(src_ref=part_ref, dst_ref=nrecv.at[me], send_sem=nsem.at[0], recv_sem=nsem.at[1],
                                     device_id=(lax.rem(me + k, nd),), device_id_type=MESH).start()

    def block(kind, first, j, ref):
        if kind == 0:
            return ref.at[pl.ds(pl.multiple_of(first, 8), ru), aligned(j, cu)]
        return ref.at[pl.ds(pl.multiple_of(first + j * rd, 8), rd), :]

    height = (ru, rd * pieces)
    own = [pltpu.make_async_copy(IN[kind].at[w], O[kind][w].at[aligned(me, height[kind]), :], lsem.at[kind, w])
           for kind in range(2) for w in layers]

    def push(kind, p, j, hops, dev, send, recv):
        first = (2 * (chip + relative(hops, p)) + core) * height[kind]
        for w in layers:
            dst = block(kind, first, j, O[kind][w])
            src = dst if p else block(kind, 0, j, IN[kind].at[w])
            pltpu.make_async_remote_copy(src_ref=src, dst_ref=dst, send_sem=send, recv_sem=recv, device_id=(dev,), device_id_type=MESH).start()

    def flag(kind, stage, j):
        return rsem.at[kind, stage, lax.rem(j, AXES * LAG)]

    def spread(kind, stage, j, hops):
        dev = me + 2 * hops[AXES - 1 - stage]
        for p in range(1 << stage):
            push(kind, p, j, hops, dev, ssem.at[kind, stage], flag(kind, stage, j))

    def await_bytes(ref, sem, recv):
        cp = pltpu.make_async_remote_copy(src_ref=ref, dst_ref=ref, send_sem=sem, recv_sem=sem, device_id=(me,), device_id_type=MESH)
        if recv:
            cp.wait_recv()
        else:
            cp.wait_send()

    def arrived(kind, stage, j):
        n = 2 << stage
        part = O[kind][0].at[pl.ds(0, n * ru), pl.ds(0, cu)] if kind == 0 else O[kind][0].at[pl.ds(0, n * rd), :]
        await_bytes(part, flag(kind, stage, j), True)

    for c in loads:
        c.wait()
    others = nrecv.at[pl.ds(0, nd - 1)]
    await_bytes(others, nsem.at[0], False)
    await_bytes(others, nsem.at[1], True)
    total_sq = nrecv[0]
    for k in range(1, nd):
        total_sq = total_sq + nrecv[k]
    norm = jnp.sqrt(jnp.sum(total_sq, keepdims=True))
    norm_ref[...] = jnp.broadcast_to(norm, norm_ref.shape)
    rate, scale = rate_ref[0], clip_scale(norm, clip_ref[0])

    def make(j):
        for w in layers:
            cols = aligned(j, cu)
            grad = natural_columns(gbuf_u, w, j * (cu // LANES), cu // LANES, nd, pieces)
            old = [sbuf_u[w, f, :, cols] for f in range(3)]
            su[w, :, cols] = adam_rows(scale, rate, grad, *old)[0].astype(BF16)
            rows = aligned(j, rd)
            old = [sbuf_d[w, f, rows, :] for f in range(3)]
            sd[w, rows, :] = adam_rows(scale, rate, gbuf_d[w, j], *old)[0].astype(BF16)

    def step(s, _):
        for stage in reversed(range(AXES + 1)):
            j = s - stage * LAG
            @pl.when(jnp.logical_and(j >= 0, j < pieces))
            def _():
                for kind in range(2):
                    hops = [hop(steps, kind, place, j) for place in range(AXES)]
                    if stage:
                        arrived(kind, stage - 1, j)
                    if stage < AXES:
                        spread(kind, stage, j, hops)
                    for p in range((1 << stage) >> 1, 1 << stage):
                        push(kind, p, j, hops, partner, dsem.at[0, kind], dsem.at[1, kind])
        @pl.when(s + AHEAD < pieces)
        def _():
            make(s + AHEAD)
        return 0
    for j in range(AHEAD):
        make(j)
    lax.fori_loop(0, pieces + AXES * LAG, step, 0)
    for c in own:
        c.start()
    for c in own:
        c.wait()
    for kind in range(2):
        full = O[kind][0]
        await_bytes(full, dsem.at[0, kind], False)
        await_bytes(full, dsem.at[1, kind], True)
        for stage in range(AXES):
            await_bytes(full.at[pl.ds(0, (2 << stage) * height[kind]), :], ssem.at[kind, stage], False)


def update(part, rate, clip, gu, gd, states, nd):
    (ru, f), (rf, d) = states[0].shape, states[1].shape
    pieces = gd.shape[0] // 2
    V, D, S = pltpu.VMEM, pltpu.SemaphoreType.DMA, jax.ShapeDtypeStruct
    anyspec, vm, sm = [pl.BlockSpec(memory_space=m) for m in (pl.ANY, pltpu.VMEM, pltpu.SMEM)]
    return pl.pallas_call(
        functools.partial(kernel_update, (nd, pieces, ru, f // pieces, rf // pieces)),
        out_shape=(S((ru * nd, f), BF16),) * 2 + (S((rf * nd, d), BF16),) * 2 + (S((8, LANES), F32),),
        in_specs=[vm, sm, sm] + [HBM] * 14, out_specs=(anyspec,) * 4 + (vm,),
        scratch_shapes=[V((2, ru, f), BF16), V((2, rf, d), BF16), V((2, pieces) + gu.shape[1:], F32), V((2, pieces) + gd.shape[1:], F32),
                        V((2, 3, ru, f), F32), V((2, 3, rf, d), F32), V((nd, 8, LANES), F32),
                        D((2, 2, 4)), D((2,)), D((2, 2)), D((2, AXES, AXES * LAG)), D((2, AXES)), D((2, 2))],
        compiler_params=pltpu.CompilerParams(collective_id=1, has_side_effects=True, vmem_limit_bytes=UPDATE_VMEM),
        name="update")(part, rate, clip, gu, gd, *states)


def kernel_emit(cfg, norm_ref, rate_ref, clip_ref, gu_hbm, gd_hbm, *refs):
    nd, nt = cfg
    weights, states, refs = refs[:4], refs[4:16], refs[16:]
    weights_out, states_out, norm_out = refs[:4], refs[4:16], refs[16]
    gbuf_u, gbuf_d, sbuf_u, sbuf_d, insem, wsem, osem = refs[17:]
    gbuf, sbuf = (gbuf_u, gbuf_d), (sbuf_u, sbuf_d)
    loads = state_loads(gu_hbm, gd_hbm, states, gbuf, sbuf, insem)
    for c in loads:
        c.start()
    copies = []
    for k, (src, dst) in enumerate(zip(weights, weights_out)):
        rows = src.shape[0] // EMIT
        for part in range(EMIT):
            piece = pl.ds(part * rows, rows)
            copies.append(pltpu.make_async_copy(src.at[piece, :], dst.at[piece, :], wsem.at[k, part]))
    for c in copies:
        c.start()
    norm = norm_ref[0:1, 0:1]
    norm_out[...] = norm
    rate, scale = rate_ref[0], clip_scale(norm, clip_ref[0])
    for n, c in enumerate(loads):
        c.wait()
        kind, layer = n // 8, n // 4 % 2
        if n % 4 < 3:
            continue
        def renew(rows, cols, grad):
            old = [sbuf[kind][layer, f, rows, cols] for f in range(3)]
            for f, value in enumerate(adam_rows(scale, rate, grad, *old)):
                sbuf[kind][layer, f, rows, cols] = value
        def body(j, _):
            if kind == 0:
                wide = sbuf_u.shape[3] // nt
                renew(slice(None), aligned(j, wide), natural_columns(gbuf_u, layer, j * (wide // LANES), wide // LANES, nd, nt))
            else:
                renew(aligned(j, gbuf_d.shape[2]), slice(None), gbuf_d[layer, j])
            return 0
        lax.fori_loop(0, nt, body, 0)
        for f in range(3):
            cp = pltpu.make_async_copy(sbuf[kind].at[layer, f], states_out[4 * f + 2 * layer + kind], osem.at[kind, layer, f])
            cp.start()
            copies.append(cp)
    for c in copies:
        c.wait()


def emit(norm, rate, clip, gu, gd, weights, states, nd):
    nt = gu.shape[0] // 2
    up, down = states[0].shape, states[1].shape
    V, D, S = pltpu.VMEM, pltpu.SemaphoreType.DMA, jax.ShapeDtypeStruct
    anyspec, vm, sm = [pl.BlockSpec(memory_space=m) for m in (pl.ANY, pltpu.VMEM, pltpu.SMEM)]
    return pl.pallas_call(
        functools.partial(kernel_emit, (nd, nt)),
        out_shape=[S(a.shape, a.dtype) for a in (*weights, *states)] + [S((1, 1), F32)],
        in_specs=[vm, sm, sm] + [HBM] * 2 + [anyspec] * 4 + [HBM] * 12, out_specs=[HBM] * 16 + [vm],
        scratch_shapes=[V((2, nt) + gu.shape[1:], F32), V((2, nt) + gd.shape[1:], F32), V((2, 3) + up, F32), V((2, 3) + down, F32),
                        D((2, 2, 4)), D((4, EMIT)), D((2, 2, 3))],
        compiler_params=pltpu.CompilerParams(vmem_limit_bytes=EMIT_VMEM), name="emit")(norm, rate, clip, gu, gd, *weights, *states)


def solution(mesh):
    groups = mesh.shape["data"]
    rows_spec = P("data", None)
    full_spec = P(None, None)
    scalar_spec = P()

    def shard_body(act_in, grad_out, w_up1, w_down1, w_up2, w_down2, *rest):
        states, learn_rate, clip_norm = rest[:12], rest[12], rest[13]
        ff, d = w_down1.shape
        down1_tiles = w_down1.reshape(groups, -1, 16, d)
        down2_tiles = w_down2.reshape(groups, -1, 16, d)
        pre1, mid_t, in_t, grad_t, up2_t = forward_one(act_in, grad_out, w_up1, w_up2, down1_tiles)
        up2_tiles = up2_t.reshape(down1_tiles.shape)
        grads_up, grads_down, sq = backward(mid_t, grad_t, in_t, pre1, up2_tiles, down2_tiles, down1_tiles)
        rate, clip = learn_rate.reshape(1), clip_norm.reshape(1)
        states = [pltpu.with_memory_space_constraint(x, pltpu.HBM) for x in states]
        grads_up, grads_down = [pltpu.with_memory_space_constraint(x, pltpu.HBM) for x in (grads_up, grads_down)]
        up1, up2, down1, down2, norm = update(sq, rate, clip, grads_up, grads_down, states, groups)
        *results, norm = emit(norm, rate, clip, grads_up, grads_down, (up1, down1, up2, down2), states, groups)
        return (*results, norm.reshape(()))

    in_specs = (rows_spec, rows_spec) + (full_spec,) * 4 + (rows_spec,) * 12 + (scalar_spec, scalar_spec)
    out_specs = (full_spec,) * 4 + (rows_spec,) * 12 + (scalar_spec,)
    return jax.shard_map(shard_body, mesh=mesh, in_specs=in_specs, out_specs=out_specs, check_vma=False)
```

```python
import functools
import math
import jax
import jax.numpy as jnp
from jax import lax
from jax.experimental import pallas as pl
from jax.experimental.pallas import tpu as pltpu
from jax.sharding import PartitionSpec as P

ROOT_HALF = math.sqrt(0.5)
INV_ROOT_TAU = 1.0 / math.sqrt(2.0 * math.pi)
F32, BF16 = jnp.float32, jnp.bfloat16
HBM = pl.BlockSpec(memory_space=pltpu.HBM)
VMEM_MAX = 64 * 1024 * 1024 - 65536
PAIR = 2
BLOCKS = 8
TURNS = 8
RING = 4
LANES = 128


def dot_nn(a, b):
    return lax.dot_general(a, b, (((1,), (0,)), ((), ())), preferred_element_type=F32)


def dot_nt(a, b):
    return lax.dot_general(a, b, (((1,), (1,)), ((), ())), preferred_element_type=F32)


def gelu(z):
    return z * (0.5 * (1.0 + lax.erf(z * ROOT_HALF)))


def at_most(j, bound):
    return jnp.minimum(j, bound)


def aligned(j, size):
    return pl.ds(pl.multiple_of(j * size, size), size)


def kernel_a(cfg, x_hbm, e_hbm, w1_hbm, w3_hbm, w2_hbm, z_hbm, ut_hbm, xt_hbm, et_hbm, w3t_hbm,
             xt, uacc, zout, w1t_v, w1_in, x_in, w1, w2, w2t, w3_in, w3_out, e_in, e_out, h0, h1,
             wsem, xsem, esem, vsem, zsem, osem):
    nt, nr, rb, tr, tb, ft, d, nd = cfg
    hb = (h0, h1)
    width = ft // nd

    def w1copy(q):
        slot = lax.rem(q, RING)
        return pltpu.make_async_copy(w1_hbm.at[aligned(q, LANES), :], w1_in.at[slot], wsem.at[slot])

    def xcopy(r):
        slot = lax.rem(r, RING)
        return pltpu.make_async_copy(x_hbm.at[aligned(r, tb), :], x_in.at[slot], xsem.at[slot])

    def w2copy(j):
        slot = lax.rem(j, 2)
        return pltpu.make_async_copy(w2_hbm.at[:, j], w2.at[slot], vsem.at[0, slot])

    def w3copy(j):
        slot = lax.rem(j, 2)
        return pltpu.make_async_copy(w3_hbm.at[:, aligned(j, ft)], w3_in.at[slot], vsem.at[1, slot])

    def w3store(j):
        slot = lax.rem(j, 2)
        return pltpu.make_async_copy(w3_out.at[slot], w3t_hbm.at[aligned(j, ft), :], osem.at[0, slot])

    def ecopy(r):
        slot = lax.rem(r, 2)
        return pltpu.make_async_copy(e_hbm.at[aligned(r, tb), :], e_in.at[slot], esem.at[slot])

    def estore(r):
        slot = lax.rem(r, 2)
        return pltpu.make_async_copy(e_out.at[slot], et_hbm.at[:, aligned(r, tb)], osem.at[1, slot])

    def zstore(j):
        slot = lax.rem(j, 2)
        return pltpu.make_async_copy(zout.at[slot], z_hbm.at[j], zsem.at[slot])

    rows_in = d // LANES
    for q in range(min(RING, rows_in)):
        w1copy(q).start()
    for r in range(min(RING, tr)):
        xcopy(r).start()
    for c in (w2copy(0), w3copy(0), ecopy(0)):
        c.start()

    def zero(r, _):
        uacc[:, aligned(r, rb)] = jnp.zeros((d, rb), F32)
        return 0
    lax.fori_loop(0, nr, zero, 0)

    def turn_in(q, _):
        @pl.when(q < rows_in)
        def _():
            w1copy(q).wait()
            w1t_v[:, aligned(q, LANES)] = w1_in[lax.rem(q, RING)].T
        @pl.when(q + RING < rows_in)
        def _():
            w1copy(q + RING).start()
        xcopy(q).wait()
        xt[:, aligned(q, tb)] = x_in[lax.rem(q, RING)].T
        @pl.when(q + RING < tr)
        def _():
            xcopy(q + RING).start()
        return 0
    lax.fori_loop(0, tr, turn_in, 0)
    xt_store = pltpu.make_async_copy(xt, xt_hbm, osem.at[2, 0])
    xt_store.start()

    def pick_w1(j, slot):
        for k in range(nd):
            w1[slot, k * width:(k + 1) * width, :] = w1t_v[aligned(k * nt + j, width), :]
    pick_w1(0, 0)

    def tile(j, _):
        slot = lax.rem(j, 2)
        nslot = 1 - slot
        @pl.when(j >= 2)
        def _():
            zstore(j - 2).wait()
            w3store(j - 2).wait()
        @pl.when(jnp.logical_and(j >= 2, j < tr + 2))
        def _():
            estore(j - 2).wait()
        w2copy(j).wait()
        w3copy(j).wait()
        @pl.when(j < tr)
        def _():
            ecopy(j).wait()
        @pl.when(j + 1 < nt)
        def _():
            w2copy(j + 1).start()
            w3copy(j + 1).start()
        @pl.when(j + 1 < min(tr, nt))
        def _():
            ecopy(j + 1).start()

        def cols(r):
            return pl.ds(r * rb, rb)
        def front(r):
            zout[slot, :, cols(r)] = dot_nn(w1[slot], xt[:, cols(r)])
        def middle(r):
            hb[r % 2][...] = gelu(zout[slot, :, cols(r)]).astype(BF16)
        def back(r):
            uacc[:, cols(r)] += dot_nn(w2t[...], hb[r % 2][...])
        front(0)
        w2t[...] = w2[slot].reshape(ft, d).T
        for r in range(nr):
            middle(r)
            if r + 1 < nr:
                front(r + 1)
            if r >= 1:
                back(r - 1)
            if r == 0:
                pick_w1(at_most(j + 1, nt - 1), nslot)
            if r == 1:
                w3_out[slot] = w3_in[slot].T
            if r == nr - 2:
                e_out[slot] = e_in[slot].T
        back(nr - 1)
        zstore(j).start()
        w3store(j).start()
        @pl.when(j < tr)
        def _():
            estore(j).start()
        return 0
    lax.fori_loop(0, nt, tile, 0)
    xt_store.wait()

    def finish(r, _):
        block = aligned(r, rb)
        xt[:, block] = uacc[:, block].astype(BF16)
        pltpu.make_async_copy(xt.at[:, block], ut_hbm.at[:, block], osem.at[2, 1]).start()
        return 0
    lax.fori_loop(0, nr, finish, 0)
    ut_store = pltpu.make_async_copy(xt, ut_hbm, osem.at[2, 1])
    for j in (nt - 2, nt - 1):
        zstore(j).wait()
        w3store(j).wait()
        if j < tr:
            estore(j).wait()
    for r in range(nt, tr):
        ecopy(r).start()
        ecopy(r).wait()
        e_out[r % 2] = e_in[r % 2].T
        estore(r).start()
        estore(r).wait()
    ut_store.wait()


def forward_one(x, e, w1, w3, w2r):
    t, d = x.shape
    nd, nt, rows2, _ = w2r.shape
    ft, nr, tr = nd * rows2, BLOCKS, TURNS
    rb, tb = t // nr, t // tr
    V, D = pltpu.VMEM, pltpu.SemaphoreType.DMA
    S = jax.ShapeDtypeStruct
    return pl.pallas_call(
        functools.partial(kernel_a, (nt, nr, rb, tr, tb, ft, d, nd)),
        out_shape=(S((nt, ft, t), F32), S((d, t), BF16), S((d, t), BF16), S((d, t), BF16), S((nt * ft, d), BF16)),
        in_specs=[HBM] * 5, out_specs=(HBM,) * 5,
        scratch_shapes=[
            V((d, t), BF16), V((d, t), F32), V((PAIR, ft, t), F32), V((nt * ft, d), BF16), V((RING, LANES, nt * ft), BF16), V((RING, tb, d), BF16),
            V((PAIR, ft, d), BF16), V((PAIR, nd, rows2, d), BF16), V((d, ft), BF16), V((PAIR, d, ft), BF16), V((PAIR, ft, d), BF16),
            V((PAIR, tb, d), BF16), V((PAIR, d, tb), BF16), V((ft, rb), BF16), V((ft, rb), BF16),
            D((RING,)), D((RING,)), D((PAIR,)), D((PAIR, PAIR)), D((PAIR,)), D((3, 2))],
        compiler_params=pltpu.CompilerParams(vmem_limit_bytes=VMEM_MAX),
        name="forward_one",
    )(x, e, w1, w3, w2r)


MESH = pl.DeviceIdType.MESH

def gelu_pair(pre):
    normal_cdf = 0.5 * (1.0 + lax.erf(pre * ROOT_HALF))
    density = jnp.exp(-0.5 * pre * pre) * INV_ROOT_TAU
    return pre * normal_cdf, normal_cdf + pre * density

def flip(value, step):
    return value + step * (1 - 2 * lax.rem(lax.div(value, step), 2))

def position():
    me = lax.axis_index("data")
    chip = lax.div(me, 2)
    steps = [(1 << k) * (1 - 2 * lax.rem(lax.div(chip, 1 << k), 2)) for k in range(AXES)]
    return me, lax.rem(me, 2), chip, steps


def hop(steps, kind, place, j):
    axis = lax.rem(j + ORDERS[kind][place], AXES)
    return steps[0] * lax.div((2 - axis) * (1 - axis), 2) + steps[1] * axis * (2 - axis) + steps[2] * lax.div(axis * (axis - 1), 2)


def relative(hops, p):
    return sum((hops[place] for place in range(AXES) if (p >> (AXES - 1 - place)) & 1), 0)


AXES = 3


def when(condition, fn):
    pl.when(condition)(fn)


def meet(peers):
    barrier = pltpu.get_barrier_semaphore()
    for peer in peers:
        pl.semaphore_signal(barrier, inc=1, device_id=(peer,), device_id_type=MESH)
    pl.semaphore_wait(barrier, len(peers))


ORDERS = ((0, 2, 1), (1, 2, 0))
PARTS = 8
BACK_BLOCKS = 4
BEGUN = 2
TURN = 128
SEEN = (3, 6, 9, 12)
DEPTH = (2, 6, 6, 6)
LAST = len(SEEN) - 1
HOLD = 3

def kernel_bc(cfg, ut_hbm, et_hbm, xt_hbm, z_hbm, w3_hbm, w4_hbm, w2_hbm,
              gu_hbm, gd_hbm, nrm_ref,
              act, side, euacc, wa, wb, wat, zb0, zb1, eb0, eb1, hb0, hb1, qb0, qb1,
              gu, gt, gd, r0u, r0d, a0u, a0d, a1u, a1d, a2u, a2d, r1u, r1d, r2u, r2d, r3u, r3d, fu, fd, nu, nd_acc,
              insem, wsem, zsem, ssem, rsem, fsem):
    nt, nr, nc, t, ft, d, nd = cfg
    rb, rc = t // nr, t // nc
    total = 2 * nt
    me, core, chip, steps = position()
    partner = flip(me, 1)
    zb, eb, hb, qb = (zb0, zb1), (eb0, eb1), (hb0, hb1), (qb0, qb1)
    G, R, ACC, FIN, NRM, OUT = (gu, gd), ((r0u, r1u, r2u, r3u), (r0d, r1d, r2d, r3d)), ((a0u, a1u, a2u), (a0d, a1d, a2d)), (fu, fd), (nu, nd_acc), (gu_hbm, gd_hbm)

    loads = [pltpu.make_async_copy(ut_hbm, act, insem.at[0]), pltpu.make_async_copy(et_hbm, side, insem.at[1])]
    for c in loads:
        c.start()

    def wcopies(j, slot, back):
        second = w2_hbm if back else w4_hbm
        cps = [pltpu.make_async_copy(second.at[:, j], wb.at[slot], wsem.at[1, slot])]
        if not back:
            cps.append(pltpu.make_async_copy(w3_hbm.at[:, j], wa.at[slot], wsem.at[0, slot]))
        return cps
    for c in wcopies(0, 0, False):
        c.start()

    meet([partner] + [me + 2 * s for s in steps])

    nu[...] = jnp.zeros_like(nu)
    nd_acc[...] = jnp.zeros_like(nd_acc)
    gt[1] = jnp.zeros_like(gt[1])
    def zero(r, _):
        euacc[:, aligned(r, rb)] = jnp.zeros((d, rb), F32)
        return 0
    lax.fori_loop(0, nr, zero, 0)

    def send(kind, stage, j):
        depth = R[kind][stage].shape[0]
        slot = lax.rem(j, depth)
        sem = (kind * len(SEEN) + stage) * max(DEPTH) + slot
        dst = R[kind][stage].at[slot]
        if stage == 0:
            src, dev = G[kind].at[lax.rem(j, G[kind].shape[0]), :, 1 - core], partner
        else:
            lo = PARTS >> stage
            src, dev = ACC[kind][stage - 1].at[lax.rem(j, HOLD), pl.ds(lo, lo)], me + 2 * hop(steps, kind, stage - 1, j)
        return pltpu.make_async_remote_copy(src_ref=src, dst_ref=dst, send_sem=ssem.at[sem], recv_sem=rsem.at[sem],
                                            device_id=(dev,), device_id_type=MESH)

    def final_copy(kind, j):
        slot = lax.rem(j, 2)
        return pltpu.make_async_copy(FIN[kind].at[slot], OUT[kind].at[j], fsem.at[kind, slot])

    def absorb(stage, j):
        place = lax.rem(j, HOLD)
        for kind in range(2):
            send(kind, stage, j).wait()
            slot = lax.rem(j, R[kind][stage].shape[0])
            got, acc = R[kind][stage], ACC[kind]
            if stage == 0:
                hops = [hop(steps, kind, place, j) for place in range(AXES)]
                for p in range(PARTS):
                    oc = chip + relative(hops, p)
                    acc[0][place, p] = G[kind][lax.rem(j, G[kind].shape[0]), oc, core] + got[slot, oc]
                continue
            kept = acc[stage - 1][place, 0:PARTS >> stage] + got[slot]
            if stage < LAST:
                acc[stage][place] = kept
            else:
                when(j >= 2, final_copy(kind, j - 2).wait)
                f = kept[0] * (1.0 / nd)
                FIN[kind][lax.rem(j, 2)] = f
                NRM[kind][...] += f * f
        for kind in range(2):
            (send(kind, stage + 1, j) if stage < LAST else final_copy(kind, j)).start()

    def comm(step):
        def due(j, fn):
            when(jnp.logical_and(j >= 0, j < total), fn)
        for stage in reversed(range(len(SEEN))):
            j = step - SEEN[stage]
            due(j, functools.partial(absorb, stage, j))
        def start():
            for kind in range(2):
                send(kind, 0, step - BEGUN).start()
        due(step - BEGUN, start)

    def turn(step, part):
        slot = lax.rem(step + 1, 2)
        lanes = pl.ds(part * TURN, TURN)
        gd[slot, :, :, :, lanes] = gt[slot, lanes, :].T.reshape(gd.shape[1:-1] + (TURN,))

    def add_up(step, r, value):
        slot, value = lax.rem(step, gu.shape[0]), value.reshape(gu.shape[1:])
        gu[slot] = value if r == 0 else gu[slot] + value

    def add_down(step, r, value):
        slot = lax.rem(step, 2)
        gt[slot] = value if r == 0 else gt[slot] + value

    def gates(r, width, pre):
        h, der = gelu_pair(pre)
        lanes = pl.ds(0, width)
        hb[r % 2][:, lanes] = h.astype(BF16)
        qb[r % 2][:, lanes] = (eb[r % 2][:, lanes].astype(F32) * der).astype(BF16)

    def pipeline(step, blocks, front, middle, back):
        front(0)
        for r in range(blocks):
            middle(r)
            if r + 1 < blocks:
                front(r + 1)
            if r >= 1:
                back(r - 1)
            for part in range(r, d // TURN, blocks):
                turn(step, part)
        back(blocks - 1)

    for c in loads:
        c.wait()

    def tile_b(j, _):
        slot = lax.rem(j, 2)
        comm(j)
        for c in wcopies(j, slot, False):
            c.wait()
        @pl.when(j + 1 < nt)
        def _():
            for c in wcopies(j + 1, 1 - slot, False):
                c.start()
        def cols(r):
            return pl.ds(r * rb, rb)
        mine = pl.ds(0, rb)
        def front(r):
            zb[r % 2][...] = dot_nn(wa[slot].reshape(ft, d), act[:, cols(r)])
            eb[r % 2][:, mine] = dot_nn(wb[slot].reshape(ft, d), side[:, cols(r)]).astype(BF16)
            if r == 0:
                wat[...] = wa[slot].reshape(ft, d).T
        def middle(r):
            gates(r, rb, zb[r % 2][...])
        def back(r):
            q = qb[r % 2][:, mine]
            add_up(j, r, dot_nt(act[:, cols(r)], q))
            add_down(j, r, dot_nt(side[:, cols(r)], hb[r % 2][:, mine]))
            euacc[:, cols(r)] += dot_nn(wat[...], q)
        pipeline(j, nr, front, middle, back)
        return 0
    lax.fori_loop(0, nt, tile_b, 0)

    xt_in = pltpu.make_async_copy(xt_hbm, side, insem.at[1])
    xt_in.start()
    for c in wcopies(0, nt % 2, True):
        c.start()
    def cast(r, _):
        act[:, aligned(r, rb)] = euacc[:, aligned(r, rb)].astype(BF16)
        return 0
    lax.fori_loop(0, nr, cast, 0)
    def zcopy(j, slot):
        return pltpu.make_async_copy(z_hbm.at[j], euacc.at[aligned(slot, ft), :], zsem.at[slot])
    zcopy(0, nt % 2).start()
    xt_in.wait()

    def tile_c(step, _):
        j = step - nt
        slot = lax.rem(step, 2)
        comm(step)
        for c in wcopies(j, slot, True):
            c.wait()
        zcopy(j, slot).wait()
        @pl.when(j + 1 < nt)
        def _():
            for c in wcopies(j + 1, 1 - slot, True):
                c.start()
            zcopy(j + 1, 1 - slot).start()
        def cols(r):
            return pl.ds(r * rc, rc)
        mine = pl.ds(0, rc)
        def front(r):
            eb[r % 2][:, mine] = dot_nn(wb[slot].reshape(ft, d), act[:, cols(r)]).astype(BF16)
        def middle(r):
            gates(r, rc, euacc[aligned(slot, ft), cols(r)])
        def back(r):
            add_down(step, r, dot_nt(act[:, cols(r)], hb[r % 2][:, mine]))
            add_up(step, r, dot_nt(side[:, cols(r)], qb[r % 2][:, mine]))
        pipeline(step, nc, front, middle, back)
        return 0
    lax.fori_loop(nt, total, tile_c, 0)

    def drain(step, _):
        comm(step)
        @pl.when(step == total)
        def _():
            for part in range(d // TURN):
                turn(step, part)
        return 0
    lax.fori_loop(total, total + SEEN[LAST], drain, 0)
    for kind in range(2):
        for j in (total - 2, total - 1):
            final_copy(kind, j).wait()

    part = jnp.zeros((8, 128), F32)
    for ref in (nu, nd_acc):
        rows, cols = ref.shape
        for a in range(rows // 8):
            for b in range(cols // 128):
                part = part + ref[8 * a:8 * a + 8, 128 * b:128 * b + 128]
    nrm_ref[...] = part


def backward(ut, et, xt, z, w3r, w4r, w2r):
    d, t = ut.shape
    nd, nt, rows2, _ = w4r.shape
    ft, nr, nc = nd * rows2, BACK_BLOCKS, BACK_BLOCKS // 2
    rb, rc = t // nr, t // nc
    bu, bd = (d // nd, ft), (rows2, d)
    V, D = pltpu.VMEM, pltpu.SemaphoreType.DMA
    S = jax.ShapeDtypeStruct
    scratch = [V((d, t), BF16)] * 2 + [V((d, t), F32)] + [V((PAIR, nd, rows2, d), BF16)] * 2 + [V((d, ft), BF16)]
    scratch += [V((ft, rb), F32)] * 2 + [V((ft, rc), BF16)] * 6
    scratch += [V((3, PARTS, 2) + bu, F32), V((PAIR, d, ft), F32), V((PAIR, PARTS, 2) + bd, F32)]
    for n, c in [(DEPTH[0], PARTS)] + [(HOLD, PARTS >> k) for k in range(LAST)] + [(DEPTH[k], PARTS >> k) for k in range(1, LAST + 1)]:
        scratch += [V((n, c) + bu, F32), V((n, c) + bd, F32)]
    scratch += [V((PAIR,) + bu, F32), V((PAIR,) + bd, F32), V(bu, F32), V(bd, F32)]
    flags = 2 * len(SEEN) * max(DEPTH)
    scratch += [D((PAIR,)), D((PAIR, PAIR)), D((PAIR,)), D((flags,)), D((flags,)), D((PAIR, PAIR))]
    return pl.pallas_call(
        functools.partial(kernel_bc, (nt, nr, nc, t, ft, d, nd)),
        out_shape=(S((2 * nt,) + bu, F32), S((2 * nt,) + bd, F32), S((8, 128), F32)),
        in_specs=[HBM] * 7, out_specs=(HBM, HBM, pl.BlockSpec(memory_space=pltpu.VMEM)),
        scratch_shapes=scratch,
        compiler_params=pltpu.CompilerParams(collective_id=0, has_side_effects=True, vmem_limit_bytes=VMEM_MAX),
        name="backward",
    )(ut, et, xt, z, w3r, w4r, w2r)


STEP = 20
BETA_ONE = 0.9
BETA_TWO = 0.95
EPSILON = 1e-8
NORM_EPS = 1e-6
CORR_ONE = 1.0 - BETA_ONE ** STEP
CORR_TWO = 1.0 - BETA_TWO ** STEP
WIDTH = 16
LAG = 2
AHEAD = 2
EMIT = 4
UPDATE_VMEM = 19 * 1024 * 1024 + 256 * 1024
EMIT_VMEM = 17 * 1024 * 1024


def clip_scale(norm, clip):
    return jnp.minimum(1.0, clip / (norm + NORM_EPS))


def adam_rows(scale, rate, grad, master, mom, vel):
    scaled = scale * grad
    mom = BETA_ONE * mom + (1.0 - BETA_ONE) * scaled
    vel = BETA_TWO * vel + (1.0 - BETA_TWO) * scaled * scaled
    master = master - rate * (mom * (1.0 / CORR_ONE)) / (jnp.sqrt(vel * (1.0 / CORR_TWO)) + EPSILON)
    return master, mom, vel


def natural_columns(gbuf, layer, first, count, nd, nt):
    rows, per = gbuf.shape[2], LANES // WIDTH
    group = lax.broadcasted_iota(jnp.int32, (rows, LANES), 1) // WIDTH
    tiles = []
    for t in range(count):
        acc = None
        for s in range(per):
            place = per * (first + t) + s
            owner, j = lax.div(place, nt), lax.rem(place, nt)
            src = gbuf[layer, j, :, aligned(lax.div(owner, per), LANES)]
            turned = pltpu.roll(src, lax.rem(s - lax.rem(owner, per) + per, per) * WIDTH, 1)
            acc = turned if acc is None else jnp.where(group == s, turned, acc)
        tiles.append(acc)
    return jnp.concatenate(tiles, axis=1)


def state_loads(gu_hbm, gd_hbm, states, gbuf, sbuf, sem, lo, hi):
    loads = []
    for kind, src in enumerate((gu_hbm, gd_hbm)):
        nt, size = src.shape[0] // 2, src.shape[2] if kind == 0 else src.shape[1]
        part = pl.ds(lo * size, (hi - lo) * size)
        for layer in range(2):
            first, count = (lo, hi - lo) if kind else (0, nt if lo == 0 else 0)
            if count:
                loads.append(pltpu.make_async_copy(src.at[pl.ds((1 - layer) * nt + first, count)], gbuf[kind].at[layer, pl.ds(first, count)],
                                                   sem.at[kind, layer, 3]))
            for f in range(3):
                whole, mine = states[4 * f + 2 * layer + kind], sbuf[kind].at[layer, f]
                pair = (whole.at[:, part], mine.at[:, part]) if kind == 0 else (whole.at[part, :], mine.at[part, :])
                loads.append(pltpu.make_async_copy(*pair, sem.at[kind, layer, f]))
    return loads


def kernel_update(cfg, part_hbm, rate_ref, clip_ref, gu_hbm, gd_hbm, *refs):
    nd, pieces, ru, cu, rd = cfg
    states, (ou1, ou2, od1, od2, norm_ref), (su, sd, gbuf_u, gbuf_d, sbuf_u, sbuf_d, nrecv, insem, nsem, lsem, rsem, ssem, dsem) = refs[:12], refs[12:17], refs[17:]
    me, core, chip, steps = position()
    partner = flip(me, 1)
    IN, O = (su, sd), ((ou1, ou2), (od1, od2))
    layers = range(len(O[0]))
    loads = [state_loads(gu_hbm, gd_hbm, states, (gbuf_u, gbuf_d), (sbuf_u, sbuf_d), insem.at[n], *span)
             for n, span in enumerate(((0, AHEAD), (AHEAD, pieces)))]
    keep = pltpu.make_async_copy(part_hbm, nrecv.at[me], nsem.at[2])
    for c in (keep, *loads[0], *loads[1]):
        c.start()
    meet([lax.rem(me + k, nd) for k in range(1, nd)])
    for k in range(1, nd):
        pltpu.make_async_remote_copy(src_ref=part_hbm, dst_ref=nrecv.at[me], send_sem=nsem.at[0], recv_sem=nsem.at[1],
                                     device_id=(lax.rem(me + k, nd),), device_id_type=MESH).start()

    def block(kind, first, j, ref):
        if kind == 0:
            return ref.at[pl.ds(pl.multiple_of(first, 8), ru), aligned(j, cu)]
        return ref.at[pl.ds(pl.multiple_of(first + j * rd, 8), rd), :]

    height = (ru, rd * pieces)
    own = [pltpu.make_async_copy(IN[kind].at[w], O[kind][w].at[aligned(me, height[kind]), :], lsem.at[kind, w])
           for kind in range(2) for w in layers]

    def push(kind, p, j, hops, dev, send, recv):
        first = (2 * (chip + relative(hops, p)) + core) * height[kind]
        for w in layers:
            dst = block(kind, first, j, O[kind][w])
            src = dst if p else block(kind, 0, j, IN[kind].at[w])
            pltpu.make_async_remote_copy(src_ref=src, dst_ref=dst, send_sem=send, recv_sem=recv, device_id=(dev,), device_id_type=MESH).start()

    def flag(kind, stage, j):
        return rsem.at[kind, stage, lax.rem(j, AXES * LAG)]

    def spread(kind, stage, j, hops):
        dev = me + 2 * hops[AXES - 1 - stage]
        for p in range(1 << stage):
            push(kind, p, j, hops, dev, ssem.at[kind, stage], flag(kind, stage, j))

    def await_bytes(ref, sem, recv):
        cp = pltpu.make_async_remote_copy(src_ref=ref, dst_ref=ref, send_sem=sem, recv_sem=sem, device_id=(me,), device_id_type=MESH)
        if recv:
            cp.wait_recv()
        else:
            cp.wait_send()

    def arrived(kind, stage, j):
        n = 2 << stage
        part = O[kind][0].at[pl.ds(0, n * ru), pl.ds(0, cu)] if kind == 0 else O[kind][0].at[pl.ds(0, n * rd), :]
        await_bytes(part, flag(kind, stage, j), True)

    keep.wait()
    others = nrecv.at[pl.ds(0, nd - 1)]
    await_bytes(others, nsem.at[0], False)
    await_bytes(others, nsem.at[1], True)
    total_sq = nrecv[0]
    for k in range(1, nd):
        total_sq = total_sq + nrecv[k]
    norm = jnp.sqrt(jnp.sum(total_sq, keepdims=True))
    norm_ref[...] = jnp.broadcast_to(norm, norm_ref.shape)
    rate, scale = rate_ref[0], clip_scale(norm, clip_ref[0])

    def make(j):
        for w in layers:
            cols = aligned(j, cu)
            grad = natural_columns(gbuf_u, w, j * (cu // LANES), cu // LANES, nd, pieces)
            old = [sbuf_u[w, f, :, cols] for f in range(3)]
            su[w, :, cols] = adam_rows(scale, rate, grad, *old)[0].astype(BF16)
            rows = aligned(j, rd)
            old = [sbuf_d[w, f, rows, :] for f in range(3)]
            sd[w, rows, :] = adam_rows(scale, rate, gbuf_d[w, j], *old)[0].astype(BF16)

    def step(s, _):
        for stage in reversed(range(AXES + 1)):
            j = s - stage * LAG
            @pl.when(jnp.logical_and(j >= 0, j < pieces))
            def _():
                for kind in range(2):
                    hops = [hop(steps, kind, place, j) for place in range(AXES)]
                    if stage:
                        arrived(kind, stage - 1, j)
                    if stage < AXES:
                        spread(kind, stage, j, hops)
                    for p in range((1 << stage) >> 1, 1 << stage):
                        push(kind, p, j, hops, partner, dsem.at[0, kind], dsem.at[1, kind])
        @pl.when(s + AHEAD < pieces)
        def _():
            make(s + AHEAD)
        return 0
    for c in loads[0]:
        c.wait()
    for j in range(AHEAD):
        make(j)
    for c in loads[1]:
        c.wait()
    lax.fori_loop(0, pieces + AXES * LAG, step, 0)
    for c in own:
        c.start()
    for c in own:
        c.wait()
    for kind in range(2):
        full = O[kind][0]
        await_bytes(full, dsem.at[0, kind], False)
        await_bytes(full, dsem.at[1, kind], True)
        for stage in range(AXES):
            await_bytes(full.at[pl.ds(0, (2 << stage) * height[kind]), :], ssem.at[kind, stage], False)


def update(part, rate, clip, gu, gd, states, nd):
    (ru, f), (rf, d) = states[0].shape, states[1].shape
    pieces = gd.shape[0] // 2
    V, D, S = pltpu.VMEM, pltpu.SemaphoreType.DMA, jax.ShapeDtypeStruct
    anyspec, vm, sm = [pl.BlockSpec(memory_space=m) for m in (pl.ANY, pltpu.VMEM, pltpu.SMEM)]
    return pl.pallas_call(
        functools.partial(kernel_update, (nd, pieces, ru, f // pieces, rf // pieces)),
        out_shape=(S((ru * nd, f), BF16),) * 2 + (S((rf * nd, d), BF16),) * 2 + (S((8, LANES), F32),),
        in_specs=[HBM, sm, sm] + [HBM] * 14, out_specs=(anyspec,) * 4 + (vm,),
        scratch_shapes=[V((PAIR, ru, f), BF16), V((PAIR, rf, d), BF16), V((PAIR, pieces) + gu.shape[1:], F32), V((PAIR, pieces) + gd.shape[1:], F32),
                        V((PAIR, 3, ru, f), F32), V((PAIR, 3, rf, d), F32), V((nd, 8, LANES), F32),
                        D((2, 2, 2, 4)), D((3,)), D((PAIR, PAIR)), D((2, AXES, AXES * LAG)), D((2, AXES)), D((PAIR, PAIR))],
        compiler_params=pltpu.CompilerParams(collective_id=1, has_side_effects=True, vmem_limit_bytes=UPDATE_VMEM),
        name="update")(part, rate, clip, gu, gd, *states)


def kernel_emit(cfg, norm_ref, rate_ref, clip_ref, gu_hbm, gd_hbm, *refs):
    nd, nt = cfg
    weights, states, refs = refs[:4], refs[4:16], refs[16:]
    weights_out, states_out, norm_out = refs[:4], refs[4:16], refs[16]
    gbuf_u, gbuf_d, sbuf_u, sbuf_d, insem, wsem, osem = refs[17:]
    gbuf, sbuf = (gbuf_u, gbuf_d), (sbuf_u, sbuf_d)
    loads = state_loads(gu_hbm, gd_hbm, states, gbuf, sbuf, insem, 0, nt)
    for c in loads:
        c.start()
    copies = []
    for k, (src, dst) in enumerate(zip(weights, weights_out)):
        rows = src.shape[0] // EMIT
        for part in range(EMIT):
            piece = pl.ds(part * rows, rows)
            copies.append(pltpu.make_async_copy(src.at[piece, :], dst.at[piece, :], wsem.at[k, part]))
    for c in copies:
        c.start()
    norm = norm_ref[0:1, 0:1]
    norm_out[...] = norm
    rate, scale = rate_ref[0], clip_scale(norm, clip_ref[0])
    for n, c in enumerate(loads):
        c.wait()
        kind, layer = n // 8, n // 4 % 2
        if n % 4 < 3:
            continue
        def renew(rows, cols, grad):
            old = [sbuf[kind][layer, f, rows, cols] for f in range(3)]
            for f, value in enumerate(adam_rows(scale, rate, grad, *old)):
                sbuf[kind][layer, f, rows, cols] = value
        def body(j, _):
            if kind == 0:
                wide = sbuf_u.shape[3] // nt
                renew(slice(None), aligned(j, wide), natural_columns(gbuf_u, layer, j * (wide // LANES), wide // LANES, nd, nt))
            else:
                renew(aligned(j, gbuf_d.shape[2]), slice(None), gbuf_d[layer, j])
            return 0
        lax.fori_loop(0, nt, body, 0)
        for f in range(3):
            cp = pltpu.make_async_copy(sbuf[kind].at[layer, f], states_out[4 * f + 2 * layer + kind], osem.at[kind, layer, f])
            cp.start()
            copies.append(cp)
    for c in copies:
        c.wait()


def emit(norm, rate, clip, gu, gd, weights, states, nd):
    nt = gu.shape[0] // 2
    up, down = states[0].shape, states[1].shape
    V, D, S = pltpu.VMEM, pltpu.SemaphoreType.DMA, jax.ShapeDtypeStruct
    anyspec, vm, sm = [pl.BlockSpec(memory_space=m) for m in (pl.ANY, pltpu.VMEM, pltpu.SMEM)]
    return pl.pallas_call(
        functools.partial(kernel_emit, (nd, nt)),
        out_shape=[S(a.shape, a.dtype) for a in (*weights, *states)] + [S((1, 1), F32)],
        in_specs=[vm, sm, sm] + [HBM] * 2 + [anyspec] * 4 + [HBM] * 12, out_specs=[HBM] * 16 + [vm],
        scratch_shapes=[V((PAIR, nt) + gu.shape[1:], F32), V((PAIR, nt) + gd.shape[1:], F32), V((PAIR, 3) + up, F32), V((PAIR, 3) + down, F32),
                        D((2, 2, 4)), D((4, EMIT)), D((2, 2, 3))],
        compiler_params=pltpu.CompilerParams(vmem_limit_bytes=EMIT_VMEM), name="emit")(norm, rate, clip, gu, gd, *weights, *states)


def solution(mesh):
    groups = mesh.shape["data"]
    rows_spec = P("data", None)
    full_spec = P(None, None)
    scalar_spec = P()

    def shard_body(act_in, grad_out, w_up1, w_down1, w_up2, w_down2, *rest):
        states, learn_rate, clip_norm = rest[:12], rest[12], rest[13]
        ff, d = w_down1.shape
        down1_tiles = w_down1.reshape(groups, -1, 16, d)
        down2_tiles = w_down2.reshape(groups, -1, 16, d)
        pre1, mid_t, in_t, grad_t, up2_t = forward_one(act_in, grad_out, w_up1, w_up2, down1_tiles)
        up2_tiles = up2_t.reshape(down1_tiles.shape)
        grads_up, grads_down, sq = backward(mid_t, grad_t, in_t, pre1, up2_tiles, down2_tiles, down1_tiles)
        rate, clip = learn_rate.reshape(1), clip_norm.reshape(1)
        states = [pltpu.with_memory_space_constraint(x, pltpu.HBM) for x in states]
        sq, grads_up, grads_down = [pltpu.with_memory_space_constraint(x, pltpu.HBM) for x in (sq, grads_up, grads_down)]
        up1, up2, down1, down2, norm = update(sq, rate, clip, grads_up, grads_down, states, groups)
        *results, norm = emit(norm, rate, clip, grads_up, grads_down, (up1, down1, up2, down2), states, groups)
        return (*results, norm.reshape(()))

    in_specs = (rows_spec, rows_spec) + (full_spec,) * 4 + (rows_spec,) * 12 + (scalar_spec, scalar_spec)
    out_specs = (full_spec,) * 4 + (rows_spec,) * 12 + (scalar_spec,)
    return jax.shard_map(shard_body, mesh=mesh, in_specs=in_specs, out_specs=out_specs, check_vma=False)
```

```python
import functools
import math
import jax
import jax.numpy as jnp
from jax import lax
from jax.experimental import pallas as pl
from jax.experimental.pallas import tpu as pltpu
from jax.sharding import PartitionSpec as P

ROOT_HALF = math.sqrt(0.5)
INV_ROOT_TAU = 1.0 / math.sqrt(2.0 * math.pi)
F32, BF16 = jnp.float32, jnp.bfloat16
HBM = pl.BlockSpec(memory_space=pltpu.HBM)
VMEM_MAX = 64 * 1024 * 1024 - 65536
PAIR = 2
BLOCKS = 8
TURNS = 8
RING = 4
LANES = 128


def dot_nn(a, b):
    return lax.dot_general(a, b, (((1,), (0,)), ((), ())), preferred_element_type=F32)


def dot_nt(a, b):
    return lax.dot_general(a, b, (((1,), (1,)), ((), ())), preferred_element_type=F32)


def gelu(z):
    return z * (0.5 * (1.0 + lax.erf(z * ROOT_HALF)))


def at_most(j, bound):
    return jnp.minimum(j, bound)


def aligned(j, size):
    return pl.ds(pl.multiple_of(j * size, size), size)


def kernel_a(cfg, x_hbm, e_hbm, w1_hbm, w3_hbm, w2_hbm, z_hbm, ut_hbm, xt_hbm, et_hbm, w3t_hbm,
             xt, uacc, zout, w1t_v, w1_in, x_in, w1, w2, w2t, w3_in, w3_out, e_in, e_out, h0, h1,
             wsem, xsem, esem, vsem, zsem, osem):
    nt, nr, rb, tr, tb, ft, d, nd = cfg
    hb = (h0, h1)
    width = ft // nd

    def w1copy(q):
        slot = lax.rem(q, RING)
        return pltpu.make_async_copy(w1_hbm.at[aligned(q, LANES), :], w1_in.at[slot], wsem.at[slot])

    def xcopy(r):
        slot = lax.rem(r, RING)
        return pltpu.make_async_copy(x_hbm.at[aligned(r, tb), :], x_in.at[slot], xsem.at[slot])

    def w2copy(j):
        slot = lax.rem(j, 2)
        return pltpu.make_async_copy(w2_hbm.at[:, j], w2.at[slot], vsem.at[0, slot])

    def w3copy(j):
        slot = lax.rem(j, 2)
        return pltpu.make_async_copy(w3_hbm.at[:, aligned(j, ft)], w3_in.at[slot], vsem.at[1, slot])

    def w3store(j):
        slot = lax.rem(j, 2)
        return pltpu.make_async_copy(w3_out.at[slot], w3t_hbm.at[aligned(j, ft), :], osem.at[0, slot])

    def ecopy(r):
        slot = lax.rem(r, 2)
        return pltpu.make_async_copy(e_hbm.at[aligned(r, tb), :], e_in.at[slot], esem.at[slot])

    def estore(r):
        slot = lax.rem(r, 2)
        return pltpu.make_async_copy(e_out.at[slot], et_hbm.at[:, aligned(r, tb)], osem.at[1, slot])

    def zstore(j):
        slot = lax.rem(j, 2)
        return pltpu.make_async_copy(zout.at[slot], z_hbm.at[j], zsem.at[slot])

    rows_in = d // LANES
    for q in range(min(RING, rows_in)):
        w1copy(q).start()
    for r in range(min(RING, tr)):
        xcopy(r).start()
    for c in (w2copy(0), w3copy(0), ecopy(0)):
        c.start()

    def zero(r, _):
        uacc[:, aligned(r, rb)] = jnp.zeros((d, rb), F32)
        return 0
    lax.fori_loop(0, nr, zero, 0)

    def turn_in(q, _):
        @pl.when(q < rows_in)
        def _():
            w1copy(q).wait()
            w1t_v[:, aligned(q, LANES)] = w1_in[lax.rem(q, RING)].T
        @pl.when(q + RING < rows_in)
        def _():
            w1copy(q + RING).start()
        xcopy(q).wait()
        xt[:, aligned(q, tb)] = x_in[lax.rem(q, RING)].T
        @pl.when(q + RING < tr)
        def _():
            xcopy(q + RING).start()
        return 0
    lax.fori_loop(0, tr, turn_in, 0)
    xt_store = pltpu.make_async_copy(xt, xt_hbm, osem.at[2, 0])
    xt_store.start()

    def pick_w1(j, slot):
        for k in range(nd):
            w1[slot, k * width:(k + 1) * width, :] = w1t_v[aligned(k * nt + j, width), :]
    pick_w1(0, 0)

    def tile(j, _):
        slot = lax.rem(j, 2)
        nslot = 1 - slot
        @pl.when(j >= 2)
        def _():
            zstore(j - 2).wait()
            w3store(j - 2).wait()
        @pl.when(jnp.logical_and(j >= 2, j < tr + 2))
        def _():
            estore(j - 2).wait()
        w2copy(j).wait()
        w3copy(j).wait()
        @pl.when(j < tr)
        def _():
            ecopy(j).wait()
        @pl.when(j + 1 < nt)
        def _():
            w2copy(j + 1).start()
            w3copy(j + 1).start()
        @pl.when(j + 1 < min(tr, nt))
        def _():
            ecopy(j + 1).start()

        def cols(r):
            return pl.ds(r * rb, rb)
        def front(r):
            zout[slot, :, cols(r)] = dot_nn(w1[slot], xt[:, cols(r)])
        def middle(r):
            hb[r % 2][...] = gelu(zout[slot, :, cols(r)]).astype(BF16)
        def back(r):
            uacc[:, cols(r)] += dot_nn(w2t[...], hb[r % 2][...])
        front(0)
        w2t[...] = w2[slot].reshape(ft, d).T
        for r in range(nr):
            middle(r)
            if r + 1 < nr:
                front(r + 1)
            if r >= 1:
                back(r - 1)
            if r == 0:
                pick_w1(at_most(j + 1, nt - 1), nslot)
            if r == 1:
                w3_out[slot] = w3_in[slot].T
            if r == nr - 2:
                e_out[slot] = e_in[slot].T
        back(nr - 1)
        zstore(j).start()
        w3store(j).start()
        @pl.when(j < tr)
        def _():
            estore(j).start()
        return 0
    lax.fori_loop(0, nt, tile, 0)
    xt_store.wait()

    def finish(r, _):
        block = aligned(r, rb)
        xt[:, block] = uacc[:, block].astype(BF16)
        pltpu.make_async_copy(xt.at[:, block], ut_hbm.at[:, block], osem.at[2, 1]).start()
        return 0
    lax.fori_loop(0, nr, finish, 0)
    ut_store = pltpu.make_async_copy(xt, ut_hbm, osem.at[2, 1])
    for j in (nt - 2, nt - 1):
        zstore(j).wait()
        w3store(j).wait()
        if j < tr:
            estore(j).wait()
    for r in range(nt, tr):
        ecopy(r).start()
        ecopy(r).wait()
        e_out[r % 2] = e_in[r % 2].T
        estore(r).start()
        estore(r).wait()
    ut_store.wait()


def forward_one(x, e, w1, w3, w2r):
    t, d = x.shape
    nd, nt, rows2, _ = w2r.shape
    ft, nr, tr = nd * rows2, BLOCKS, TURNS
    rb, tb = t // nr, t // tr
    V, D = pltpu.VMEM, pltpu.SemaphoreType.DMA
    S = jax.ShapeDtypeStruct
    return pl.pallas_call(
        functools.partial(kernel_a, (nt, nr, rb, tr, tb, ft, d, nd)),
        out_shape=(S((nt, ft, t), F32), S((d, t), BF16), S((d, t), BF16), S((d, t), BF16), S((nt * ft, d), BF16)),
        in_specs=[HBM] * 5, out_specs=(HBM,) * 5,
        scratch_shapes=[
            V((d, t), BF16), V((d, t), F32), V((PAIR, ft, t), F32), V((nt * ft, d), BF16), V((RING, LANES, nt * ft), BF16), V((RING, tb, d), BF16),
            V((PAIR, ft, d), BF16), V((PAIR, nd, rows2, d), BF16), V((d, ft), BF16), V((PAIR, d, ft), BF16), V((PAIR, ft, d), BF16),
            V((PAIR, tb, d), BF16), V((PAIR, d, tb), BF16), V((ft, rb), BF16), V((ft, rb), BF16),
            D((RING,)), D((RING,)), D((PAIR,)), D((PAIR, PAIR)), D((PAIR,)), D((3, 2))],
        compiler_params=pltpu.CompilerParams(vmem_limit_bytes=VMEM_MAX),
        name="forward_one",
    )(x, e, w1, w3, w2r)


MESH = pl.DeviceIdType.MESH

def gelu_pair(pre):
    normal_cdf = 0.5 * (1.0 + lax.erf(pre * ROOT_HALF))
    density = jnp.exp(-0.5 * pre * pre) * INV_ROOT_TAU
    return pre * normal_cdf, normal_cdf + pre * density

def flip(value, step):
    return value + step * (1 - 2 * lax.rem(lax.div(value, step), 2))

def position():
    me = lax.axis_index("data")
    chip = lax.div(me, 2)
    steps = [(1 << k) * (1 - 2 * lax.rem(lax.div(chip, 1 << k), 2)) for k in range(AXES)]
    return me, lax.rem(me, 2), chip, steps


def hop(steps, kind, place, j):
    axis = lax.rem(j + ORDERS[kind][place], AXES)
    return steps[0] * lax.div((2 - axis) * (1 - axis), 2) + steps[1] * axis * (2 - axis) + steps[2] * lax.div(axis * (axis - 1), 2)


def relative(hops, p):
    return sum((hops[place] for place in range(AXES) if (p >> (AXES - 1 - place)) & 1), 0)


AXES = 3


def when(condition, fn):
    pl.when(condition)(fn)


def meet(peers):
    barrier = pltpu.get_barrier_semaphore()
    for peer in peers:
        pl.semaphore_signal(barrier, inc=1, device_id=(peer,), device_id_type=MESH)
    pl.semaphore_wait(barrier, len(peers))


ORDERS = ((0, 2, 1), (1, 2, 0))
PARTS = 8
BACK_BLOCKS = 4
BEGUN = 2
TURN = 128
SEEN = (3, 6, 9, 12)
DEPTH = (2, 6, 6, 6)
LAST = len(SEEN) - 1
HOLD = 3

def kernel_bc(cfg, ut_hbm, et_hbm, xt_hbm, z_hbm, w3_hbm, w4_hbm, w2_hbm,
              gu_hbm, gd_hbm, nrm_ref,
              act, side, euacc, wa, wb, wat, zb0, zb1, eb0, eb1, hb0, hb1, qb0, qb1,
              gu, gt, gd, r0u, r0d, a0u, a0d, a1u, a1d, a2u, a2d, r1u, r1d, r2u, r2d, r3u, r3d, fu, fd, nu, nd_acc,
              insem, wsem, zsem, ssem, rsem, fsem):
    nt, nr, nc, t, ft, d, nd = cfg
    rb, rc = t // nr, t // nc
    total = 2 * nt
    me, core, chip, steps = position()
    partner = flip(me, 1)
    zb, eb, hb, qb = (zb0, zb1), (eb0, eb1), (hb0, hb1), (qb0, qb1)
    G, R, ACC, FIN, NRM, OUT = (gu, gd), ((r0u, r1u, r2u, r3u), (r0d, r1d, r2d, r3d)), ((a0u, a1u, a2u), (a0d, a1d, a2d)), (fu, fd), (nu, nd_acc), (gu_hbm, gd_hbm)

    loads = [pltpu.make_async_copy(ut_hbm, act, insem.at[0]), pltpu.make_async_copy(et_hbm, side, insem.at[1])]
    for c in loads:
        c.start()

    def wcopies(j, slot, back):
        second = w2_hbm if back else w4_hbm
        cps = [pltpu.make_async_copy(second.at[:, j], wb.at[slot], wsem.at[1, slot])]
        if not back:
            cps.append(pltpu.make_async_copy(w3_hbm.at[:, j], wa.at[slot], wsem.at[0, slot]))
        return cps
    for c in wcopies(0, 0, False):
        c.start()

    meet([partner] + [me + 2 * s for s in steps])

    nu[...] = jnp.zeros_like(nu)
    nd_acc[...] = jnp.zeros_like(nd_acc)
    gt[1] = jnp.zeros_like(gt[1])
    def zero(r, _):
        euacc[:, aligned(r, rb)] = jnp.zeros((d, rb), F32)
        return 0
    lax.fori_loop(0, nr, zero, 0)

    def send(kind, stage, j):
        depth = R[kind][stage].shape[0]
        slot = lax.rem(j, depth)
        sem = (kind * len(SEEN) + stage) * max(DEPTH) + slot
        dst = R[kind][stage].at[slot]
        if stage == 0:
            src, dev = G[kind].at[lax.rem(j, G[kind].shape[0]), :, 1 - core], partner
        else:
            lo = PARTS >> stage
            src, dev = ACC[kind][stage - 1].at[lax.rem(j, HOLD), pl.ds(lo, lo)], me + 2 * hop(steps, kind, stage - 1, j)
        return pltpu.make_async_remote_copy(src_ref=src, dst_ref=dst, send_sem=ssem.at[sem], recv_sem=rsem.at[sem],
                                            device_id=(dev,), device_id_type=MESH)

    def final_copy(kind, j):
        slot = lax.rem(j, 2)
        return pltpu.make_async_copy(FIN[kind].at[slot], OUT[kind].at[j], fsem.at[kind, slot])

    def absorb(stage, j):
        place = lax.rem(j, HOLD)
        for kind in range(2):
            send(kind, stage, j).wait()
            slot = lax.rem(j, R[kind][stage].shape[0])
            got, acc = R[kind][stage], ACC[kind]
            if stage == 0:
                hops = [hop(steps, kind, place, j) for place in range(AXES)]
                for p in range(PARTS):
                    oc = chip + relative(hops, p)
                    acc[0][place, p] = G[kind][lax.rem(j, G[kind].shape[0]), oc, core] + got[slot, oc]
                continue
            kept = acc[stage - 1][place, 0:PARTS >> stage] + got[slot]
            if stage < LAST:
                acc[stage][place] = kept
            else:
                when(j >= 2, final_copy(kind, j - 2).wait)
                f = kept[0] * (1.0 / nd)
                FIN[kind][lax.rem(j, 2)] = f
                NRM[kind][...] += f * f
        for kind in range(2):
            (send(kind, stage + 1, j) if stage < LAST else final_copy(kind, j)).start()

    def comm(step):
        def due(j, fn):
            when(jnp.logical_and(j >= 0, j < total), fn)
        for stage in reversed(range(len(SEEN))):
            j = step - SEEN[stage]
            due(j, functools.partial(absorb, stage, j))
        def start():
            for kind in range(2):
                send(kind, 0, step - BEGUN).start()
        due(step - BEGUN, start)

    def turn(step, part):
        slot = lax.rem(step + 1, 2)
        lanes = pl.ds(part * TURN, TURN)
        gd[slot, :, :, :, lanes] = gt[slot, lanes, :].T.reshape(gd.shape[1:-1] + (TURN,))

    def add_up(step, r, value):
        slot, value = lax.rem(step, gu.shape[0]), value.reshape(gu.shape[1:])
        gu[slot] = value if r == 0 else gu[slot] + value

    def add_down(step, r, value):
        slot = lax.rem(step, 2)
        gt[slot] = value if r == 0 else gt[slot] + value

    def gates(r, width, pre):
        h, der = gelu_pair(pre)
        lanes = pl.ds(0, width)
        hb[r % 2][:, lanes] = h.astype(BF16)
        qb[r % 2][:, lanes] = (eb[r % 2][:, lanes].astype(F32) * der).astype(BF16)

    def pipeline(step, blocks, front, middle, back):
        front(0)
        for r in range(blocks):
            middle(r)
            if r + 1 < blocks:
                front(r + 1)
            if r >= 1:
                back(r - 1)
            for part in range(r, d // TURN, blocks):
                turn(step, part)
        back(blocks - 1)

    for c in loads:
        c.wait()

    def tile_b(j, _):
        slot = lax.rem(j, 2)
        comm(j)
        for c in wcopies(j, slot, False):
            c.wait()
        @pl.when(j + 1 < nt)
        def _():
            for c in wcopies(j + 1, 1 - slot, False):
                c.start()
        def cols(r):
            return pl.ds(r * rb, rb)
        mine = pl.ds(0, rb)
        def front(r):
            zb[r % 2][...] = dot_nn(wa[slot].reshape(ft, d), act[:, cols(r)])
            eb[r % 2][:, mine] = dot_nn(wb[slot].reshape(ft, d), side[:, cols(r)]).astype(BF16)
            if r == 0:
                wat[...] = wa[slot].reshape(ft, d).T
        def middle(r):
            gates(r, rb, zb[r % 2][...])
        def back(r):
            q = qb[r % 2][:, mine]
            add_up(j, r, dot_nt(act[:, cols(r)], q))
            add_down(j, r, dot_nt(side[:, cols(r)], hb[r % 2][:, mine]))
            euacc[:, cols(r)] += dot_nn(wat[...], q)
        pipeline(j, nr, front, middle, back)
        return 0
    lax.fori_loop(0, nt, tile_b, 0)

    xt_in = pltpu.make_async_copy(xt_hbm, side, insem.at[1])
    xt_in.start()
    for c in wcopies(0, nt % 2, True):
        c.start()
    def zcopy(j, slot):
        return pltpu.make_async_copy(z_hbm.at[j], euacc.at[aligned(slot, ft), :], zsem.at[slot])
    def cast(q, _):
        rows = aligned(lax.rem(q + ft // TURN, d // TURN), TURN)
        act[rows, :] = euacc[rows, :].astype(BF16)
        return 0
    lax.fori_loop(0, ft // TURN, cast, 0)
    zcopy(0, nt % 2).start()
    lax.fori_loop(ft // TURN, d // TURN, cast, 0)
    xt_in.wait()

    def tile_c(step, _):
        j = step - nt
        slot = lax.rem(step, 2)
        comm(step)
        for c in wcopies(j, slot, True):
            c.wait()
        zcopy(j, slot).wait()
        @pl.when(j + 1 < nt)
        def _():
            for c in wcopies(j + 1, 1 - slot, True):
                c.start()
            zcopy(j + 1, 1 - slot).start()
        def cols(r):
            return pl.ds(r * rc, rc)
        mine = pl.ds(0, rc)
        def front(r):
            eb[r % 2][:, mine] = dot_nn(wb[slot].reshape(ft, d), act[:, cols(r)]).astype(BF16)
        def middle(r):
            gates(r, rc, euacc[aligned(slot, ft), cols(r)])
        def back(r):
            add_down(step, r, dot_nt(act[:, cols(r)], hb[r % 2][:, mine]))
            add_up(step, r, dot_nt(side[:, cols(r)], qb[r % 2][:, mine]))
        pipeline(step, nc, front, middle, back)
        return 0
    lax.fori_loop(nt, total, tile_c, 0)

    def drain(step, _):
        comm(step)
        @pl.when(step == total)
        def _():
            for part in range(d // TURN):
                turn(step, part)
        return 0
    lax.fori_loop(total, total + SEEN[LAST], drain, 0)
    for kind in range(2):
        for j in (total - 2, total - 1):
            final_copy(kind, j).wait()

    part = jnp.zeros((8, 128), F32)
    for ref in (nu, nd_acc):
        rows, cols = ref.shape
        for a in range(rows // 8):
            for b in range(cols // 128):
                part = part + ref[8 * a:8 * a + 8, 128 * b:128 * b + 128]
    nrm_ref[...] = part


def backward(ut, et, xt, z, w3r, w4r, w2r):
    d, t = ut.shape
    nd, nt, rows2, _ = w4r.shape
    ft, nr, nc = nd * rows2, BACK_BLOCKS, BACK_BLOCKS // 2
    rb, rc = t // nr, t // nc
    bu, bd = (d // nd, ft), (rows2, d)
    V, D = pltpu.VMEM, pltpu.SemaphoreType.DMA
    S = jax.ShapeDtypeStruct
    scratch = [V((d, t), BF16)] * 2 + [V((d, t), F32)] + [V((PAIR, nd, rows2, d), BF16)] * 2 + [V((d, ft), BF16)]
    scratch += [V((ft, rb), F32)] * 2 + [V((ft, rc), BF16)] * 6
    scratch += [V((3, PARTS, 2) + bu, F32), V((PAIR, d, ft), F32), V((PAIR, PARTS, 2) + bd, F32)]
    for n, c in [(DEPTH[0], PARTS)] + [(HOLD, PARTS >> k) for k in range(LAST)] + [(DEPTH[k], PARTS >> k) for k in range(1, LAST + 1)]:
        scratch += [V((n, c) + bu, F32), V((n, c) + bd, F32)]
    scratch += [V((PAIR,) + bu, F32), V((PAIR,) + bd, F32), V(bu, F32), V(bd, F32)]
    flags = 2 * len(SEEN) * max(DEPTH)
    scratch += [D((PAIR,)), D((PAIR, PAIR)), D((PAIR,)), D((flags,)), D((flags,)), D((PAIR, PAIR))]
    return pl.pallas_call(
        functools.partial(kernel_bc, (nt, nr, nc, t, ft, d, nd)),
        out_shape=(S((2 * nt,) + bu, F32), S((2 * nt,) + bd, F32), S((8, 128), F32)),
        in_specs=[HBM] * 7, out_specs=(HBM, HBM, pl.BlockSpec(memory_space=pltpu.VMEM)),
        scratch_shapes=scratch,
        compiler_params=pltpu.CompilerParams(collective_id=0, has_side_effects=True, vmem_limit_bytes=VMEM_MAX),
        name="backward",
    )(ut, et, xt, z, w3r, w4r, w2r)


STEP = 20
BETA_ONE = 0.9
BETA_TWO = 0.95
EPSILON = 1e-8
NORM_EPS = 1e-6
CORR_ONE = 1.0 - BETA_ONE ** STEP
CORR_TWO = 1.0 - BETA_TWO ** STEP
WIDTH = 16
LAG = 3
AHEAD = 2
EMIT = 4
UPDATE_VMEM = 19 * 1024 * 1024 + 256 * 1024
EMIT_VMEM = 17 * 1024 * 1024


def clip_scale(norm, clip):
    return jnp.minimum(1.0, clip / (norm + NORM_EPS))


def adam_rows(scale, rate, grad, master, mom, vel):
    scaled = scale * grad
    mom = BETA_ONE * mom + (1.0 - BETA_ONE) * scaled
    vel = BETA_TWO * vel + (1.0 - BETA_TWO) * scaled * scaled
    master = master - rate * (mom * (1.0 / CORR_ONE)) / (jnp.sqrt(vel * (1.0 / CORR_TWO)) + EPSILON)
    return master, mom, vel


def natural_columns(gbuf, layer, first, count, nd, nt):
    rows, per = gbuf.shape[2], LANES // WIDTH
    group = lax.broadcasted_iota(jnp.int32, (rows, LANES), 1) // WIDTH
    tiles = []
    for t in range(count):
        acc = None
        for s in range(per):
            place = per * (first + t) + s
            owner, j = lax.div(place, nt), lax.rem(place, nt)
            src = gbuf[layer, j, :, aligned(lax.div(owner, per), LANES)]
            turned = pltpu.roll(src, lax.rem(s - lax.rem(owner, per) + per, per) * WIDTH, 1)
            acc = turned if acc is None else jnp.where(group == s, turned, acc)
        tiles.append(acc)
    return jnp.concatenate(tiles, axis=1)


def state_loads(gu_hbm, gd_hbm, states, gbuf, sbuf, sem, lo, hi):
    loads = []
    for kind, src in enumerate((gu_hbm, gd_hbm)):
        nt, size = src.shape[0] // 2, src.shape[2] if kind == 0 else src.shape[1]
        part = pl.ds(lo * size, (hi - lo) * size)
        for layer in range(2):
            first, count = (lo, hi - lo) if kind else (0, nt if lo == 0 else 0)
            if count:
                loads.append(pltpu.make_async_copy(src.at[pl.ds((1 - layer) * nt + first, count)], gbuf[kind].at[layer, pl.ds(first, count)],
                                                   sem.at[kind, layer, 3]))
            for f in range(3):
                whole, mine = states[4 * f + 2 * layer + kind], sbuf[kind].at[layer, f]
                pair = (whole.at[:, part], mine.at[:, part]) if kind == 0 else (whole.at[part, :], mine.at[part, :])
                loads.append(pltpu.make_async_copy(*pair, sem.at[kind, layer, f]))
    return loads


def kernel_update(cfg, part_hbm, rate_ref, clip_ref, gu_hbm, gd_hbm, *refs):
    nd, pieces, ru, cu, rd = cfg
    states, (ou1, ou2, od1, od2, norm_ref), (su, sd, gbuf_u, gbuf_d, sbuf_u, sbuf_d, nrecv, insem, nsem, lsem, rsem, ssem, dsem) = refs[:12], refs[12:17], refs[17:]
    me, core, chip, steps = position()
    partner = flip(me, 1)
    IN, O = (su, sd), ((ou1, ou2), (od1, od2))
    layers = range(len(O[0]))
    loads = [state_loads(gu_hbm, gd_hbm, states, (gbuf_u, gbuf_d), (sbuf_u, sbuf_d), insem.at[n], *span)
             for n, span in enumerate(((0, AHEAD), (AHEAD, pieces)))]
    keep = pltpu.make_async_copy(part_hbm, nrecv.at[me], nsem.at[2])
    for c in (keep, *loads[0], *loads[1]):
        c.start()
    meet([lax.rem(me + k, nd) for k in range(1, nd)])
    for k in range(1, nd):
        pltpu.make_async_remote_copy(src_ref=part_hbm, dst_ref=nrecv.at[me], send_sem=nsem.at[0], recv_sem=nsem.at[1],
                                     device_id=(lax.rem(me + k, nd),), device_id_type=MESH).start()

    def block(kind, first, j, ref):
        if kind == 0:
            return ref.at[pl.ds(pl.multiple_of(first, 8), ru), aligned(j, cu)]
        return ref.at[pl.ds(pl.multiple_of(first + j * rd, 8), rd), :]

    height = (ru, rd * pieces)
    own = [pltpu.make_async_copy(IN[kind].at[w], O[kind][w].at[aligned(me, height[kind]), :], lsem.at[kind, w])
           for kind in range(2) for w in layers]

    def push(kind, p, j, hops, dev, send, recv):
        first = (2 * (chip + relative(hops, p)) + core) * height[kind]
        for w in layers:
            dst = block(kind, first, j, O[kind][w])
            src = dst if p else block(kind, 0, j, IN[kind].at[w])
            pltpu.make_async_remote_copy(src_ref=src, dst_ref=dst, send_sem=send, recv_sem=recv, device_id=(dev,), device_id_type=MESH).start()

    def flag(kind, stage, j):
        return rsem.at[kind, stage, lax.rem(j, AXES * LAG)]

    def spread(kind, stage, j, hops):
        dev = me + 2 * hops[AXES - 1 - stage]
        for p in range(1 << stage):
            push(kind, p, j, hops, dev, ssem.at[kind, stage], flag(kind, stage, j))

    def await_bytes(ref, sem, recv):
        cp = pltpu.make_async_remote_copy(src_ref=ref, dst_ref=ref, send_sem=sem, recv_sem=sem, device_id=(me,), device_id_type=MESH)
        if recv:
            cp.wait_recv()
        else:
            cp.wait_send()

    def arrived(kind, stage, j):
        n = 2 << stage
        part = O[kind][0].at[pl.ds(0, n * ru), pl.ds(0, cu)] if kind == 0 else O[kind][0].at[pl.ds(0, n * rd), :]
        await_bytes(part, flag(kind, stage, j), True)

    keep.wait()
    others = nrecv.at[pl.ds(0, nd - 1)]
    await_bytes(others, nsem.at[0], False)
    await_bytes(others, nsem.at[1], True)
    total_sq = nrecv[0]
    for k in range(1, nd):
        total_sq = total_sq + nrecv[k]
    norm = jnp.sqrt(jnp.sum(total_sq, keepdims=True))
    norm_ref[...] = jnp.broadcast_to(norm, norm_ref.shape)
    rate, scale = rate_ref[0], clip_scale(norm, clip_ref[0])

    def make(j):
        for w in layers:
            cols = aligned(j, cu)
            grad = natural_columns(gbuf_u, w, j * (cu // LANES), cu // LANES, nd, pieces)
            old = [sbuf_u[w, f, :, cols] for f in range(3)]
            su[w, :, cols] = adam_rows(scale, rate, grad, *old)[0].astype(BF16)
            rows = aligned(j, rd)
            old = [sbuf_d[w, f, rows, :] for f in range(3)]
            sd[w, rows, :] = adam_rows(scale, rate, gbuf_d[w, j], *old)[0].astype(BF16)

    def step(s, _):
        for stage in reversed(range(AXES + 1)):
            j = s - stage * LAG
            @pl.when(jnp.logical_and(j >= 0, j < pieces))
            def _():
                for kind in range(2):
                    hops = [hop(steps, kind, place, j) for place in range(AXES)]
                    if stage:
                        arrived(kind, stage - 1, j)
                    if stage < AXES:
                        spread(kind, stage, j, hops)
                    for p in range((1 << stage) >> 1, 1 << stage):
                        push(kind, p, j, hops, partner, dsem.at[0, kind], dsem.at[1, kind])
        @pl.when(s + AHEAD < pieces)
        def _():
            make(s + AHEAD)
        return 0
    for c in loads[0]:
        c.wait()
    for j in range(AHEAD):
        make(j)
    for c in loads[1]:
        c.wait()
    lax.fori_loop(0, pieces + AXES * LAG, step, 0)
    for c in own:
        c.start()
    for c in own:
        c.wait()
    for kind in range(2):
        full = O[kind][0]
        await_bytes(full, dsem.at[0, kind], False)
        await_bytes(full, dsem.at[1, kind], True)
        for stage in range(AXES):
            await_bytes(full.at[pl.ds(0, (2 << stage) * height[kind]), :], ssem.at[kind, stage], False)


def update(part, rate, clip, gu, gd, states, nd):
    (ru, f), (rf, d) = states[0].shape, states[1].shape
    pieces = gd.shape[0] // 2
    V, D, S = pltpu.VMEM, pltpu.SemaphoreType.DMA, jax.ShapeDtypeStruct
    anyspec, vm, sm = [pl.BlockSpec(memory_space=m) for m in (pl.ANY, pltpu.VMEM, pltpu.SMEM)]
    return pl.pallas_call(
        functools.partial(kernel_update, (nd, pieces, ru, f // pieces, rf // pieces)),
        out_shape=(S((ru * nd, f), BF16),) * 2 + (S((rf * nd, d), BF16),) * 2 + (S((8, LANES), F32),),
        in_specs=[HBM, sm, sm] + [HBM] * 14, out_specs=(anyspec,) * 4 + (vm,),
        scratch_shapes=[V((PAIR, ru, f), BF16), V((PAIR, rf, d), BF16), V((PAIR, pieces) + gu.shape[1:], F32), V((PAIR, pieces) + gd.shape[1:], F32),
                        V((PAIR, 3, ru, f), F32), V((PAIR, 3, rf, d), F32), V((nd, 8, LANES), F32),
                        D((2, 2, 2, 4)), D((3,)), D((PAIR, PAIR)), D((2, AXES, AXES * LAG)), D((2, AXES)), D((PAIR, PAIR))],
        compiler_params=pltpu.CompilerParams(collective_id=1, has_side_effects=True, vmem_limit_bytes=UPDATE_VMEM),
        name="update")(part, rate, clip, gu, gd, *states)


def kernel_emit(cfg, norm_ref, rate_ref, clip_ref, gu_hbm, gd_hbm, *refs):
    nd, nt = cfg
    weights, states, refs = refs[:4], refs[4:16], refs[16:]
    weights_out, states_out, norm_out = refs[:4], refs[4:16], refs[16]
    gbuf_u, gbuf_d, sbuf_u, sbuf_d, insem, wsem, osem = refs[17:]
    gbuf, sbuf = (gbuf_u, gbuf_d), (sbuf_u, sbuf_d)
    loads = state_loads(gu_hbm, gd_hbm, states, gbuf, sbuf, insem, 0, nt)
    for c in loads:
        c.start()
    copies = []
    for k, (src, dst) in enumerate(zip(weights, weights_out)):
        rows = src.shape[0] // EMIT
        for part in range(EMIT):
            piece = pl.ds(part * rows, rows)
            copies.append(pltpu.make_async_copy(src.at[piece, :], dst.at[piece, :], wsem.at[k, part]))
    for c in copies:
        c.start()
    norm = norm_ref[0:1, 0:1]
    norm_out[...] = norm
    rate, scale = rate_ref[0], clip_scale(norm, clip_ref[0])
    for n, c in enumerate(loads):
        c.wait()
        kind, layer = n // 8, n // 4 % 2
        if n % 4 < 3:
            continue
        def renew(rows, cols, grad):
            old = [sbuf[kind][layer, f, rows, cols] for f in range(3)]
            for f, value in enumerate(adam_rows(scale, rate, grad, *old)):
                sbuf[kind][layer, f, rows, cols] = value
        def body(j, _):
            if kind == 0:
                wide = sbuf_u.shape[3] // nt
                renew(slice(None), aligned(j, wide), natural_columns(gbuf_u, layer, j * (wide // LANES), wide // LANES, nd, nt))
            else:
                renew(aligned(j, gbuf_d.shape[2]), slice(None), gbuf_d[layer, j])
            return 0
        lax.fori_loop(0, nt, body, 0)
        for f in range(3):
            cp = pltpu.make_async_copy(sbuf[kind].at[layer, f], states_out[4 * f + 2 * layer + kind], osem.at[kind, layer, f])
            cp.start()
            copies.append(cp)
    for c in copies:
        c.wait()


def emit(norm, rate, clip, gu, gd, weights, states, nd):
    nt = gu.shape[0] // 2
    up, down = states[0].shape, states[1].shape
    V, D, S = pltpu.VMEM, pltpu.SemaphoreType.DMA, jax.ShapeDtypeStruct
    anyspec, vm, sm = [pl.BlockSpec(memory_space=m) for m in (pl.ANY, pltpu.VMEM, pltpu.SMEM)]
    return pl.pallas_call(
        functools.partial(kernel_emit, (nd, nt)),
        out_shape=[S(a.shape, a.dtype) for a in (*weights, *states)] + [S((1, 1), F32)],
        in_specs=[vm, sm, sm] + [HBM] * 2 + [anyspec] * 4 + [HBM] * 12, out_specs=[HBM] * 16 + [vm],
        scratch_shapes=[V((PAIR, nt) + gu.shape[1:], F32), V((PAIR, nt) + gd.shape[1:], F32), V((PAIR, 3) + up, F32), V((PAIR, 3) + down, F32),
                        D((2, 2, 4)), D((4, EMIT)), D((2, 2, 3))],
        compiler_params=pltpu.CompilerParams(vmem_limit_bytes=EMIT_VMEM), name="emit")(norm, rate, clip, gu, gd, *weights, *states)


def solution(mesh):
    groups = mesh.shape["data"]
    rows_spec = P("data", None)
    full_spec = P(None, None)
    scalar_spec = P()

    def shard_body(act_in, grad_out, w_up1, w_down1, w_up2, w_down2, *rest):
        states, learn_rate, clip_norm = rest[:12], rest[12], rest[13]
        ff, d = w_down1.shape
        down1_tiles = w_down1.reshape(groups, -1, 16, d)
        down2_tiles = w_down2.reshape(groups, -1, 16, d)
        pre1, mid_t, in_t, grad_t, up2_t = forward_one(act_in, grad_out, w_up1, w_up2, down1_tiles)
        up2_tiles = up2_t.reshape(down1_tiles.shape)
        grads_up, grads_down, sq = backward(mid_t, grad_t, in_t, pre1, up2_tiles, down2_tiles, down1_tiles)
        rate, clip = learn_rate.reshape(1), clip_norm.reshape(1)
        states = [pltpu.with_memory_space_constraint(x, pltpu.HBM) for x in states]
        sq, grads_up, grads_down = [pltpu.with_memory_space_constraint(x, pltpu.HBM) for x in (sq, grads_up, grads_down)]
        up1, up2, down1, down2, norm = update(sq, rate, clip, grads_up, grads_down, states, groups)
        *results, norm = emit(norm, rate, clip, grads_up, grads_down, (up1, down1, up2, down2), states, groups)
        return (*results, norm.reshape(()))

    in_specs = (rows_spec, rows_spec) + (full_spec,) * 4 + (rows_spec,) * 12 + (scalar_spec, scalar_spec)
    out_specs = (full_spec,) * 4 + (rows_spec,) * 12 + (scalar_spec,)
    return jax.shard_map(shard_body, mesh=mesh, in_specs=in_specs, out_specs=out_specs, check_vma=False)
```

```python
import functools
import math
import jax
import jax.numpy as jnp
from jax import lax
from jax.experimental import pallas as pl
from jax.experimental.pallas import tpu as pltpu
from jax.sharding import PartitionSpec as P

ROOT_HALF = math.sqrt(0.5)
INV_ROOT_TAU = 1.0 / math.sqrt(2.0 * math.pi)
F32, BF16 = jnp.float32, jnp.bfloat16
HBM = pl.BlockSpec(memory_space=pltpu.HBM)
VMEM_MAX = 64 * 1024 * 1024 - 65536
PAIR = 2
BLOCKS = 8
TURNS = 8
RING = 4
LANES = 128


def dot_nn(a, b):
    return lax.dot_general(a, b, (((1,), (0,)), ((), ())), preferred_element_type=F32)


def dot_nt(a, b):
    return lax.dot_general(a, b, (((1,), (1,)), ((), ())), preferred_element_type=F32)


def gelu(z):
    return z * (0.5 * (1.0 + lax.erf(z * ROOT_HALF)))


def at_most(j, bound):
    return jnp.minimum(j, bound)


def aligned(j, size):
    return pl.ds(pl.multiple_of(j * size, size), size)


def kernel_a(cfg, x_hbm, e_hbm, w1_hbm, w3_hbm, w2_hbm, z_hbm, ut_hbm, xt_hbm, et_hbm, w3t_hbm,
             xt, uacc, zout, w1t_v, w1_in, x_in, w1, w2, w2t, w3_in, w3_out, e_in, e_out, h0, h1,
             wsem, xsem, esem, vsem, zsem, osem):
    nt, nr, rb, tr, tb, ft, d, nd = cfg
    hb = (h0, h1)
    width = ft // nd

    def w1copy(q):
        slot = lax.rem(q, RING)
        return pltpu.make_async_copy(w1_hbm.at[aligned(q, LANES), :], w1_in.at[slot], wsem.at[slot])

    def xcopy(r):
        slot = lax.rem(r, RING)
        return pltpu.make_async_copy(x_hbm.at[aligned(r, tb), :], x_in.at[slot], xsem.at[slot])

    def w2copy(j):
        slot = lax.rem(j, 2)
        return pltpu.make_async_copy(w2_hbm.at[:, j], w2.at[slot], vsem.at[0, slot])

    def w3copy(j):
        slot = lax.rem(j, 2)
        return pltpu.make_async_copy(w3_hbm.at[:, aligned(j, ft)], w3_in.at[slot], vsem.at[1, slot])

    def w3store(j):
        slot = lax.rem(j, 2)
        return pltpu.make_async_copy(w3_out.at[slot], w3t_hbm.at[aligned(j, ft), :], osem.at[0, slot])

    def ecopy(r):
        slot = lax.rem(r, 2)
        return pltpu.make_async_copy(e_hbm.at[aligned(r, tb), :], e_in.at[slot], esem.at[slot])

    def estore(r):
        slot = lax.rem(r, 2)
        return pltpu.make_async_copy(e_out.at[slot], et_hbm.at[:, aligned(r, tb)], osem.at[1, slot])

    def zstore(j):
        slot = lax.rem(j, 2)
        return pltpu.make_async_copy(zout.at[slot], z_hbm.at[j], zsem.at[slot])

    rows_in = d // LANES
    for q in range(min(RING, rows_in)):
        w1copy(q).start()
    for r in range(min(RING, tr)):
        xcopy(r).start()
    for c in (w2copy(0), w3copy(0), ecopy(0)):
        c.start()

    def zero(r, _):
        uacc[:, aligned(r, rb)] = jnp.zeros((d, rb), F32)
        return 0
    lax.fori_loop(0, nr, zero, 0)

    def turn_in(q, _):
        @pl.when(q < rows_in)
        def _():
            w1copy(q).wait()
            w1t_v[:, aligned(q, LANES)] = w1_in[lax.rem(q, RING)].T
        @pl.when(q + RING < rows_in)
        def _():
            w1copy(q + RING).start()
        xcopy(q).wait()
        xt[:, aligned(q, tb)] = x_in[lax.rem(q, RING)].T
        @pl.when(q + RING < tr)
        def _():
            xcopy(q + RING).start()
        return 0
    lax.fori_loop(0, tr, turn_in, 0)
    xt_store = pltpu.make_async_copy(xt, xt_hbm, osem.at[2, 0])
    xt_store.start()

    def pick_w1(j, slot):
        for k in range(nd):
            w1[slot, k * width:(k + 1) * width, :] = w1t_v[aligned(k * nt + j, width), :]
    pick_w1(0, 0)

    def tile(j, _):
        slot = lax.rem(j, 2)
        nslot = 1 - slot
        @pl.when(j >= 2)
        def _():
            zstore(j - 2).wait()
            w3store(j - 2).wait()
        @pl.when(jnp.logical_and(j >= 2, j < tr + 2))
        def _():
            estore(j - 2).wait()
        w2copy(j).wait()
        w3copy(j).wait()
        @pl.when(j < tr)
        def _():
            ecopy(j).wait()
        @pl.when(j + 1 < nt)
        def _():
            w2copy(j + 1).start()
            w3copy(j + 1).start()
        @pl.when(j + 1 < min(tr, nt))
        def _():
            ecopy(j + 1).start()

        def cols(r):
            return pl.ds(r * rb, rb)
        def front(r):
            zout[slot, :, cols(r)] = dot_nn(w1[slot], xt[:, cols(r)])
        def middle(r):
            hb[r % 2][...] = gelu(zout[slot, :, cols(r)]).astype(BF16)
        def back(r):
            uacc[:, cols(r)] += dot_nn(w2t[...], hb[r % 2][...])
        front(0)
        w2t[...] = w2[slot].reshape(ft, d).T
        for r in range(nr):
            middle(r)
            if r + 1 < nr:
                front(r + 1)
            if r >= 1:
                back(r - 1)
            if r == 0:
                pick_w1(at_most(j + 1, nt - 1), nslot)
            if r == 1:
                w3_out[slot] = w3_in[slot].T
            if r == nr - 2:
                e_out[slot] = e_in[slot].T
        back(nr - 1)
        zstore(j).start()
        w3store(j).start()
        @pl.when(j < tr)
        def _():
            estore(j).start()
        return 0
    lax.fori_loop(0, nt, tile, 0)
    xt_store.wait()

    def finish(r, _):
        block = aligned(r, rb)
        xt[:, block] = uacc[:, block].astype(BF16)
        pltpu.make_async_copy(xt.at[:, block], ut_hbm.at[:, block], osem.at[2, 1]).start()
        return 0
    lax.fori_loop(0, nr, finish, 0)
    ut_store = pltpu.make_async_copy(xt, ut_hbm, osem.at[2, 1])
    for j in (nt - 2, nt - 1):
        zstore(j).wait()
        w3store(j).wait()
        if j < tr:
            estore(j).wait()
    for r in range(nt, tr):
        ecopy(r).start()
        ecopy(r).wait()
        e_out[r % 2] = e_in[r % 2].T
        estore(r).start()
        estore(r).wait()
    ut_store.wait()


def forward_one(x, e, w1, w3, w2r):
    t, d = x.shape
    nd, nt, rows2, _ = w2r.shape
    ft, nr, tr = nd * rows2, BLOCKS, TURNS
    rb, tb = t // nr, t // tr
    V, D = pltpu.VMEM, pltpu.SemaphoreType.DMA
    S = jax.ShapeDtypeStruct
    return pl.pallas_call(
        functools.partial(kernel_a, (nt, nr, rb, tr, tb, ft, d, nd)),
        out_shape=(S((nt, ft, t), F32), S((d, t), BF16), S((d, t), BF16), S((d, t), BF16), S((nt * ft, d), BF16)),
        in_specs=[HBM] * 5, out_specs=(HBM,) * 5,
        scratch_shapes=[
            V((d, t), BF16), V((d, t), F32), V((PAIR, ft, t), F32), V((nt * ft, d), BF16), V((RING, LANES, nt * ft), BF16), V((RING, tb, d), BF16),
            V((PAIR, ft, d), BF16), V((PAIR, nd, rows2, d), BF16), V((d, ft), BF16), V((PAIR, d, ft), BF16), V((PAIR, ft, d), BF16),
            V((PAIR, tb, d), BF16), V((PAIR, d, tb), BF16), V((ft, rb), BF16), V((ft, rb), BF16),
            D((RING,)), D((RING,)), D((PAIR,)), D((PAIR, PAIR)), D((PAIR,)), D((3, 2))],
        compiler_params=pltpu.CompilerParams(vmem_limit_bytes=VMEM_MAX),
        name="forward_one",
    )(x, e, w1, w3, w2r)


MESH = pl.DeviceIdType.MESH

def gelu_pair(pre):
    normal_cdf = 0.5 * (1.0 + lax.erf(pre * ROOT_HALF))
    density = jnp.exp(-0.5 * pre * pre) * INV_ROOT_TAU
    return pre * normal_cdf, normal_cdf + pre * density

def flip(value, step):
    return value + step * (1 - 2 * lax.rem(lax.div(value, step), 2))

def position():
    me = lax.axis_index("data")
    chip = lax.div(me, 2)
    steps = [(1 << k) * (1 - 2 * lax.rem(lax.div(chip, 1 << k), 2)) for k in range(AXES)]
    return me, lax.rem(me, 2), chip, steps


def hop(steps, kind, place, j):
    axis = lax.rem(j + ORDERS[kind][place], AXES)
    return steps[0] * lax.div((2 - axis) * (1 - axis), 2) + steps[1] * axis * (2 - axis) + steps[2] * lax.div(axis * (axis - 1), 2)


def relative(hops, p):
    return sum((hops[place] for place in range(AXES) if (p >> (AXES - 1 - place)) & 1), 0)


AXES = 3


def when(condition, fn):
    pl.when(condition)(fn)


def meet(peers):
    barrier = pltpu.get_barrier_semaphore()
    for peer in peers:
        pl.semaphore_signal(barrier, inc=1, device_id=(peer,), device_id_type=MESH)
    pl.semaphore_wait(barrier, len(peers))


ORDERS = ((0, 2, 1), (1, 2, 0))
PARTS = 8
BACK_BLOCKS = 4
BEGUN = 2
TURN = 128
SEEN = (3, 6, 9, 12)
DEPTH = (2, 6, 6, 6)
LAST = len(SEEN) - 1
HOLD = 3

def kernel_bc(cfg, ut_hbm, et_hbm, xt_hbm, z_hbm, w3_hbm, w4_hbm, w2_hbm,
              gu_hbm, gd_hbm, nrm_ref,
              act, side, euacc, wa, wb, wat, zb0, zb1, eb0, eb1, hb0, hb1, qb0, qb1,
              gu, gt, gd, r0u, r0d, a0u, a0d, a1u, a1d, a2u, a2d, r1u, r1d, r2u, r2d, r3u, r3d, fu, fd, nu, nd_acc,
              insem, wsem, zsem, ssem, rsem, fsem):
    nt, nr, nc, t, ft, d, nd = cfg
    rb, rc = t // nr, t // nc
    total = 2 * nt
    me, core, chip, steps = position()
    partner = flip(me, 1)
    zb, eb, hb, qb = (zb0, zb1), (eb0, eb1), (hb0, hb1), (qb0, qb1)
    G, R, ACC, FIN, NRM, OUT = (gu, gd), ((r0u, r1u, r2u, r3u), (r0d, r1d, r2d, r3d)), ((a0u, a1u, a2u), (a0d, a1d, a2d)), (fu, fd), (nu, nd_acc), (gu_hbm, gd_hbm)

    loads = [pltpu.make_async_copy(ut_hbm, act, insem.at[0]), pltpu.make_async_copy(et_hbm, side, insem.at[1])]
    for c in loads:
        c.start()

    def wcopies(j, slot, back):
        second = w2_hbm if back else w4_hbm
        cps = [pltpu.make_async_copy(second.at[:, j], wb.at[slot], wsem.at[slot])]
        if not back:
            cps.append(pltpu.make_async_copy(w3_hbm.at[:, j], wa.at[slot], wsem.at[slot]))
        return cps
    for c in wcopies(0, 0, False):
        c.start()

    meet([partner] + [me + 2 * s for s in steps])

    nu[...] = jnp.zeros_like(nu)
    nd_acc[...] = jnp.zeros_like(nd_acc)
    gt[1] = jnp.zeros_like(gt[1])
    def zero(r, _):
        euacc[:, aligned(r, rb)] = jnp.zeros((d, rb), F32)
        return 0
    lax.fori_loop(0, nr, zero, 0)

    def flag_of(stage, j):
        return stage * max(DEPTH) + lax.rem(j, DEPTH[stage])

    both = (gu.at[0], r0u.at[0], r1u.at[0], r2u.at[0])

    def join(stage, j):
        sem = flag_of(stage, j)
        pltpu.make_async_remote_copy(src_ref=both[stage], dst_ref=both[stage], send_sem=ssem.at[sem], recv_sem=rsem.at[sem],
                                     device_id=(me,), device_id_type=MESH).wait()

    def send(kind, stage, j):
        depth = R[kind][stage].shape[0]
        slot = lax.rem(j, depth)
        sem = flag_of(stage, j)
        dst = R[kind][stage].at[slot]
        if stage == 0:
            src, dev = G[kind].at[lax.rem(j, G[kind].shape[0]), :, 1 - core], partner
        else:
            lo = PARTS >> stage
            src, dev = ACC[kind][stage - 1].at[lax.rem(j, HOLD), pl.ds(lo, lo)], me + 2 * hop(steps, kind, stage - 1, j)
        return pltpu.make_async_remote_copy(src_ref=src, dst_ref=dst, send_sem=ssem.at[sem], recv_sem=rsem.at[sem],
                                            device_id=(dev,), device_id_type=MESH)

    def final_copy(kind, j):
        slot = lax.rem(j, 2)
        return pltpu.make_async_copy(FIN[kind].at[slot], OUT[kind].at[j], fsem.at[kind, slot])

    def absorb(stage, j):
        place = lax.rem(j, HOLD)
        join(stage, j)
        for kind in range(2):
            slot = lax.rem(j, R[kind][stage].shape[0])
            got, acc = R[kind][stage], ACC[kind]
            if stage == 0:
                hops = [hop(steps, kind, place, j) for place in range(AXES)]
                for p in range(PARTS):
                    oc = chip + relative(hops, p)
                    acc[0][place, p] = G[kind][lax.rem(j, G[kind].shape[0]), oc, core] + got[slot, oc]
                continue
            kept = acc[stage - 1][place, 0:PARTS >> stage] + got[slot]
            if stage < LAST:
                acc[stage][place] = kept
            else:
                when(j >= 2, final_copy(kind, j - 2).wait)
                f = kept[0] * (1.0 / nd)
                FIN[kind][lax.rem(j, 2)] = f
                NRM[kind][...] += f * f
        for kind in range(2):
            (send(kind, stage + 1, j) if stage < LAST else final_copy(kind, j)).start()

    def comm(step):
        def due(j, fn):
            when(jnp.logical_and(j >= 0, j < total), fn)
        for stage in reversed(range(len(SEEN))):
            j = step - SEEN[stage]
            due(j, functools.partial(absorb, stage, j))
        def start():
            for kind in range(2):
                send(kind, 0, step - BEGUN).start()
        due(step - BEGUN, start)

    def turn(step, part):
        slot = lax.rem(step + 1, 2)
        lanes = pl.ds(part * TURN, TURN)
        gd[slot, :, :, :, lanes] = gt[slot, lanes, :].T.reshape(gd.shape[1:-1] + (TURN,))

    def add_up(step, r, value):
        slot, value = lax.rem(step, gu.shape[0]), value.reshape(gu.shape[1:])
        gu[slot] = value if r == 0 else gu[slot] + value

    def add_down(step, r, value):
        slot = lax.rem(step, 2)
        gt[slot] = value if r == 0 else gt[slot] + value

    def gates(r, width, pre):
        h, der = gelu_pair(pre)
        lanes = pl.ds(0, width)
        hb[r % 2][:, lanes] = h.astype(BF16)
        qb[r % 2][:, lanes] = (eb[r % 2][:, lanes].astype(F32) * der).astype(BF16)

    def pipeline(step, blocks, front, middle, back):
        front(0)
        for r in range(blocks):
            middle(r)
            if r + 1 < blocks:
                front(r + 1)
            if r >= 1:
                back(r - 1)
            for part in range(r, d // TURN, blocks):
                turn(step, part)
        back(blocks - 1)

    for c in loads:
        c.wait()

    def tile_b(j, _):
        slot = lax.rem(j, 2)
        comm(j)
        pltpu.make_async_copy(wa, wa, wsem.at[slot]).wait()
        @pl.when(j + 1 < nt)
        def _():
            for c in wcopies(j + 1, 1 - slot, False):
                c.start()
        def cols(r):
            return pl.ds(r * rb, rb)
        mine = pl.ds(0, rb)
        def front(r):
            zb[r % 2][...] = dot_nn(wa[slot].reshape(ft, d), act[:, cols(r)])
            eb[r % 2][:, mine] = dot_nn(wb[slot].reshape(ft, d), side[:, cols(r)]).astype(BF16)
            if r == 0:
                wat[...] = wa[slot].reshape(ft, d).T
        def middle(r):
            gates(r, rb, zb[r % 2][...])
        def back(r):
            q = qb[r % 2][:, mine]
            add_up(j, r, dot_nt(act[:, cols(r)], q))
            add_down(j, r, dot_nt(side[:, cols(r)], hb[r % 2][:, mine]))
            euacc[:, cols(r)] += dot_nn(wat[...], q)
        pipeline(j, nr, front, middle, back)
        return 0
    lax.fori_loop(0, nt, tile_b, 0)

    xt_in = pltpu.make_async_copy(xt_hbm, side, insem.at[1])
    xt_in.start()
    for c in wcopies(0, nt % 2, True):
        c.start()
    def zcopy(j, slot):
        return pltpu.make_async_copy(z_hbm.at[j], euacc.at[aligned(slot, ft), :], zsem.at[slot])
    def cast(q, _):
        rows = aligned(lax.rem(q + ft // TURN, d // TURN), TURN)
        act[rows, :] = euacc[rows, :].astype(BF16)
        return 0
    lax.fori_loop(0, ft // TURN, cast, 0)
    zcopy(0, nt % 2).start()
    lax.fori_loop(ft // TURN, d // TURN, cast, 0)
    xt_in.wait()

    def tile_c(step, _):
        j = step - nt
        slot = lax.rem(step, 2)
        comm(step)
        for c in wcopies(j, slot, True):
            c.wait()
        zcopy(j, slot).wait()
        @pl.when(j + 1 < nt)
        def _():
            for c in wcopies(j + 1, 1 - slot, True):
                c.start()
            zcopy(j + 1, 1 - slot).start()
        def cols(r):
            return pl.ds(r * rc, rc)
        mine = pl.ds(0, rc)
        def front(r):
            eb[r % 2][:, mine] = dot_nn(wb[slot].reshape(ft, d), act[:, cols(r)]).astype(BF16)
        def middle(r):
            gates(r, rc, euacc[aligned(slot, ft), cols(r)])
        def back(r):
            add_down(step, r, dot_nt(act[:, cols(r)], hb[r % 2][:, mine]))
            add_up(step, r, dot_nt(side[:, cols(r)], qb[r % 2][:, mine]))
        pipeline(step, nc, front, middle, back)
        return 0
    lax.fori_loop(nt, total, tile_c, 0)

    def drain(step, _):
        comm(step)
        @pl.when(step == total)
        def _():
            for part in range(d // TURN):
                turn(step, part)
        return 0
    lax.fori_loop(total, total + SEEN[LAST], drain, 0)
    for kind in range(2):
        for j in (total - 2, total - 1):
            final_copy(kind, j).wait()

    part = jnp.zeros((8, 128), F32)
    for ref in (nu, nd_acc):
        rows, cols = ref.shape
        for a in range(rows // 8):
            for b in range(cols // 128):
                part = part + ref[8 * a:8 * a + 8, 128 * b:128 * b + 128]
    nrm_ref[...] = part


def backward(ut, et, xt, z, w3r, w4r, w2r):
    d, t = ut.shape
    nd, nt, rows2, _ = w4r.shape
    ft, nr, nc = nd * rows2, BACK_BLOCKS, BACK_BLOCKS // 2
    rb, rc = t // nr, t // nc
    bu, bd = (d // nd, ft), (rows2, d)
    V, D = pltpu.VMEM, pltpu.SemaphoreType.DMA
    S = jax.ShapeDtypeStruct
    scratch = [V((d, t), BF16)] * 2 + [V((d, t), F32)] + [V((PAIR, nd, rows2, d), BF16)] * 2 + [V((d, ft), BF16)]
    scratch += [V((ft, rb), F32)] * 2 + [V((ft, rc), BF16)] * 6
    scratch += [V((3, PARTS, 2) + bu, F32), V((PAIR, d, ft), F32), V((PAIR, PARTS, 2) + bd, F32)]
    for n, c in [(DEPTH[0], PARTS)] + [(HOLD, PARTS >> k) for k in range(LAST)] + [(DEPTH[k], PARTS >> k) for k in range(1, LAST + 1)]:
        scratch += [V((n, c) + bu, F32), V((n, c) + bd, F32)]
    scratch += [V((PAIR,) + bu, F32), V((PAIR,) + bd, F32), V(bu, F32), V(bd, F32)]
    flags = len(SEEN) * max(DEPTH)
    scratch += [D((PAIR,)), D((PAIR,)), D((PAIR,)), D((flags,)), D((flags,)), D((PAIR, PAIR))]
    return pl.pallas_call(
        functools.partial(kernel_bc, (nt, nr, nc, t, ft, d, nd)),
        out_shape=(S((2 * nt,) + bu, F32), S((2 * nt,) + bd, F32), S((8, 128), F32)),
        in_specs=[HBM] * 7, out_specs=(HBM, HBM, pl.BlockSpec(memory_space=pltpu.VMEM)),
        scratch_shapes=scratch,
        compiler_params=pltpu.CompilerParams(collective_id=0, has_side_effects=True, vmem_limit_bytes=VMEM_MAX),
        name="backward",
    )(ut, et, xt, z, w3r, w4r, w2r)


STEP = 20
BETA_ONE = 0.9
BETA_TWO = 0.95
EPSILON = 1e-8
NORM_EPS = 1e-6
CORR_ONE = 1.0 - BETA_ONE ** STEP
CORR_TWO = 1.0 - BETA_TWO ** STEP
WIDTH = 16
LAG = 3
AHEAD = 2
EMIT = 4
UPDATE_VMEM = 19 * 1024 * 1024 + 256 * 1024
EMIT_VMEM = 17 * 1024 * 1024


def clip_scale(norm, clip):
    return jnp.minimum(1.0, clip / (norm + NORM_EPS))


def adam_rows(scale, rate, grad, master, mom, vel):
    scaled = scale * grad
    mom = BETA_ONE * mom + (1.0 - BETA_ONE) * scaled
    vel = BETA_TWO * vel + (1.0 - BETA_TWO) * scaled * scaled
    master = master - rate * (mom * (1.0 / CORR_ONE)) / (jnp.sqrt(vel * (1.0 / CORR_TWO)) + EPSILON)
    return master, mom, vel


def natural_columns(gbuf, layer, first, count, nd, nt):
    rows, per = gbuf.shape[2], LANES // WIDTH
    group = lax.broadcasted_iota(jnp.int32, (rows, LANES), 1) // WIDTH
    tiles = []
    for t in range(count):
        acc = None
        for s in range(per):
            place = per * (first + t) + s
            owner, j = lax.div(place, nt), lax.rem(place, nt)
            src = gbuf[layer, j, :, aligned(lax.div(owner, per), LANES)]
            turned = pltpu.roll(src, lax.rem(s - lax.rem(owner, per) + per, per) * WIDTH, 1)
            acc = turned if acc is None else jnp.where(group == s, turned, acc)
        tiles.append(acc)
    return jnp.concatenate(tiles, axis=1)


def state_loads(gu_hbm, gd_hbm, states, gbuf, sbuf, sem, lo, hi):
    loads = []
    for kind, src in enumerate((gu_hbm, gd_hbm)):
        nt, size = src.shape[0] // 2, src.shape[2] if kind == 0 else src.shape[1]
        part = pl.ds(lo * size, (hi - lo) * size)
        for layer in range(2):
            first, count = (lo, hi - lo) if kind else (0, nt if lo == 0 else 0)
            if count:
                loads.append(pltpu.make_async_copy(src.at[pl.ds((1 - layer) * nt + first, count)], gbuf[kind].at[layer, pl.ds(first, count)],
                                                   sem.at[kind, layer, 3]))
            for f in range(3):
                whole, mine = states[4 * f + 2 * layer + kind], sbuf[kind].at[layer, f]
                pair = (whole.at[:, part], mine.at[:, part]) if kind == 0 else (whole.at[part, :], mine.at[part, :])
                loads.append(pltpu.make_async_copy(*pair, sem.at[kind, layer, f]))
    return loads


def kernel_update(cfg, part_hbm, rate_ref, clip_ref, gu_hbm, gd_hbm, *refs):
    nd, pieces, ru, cu, rd = cfg
    states, (ou1, ou2, od1, od2, norm_ref), (su, sd, gbuf_u, gbuf_d, sbuf_u, sbuf_d, nrecv, insem, nsem, lsem, rsem, ssem, dsem) = refs[:12], refs[12:17], refs[17:]
    me, core, chip, steps = position()
    partner = flip(me, 1)
    IN, O = (su, sd), ((ou1, ou2), (od1, od2))
    layers = range(len(O[0]))
    loads = [state_loads(gu_hbm, gd_hbm, states, (gbuf_u, gbuf_d), (sbuf_u, sbuf_d), insem.at[n], *span)
             for n, span in enumerate(((0, AHEAD), (AHEAD, pieces)))]
    keep = pltpu.make_async_copy(part_hbm, nrecv.at[me], nsem.at[2])
    for c in (keep, *loads[0], *loads[1]):
        c.start()
    meet([lax.rem(me + k, nd) for k in range(1, nd)])
    for k in range(1, nd):
        pltpu.make_async_remote_copy(src_ref=part_hbm, dst_ref=nrecv.at[me], send_sem=nsem.at[0], recv_sem=nsem.at[1],
                                     device_id=(lax.rem(me + k, nd),), device_id_type=MESH).start()

    def block(kind, first, j, ref):
        if kind == 0:
            return ref.at[pl.ds(pl.multiple_of(first, 8), ru), aligned(j, cu)]
        return ref.at[pl.ds(pl.multiple_of(first + j * rd, 8), rd), :]

    height = (ru, rd * pieces)
    own = [pltpu.make_async_copy(IN[kind].at[w], O[kind][w].at[aligned(me, height[kind]), :], lsem.at[kind, w])
           for kind in range(2) for w in layers]

    def push(kind, p, j, hops, dev, send, recv):
        first = (2 * (chip + relative(hops, p)) + core) * height[kind]
        for w in layers:
            dst = block(kind, first, j, O[kind][w])
            src = dst if p else block(kind, 0, j, IN[kind].at[w])
            pltpu.make_async_remote_copy(src_ref=src, dst_ref=dst, send_sem=send, recv_sem=recv, device_id=(dev,), device_id_type=MESH).start()

    def flag(kind, stage, j):
        return rsem.at[kind, stage, lax.rem(j, AXES * LAG)]

    def spread(kind, stage, j, hops):
        dev = me + 2 * hops[AXES - 1 - stage]
        for p in range(1 << stage):
            push(kind, p, j, hops, dev, ssem.at[kind, stage], flag(kind, stage, j))

    def await_bytes(ref, sem, recv):
        cp = pltpu.make_async_remote_copy(src_ref=ref, dst_ref=ref, send_sem=sem, recv_sem=sem, device_id=(me,), device_id_type=MESH)
        if recv:
            cp.wait_recv()
        else:
            cp.wait_send()

    def arrived(kind, stage, j):
        n = 2 << stage
        part = O[kind][0].at[pl.ds(0, n * ru), pl.ds(0, cu)] if kind == 0 else O[kind][0].at[pl.ds(0, n * rd), :]
        await_bytes(part, flag(kind, stage, j), True)

    keep.wait()
    others = nrecv.at[pl.ds(0, nd - 1)]
    await_bytes(others, nsem.at[0], False)
    await_bytes(others, nsem.at[1], True)
    total_sq = nrecv[0]
    for k in range(1, nd):
        total_sq = total_sq + nrecv[k]
    norm = jnp.sqrt(jnp.sum(total_sq, keepdims=True))
    norm_ref[...] = jnp.broadcast_to(norm, norm_ref.shape)
    rate, scale = rate_ref[0], clip_scale(norm, clip_ref[0])

    def make(j):
        for w in layers:
            cols = aligned(j, cu)
            grad = natural_columns(gbuf_u, w, j * (cu // LANES), cu // LANES, nd, pieces)
            old = [sbuf_u[w, f, :, cols] for f in range(3)]
            su[w, :, cols] = adam_rows(scale, rate, grad, *old)[0].astype(BF16)
            rows = aligned(j, rd)
            old = [sbuf_d[w, f, rows, :] for f in range(3)]
            sd[w, rows, :] = adam_rows(scale, rate, gbuf_d[w, j], *old)[0].astype(BF16)

    def step(s, _):
        for stage in reversed(range(AXES + 1)):
            j = s - stage * LAG
            @pl.when(jnp.logical_and(j >= 0, j < pieces))
            def _():
                for kind in range(2):
                    hops = [hop(steps, kind, place, j) for place in range(AXES)]
                    if stage:
                        arrived(kind, stage - 1, j)
                    if stage < AXES:
                        spread(kind, stage, j, hops)
                    for p in range((1 << stage) >> 1, 1 << stage):
                        push(kind, p, j, hops, partner, dsem.at[0, kind], dsem.at[1, kind])
        @pl.when(s + AHEAD < pieces)
        def _():
            make(s + AHEAD)
        return 0
    for c in loads[0]:
        c.wait()
    for j in range(AHEAD):
        make(j)
    for c in loads[1]:
        c.wait()
    lax.fori_loop(0, pieces + AXES * LAG, step, 0)
    for c in own:
        c.start()
    for c in own:
        c.wait()
    for kind in range(2):
        full = O[kind][0]
        await_bytes(full, dsem.at[0, kind], False)
        await_bytes(full, dsem.at[1, kind], True)
        for stage in range(AXES):
            await_bytes(full.at[pl.ds(0, (2 << stage) * height[kind]), :], ssem.at[kind, stage], False)


def update(part, rate, clip, gu, gd, states, nd):
    (ru, f), (rf, d) = states[0].shape, states[1].shape
    pieces = gd.shape[0] // 2
    V, D, S = pltpu.VMEM, pltpu.SemaphoreType.DMA, jax.ShapeDtypeStruct
    anyspec, vm, sm = [pl.BlockSpec(memory_space=m) for m in (pl.ANY, pltpu.VMEM, pltpu.SMEM)]
    return pl.pallas_call(
        functools.partial(kernel_update, (nd, pieces, ru, f // pieces, rf // pieces)),
        out_shape=(S((ru * nd, f), BF16),) * 2 + (S((rf * nd, d), BF16),) * 2 + (S((8, LANES), F32),),
        in_specs=[HBM, sm, sm] + [HBM] * 14, out_specs=(anyspec,) * 4 + (vm,),
        scratch_shapes=[V((PAIR, ru, f), BF16), V((PAIR, rf, d), BF16), V((PAIR, pieces) + gu.shape[1:], F32), V((PAIR, pieces) + gd.shape[1:], F32),
                        V((PAIR, 3, ru, f), F32), V((PAIR, 3, rf, d), F32), V((nd, 8, LANES), F32),
                        D((2, 2, 2, 4)), D((3,)), D((PAIR, PAIR)), D((2, AXES, AXES * LAG)), D((2, AXES)), D((PAIR, PAIR))],
        compiler_params=pltpu.CompilerParams(collective_id=1, has_side_effects=True, vmem_limit_bytes=UPDATE_VMEM),
        name="update")(part, rate, clip, gu, gd, *states)


def kernel_emit(cfg, norm_ref, rate_ref, clip_ref, gu_hbm, gd_hbm, *refs):
    nd, nt = cfg
    weights, states, refs = refs[:4], refs[4:16], refs[16:]
    weights_out, states_out, norm_out = refs[:4], refs[4:16], refs[16]
    gbuf_u, gbuf_d, sbuf_u, sbuf_d, insem, wsem, osem = refs[17:]
    gbuf, sbuf = (gbuf_u, gbuf_d), (sbuf_u, sbuf_d)
    loads = state_loads(gu_hbm, gd_hbm, states, gbuf, sbuf, insem, 0, nt)
    for c in loads:
        c.start()
    copies = []
    for k, (src, dst) in enumerate(zip(weights, weights_out)):
        rows = src.shape[0] // EMIT
        for part in range(EMIT):
            piece = pl.ds(part * rows, rows)
            copies.append(pltpu.make_async_copy(src.at[piece, :], dst.at[piece, :], wsem.at[k, part]))
    for c in copies:
        c.start()
    norm = norm_ref[0:1, 0:1]
    norm_out[...] = norm
    rate, scale = rate_ref[0], clip_scale(norm, clip_ref[0])
    for n, c in enumerate(loads):
        c.wait()
        kind, layer = n // 8, n // 4 % 2
        if n % 4 < 3:
            continue
        def renew(rows, cols, grad):
            old = [sbuf[kind][layer, f, rows, cols] for f in range(3)]
            for f, value in enumerate(adam_rows(scale, rate, grad, *old)):
                sbuf[kind][layer, f, rows, cols] = value
        def body(j, _):
            if kind == 0:
                wide = sbuf_u.shape[3] // nt
                renew(slice(None), aligned(j, wide), natural_columns(gbuf_u, layer, j * (wide // LANES), wide // LANES, nd, nt))
            else:
                renew(aligned(j, gbuf_d.shape[2]), slice(None), gbuf_d[layer, j])
            return 0
        lax.fori_loop(0, nt, body, 0)
        for f in range(3):
            cp = pltpu.make_async_copy(sbuf[kind].at[layer, f], states_out[4 * f + 2 * layer + kind], osem.at[kind, layer, f])
            cp.start()
            copies.append(cp)
    for c in copies:
        c.wait()


def emit(norm, rate, clip, gu, gd, weights, states, nd):
    nt = gu.shape[0] // 2
    up, down = states[0].shape, states[1].shape
    V, D, S = pltpu.VMEM, pltpu.SemaphoreType.DMA, jax.ShapeDtypeStruct
    anyspec, vm, sm = [pl.BlockSpec(memory_space=m) for m in (pl.ANY, pltpu.VMEM, pltpu.SMEM)]
    return pl.pallas_call(
        functools.partial(kernel_emit, (nd, nt)),
        out_shape=[S(a.shape, a.dtype) for a in (*weights, *states)] + [S((1, 1), F32)],
        in_specs=[vm, sm, sm] + [HBM] * 2 + [anyspec] * 4 + [HBM] * 12, out_specs=[HBM] * 16 + [vm],
        scratch_shapes=[V((PAIR, nt) + gu.shape[1:], F32), V((PAIR, nt) + gd.shape[1:], F32), V((PAIR, 3) + up, F32), V((PAIR, 3) + down, F32),
                        D((2, 2, 4)), D((4, EMIT)), D((2, 2, 3))],
        compiler_params=pltpu.CompilerParams(vmem_limit_bytes=EMIT_VMEM), name="emit")(norm, rate, clip, gu, gd, *weights, *states)


def solution(mesh):
    groups = mesh.shape["data"]
    rows_spec = P("data", None)
    full_spec = P(None, None)
    scalar_spec = P()

    def shard_body(act_in, grad_out, w_up1, w_down1, w_up2, w_down2, *rest):
        states, learn_rate, clip_norm = rest[:12], rest[12], rest[13]
        ff, d = w_down1.shape
        down1_tiles = w_down1.reshape(groups, -1, 16, d)
        down2_tiles = w_down2.reshape(groups, -1, 16, d)
        pre1, mid_t, in_t, grad_t, up2_t = forward_one(act_in, grad_out, w_up1, w_up2, down1_tiles)
        up2_tiles = up2_t.reshape(down1_tiles.shape)
        grads_up, grads_down, sq = backward(mid_t, grad_t, in_t, pre1, up2_tiles, down2_tiles, down1_tiles)
        rate, clip = learn_rate.reshape(1), clip_norm.reshape(1)
        states = [pltpu.with_memory_space_constraint(x, pltpu.HBM) for x in states]
        sq, grads_up, grads_down = [pltpu.with_memory_space_constraint(x, pltpu.HBM) for x in (sq, grads_up, grads_down)]
        up1, up2, down1, down2, norm = update(sq, rate, clip, grads_up, grads_down, states, groups)
        *results, norm = emit(norm, rate, clip, grads_up, grads_down, (up1, down1, up2, down2), states, groups)
        return (*results, norm.reshape(()))

    in_specs = (rows_spec, rows_spec) + (full_spec,) * 4 + (rows_spec,) * 12 + (scalar_spec, scalar_spec)
    out_specs = (full_spec,) * 4 + (rows_spec,) * 12 + (scalar_spec,)
    return jax.shard_map(shard_body, mesh=mesh, in_specs=in_specs, out_specs=out_specs, check_vma=False)
```

```python
import functools
import math
import jax
import jax.numpy as jnp
from jax import lax
from jax.experimental import pallas as pl
from jax.experimental.pallas import tpu as pltpu
from jax.sharding import PartitionSpec as P

ROOT_HALF = math.sqrt(0.5)
INV_ROOT_TAU = 1.0 / math.sqrt(2.0 * math.pi)
F32, BF16 = jnp.float32, jnp.bfloat16
HBM = pl.BlockSpec(memory_space=pltpu.HBM)
VMEM_MAX = 64 * 1024 * 1024 - 65536
PAIR = 2
BLOCKS = 8
TURNS = 8
RING = 4
LANES = 128


def dot_nn(a, b):
    return lax.dot_general(a, b, (((1,), (0,)), ((), ())), preferred_element_type=F32)


def dot_nt(a, b):
    return lax.dot_general(a, b, (((1,), (1,)), ((), ())), preferred_element_type=F32)


def gelu(z):
    return z * (0.5 * (1.0 + lax.erf(z * ROOT_HALF)))


def at_most(j, bound):
    return jnp.minimum(j, bound)


def aligned(j, size):
    return pl.ds(pl.multiple_of(j * size, size), size)


def kernel_a(cfg, x_hbm, e_hbm, w1_hbm, w3_hbm, w2_hbm, z_hbm, ut_hbm, xt_hbm, et_hbm, w3t_hbm,
             xt, uacc, zout, w1t_v, w1_in, x_in, w1, w2, w2t, w3_in, w3_out, e_in, e_out, h0, h1,
             wsem, xsem, esem, vsem, zsem, osem):
    nt, nr, rb, tr, tb, ft, d, nd = cfg
    hb = (h0, h1)
    width = ft // nd

    def w1copy(q):
        slot = lax.rem(q, RING)
        return pltpu.make_async_copy(w1_hbm.at[aligned(q, LANES), :], w1_in.at[slot], wsem.at[slot])

    def xcopy(r):
        slot = lax.rem(r, RING)
        return pltpu.make_async_copy(x_hbm.at[aligned(r, tb), :], x_in.at[slot], xsem.at[slot])

    def w2copy(j):
        slot = lax.rem(j, 2)
        return pltpu.make_async_copy(w2_hbm.at[:, j], w2.at[slot], vsem.at[0, slot])

    def w3copy(j):
        slot = lax.rem(j, 2)
        return pltpu.make_async_copy(w3_hbm.at[:, aligned(j, ft)], w3_in.at[slot], vsem.at[1, slot])

    def w3store(j):
        slot = lax.rem(j, 2)
        return pltpu.make_async_copy(w3_out.at[slot], w3t_hbm.at[aligned(j, ft), :], osem.at[0, slot])

    def ecopy(r):
        slot = lax.rem(r, 2)
        return pltpu.make_async_copy(e_hbm.at[aligned(r, tb), :], e_in.at[slot], esem.at[slot])

    def estore(r):
        slot = lax.rem(r, 2)
        return pltpu.make_async_copy(e_out.at[slot], et_hbm.at[:, aligned(r, tb)], osem.at[1, slot])

    def zstore(j):
        slot = lax.rem(j, 2)
        return pltpu.make_async_copy(zout.at[slot], z_hbm.at[j], zsem.at[slot])

    rows_in = d // LANES
    for q in range(min(RING, rows_in)):
        w1copy(q).start()
    for r in range(min(RING, tr)):
        xcopy(r).start()
    for c in (w2copy(0), w3copy(0), ecopy(0)):
        c.start()

    def zero(r, _):
        uacc[:, aligned(r, rb)] = jnp.zeros((d, rb), F32)
        return 0
    lax.fori_loop(0, nr, zero, 0)

    def turn_in(q, _):
        @pl.when(q < rows_in)
        def _():
            w1copy(q).wait()
            w1t_v[:, aligned(q, LANES)] = w1_in[lax.rem(q, RING)].T
        @pl.when(q + RING < rows_in)
        def _():
            w1copy(q + RING).start()
        xcopy(q).wait()
        xt[:, aligned(q, tb)] = x_in[lax.rem(q, RING)].T
        @pl.when(q + RING < tr)
        def _():
            xcopy(q + RING).start()
        return 0
    lax.fori_loop(0, tr, turn_in, 0)
    xt_store = pltpu.make_async_copy(xt, xt_hbm, osem.at[2, 0])
    xt_store.start()

    def pick_w1(j, slot):
        for k in range(nd):
            w1[slot, k * width:(k + 1) * width, :] = w1t_v[aligned(k * nt + j, width), :]
    pick_w1(0, 0)

    def tile(j, _):
        slot = lax.rem(j, 2)
        nslot = 1 - slot
        @pl.when(j >= 2)
        def _():
            zstore(j - 2).wait()
            w3store(j - 2).wait()
        @pl.when(jnp.logical_and(j >= 2, j < tr + 2))
        def _():
            estore(j - 2).wait()
        w2copy(j).wait()
        w3copy(j).wait()
        @pl.when(j < tr)
        def _():
            ecopy(j).wait()
        @pl.when(j + 1 < nt)
        def _():
            w2copy(j + 1).start()
            w3copy(j + 1).start()
        @pl.when(j + 1 < min(tr, nt))
        def _():
            ecopy(j + 1).start()

        def cols(r):
            return pl.ds(r * rb, rb)
        def front(r):
            zout[slot, :, cols(r)] = dot_nn(w1[slot], xt[:, cols(r)])
        def middle(r):
            hb[r % 2][...] = gelu(zout[slot, :, cols(r)]).astype(BF16)
        def back(r):
            uacc[:, cols(r)] += dot_nn(w2t[...], hb[r % 2][...])
        front(0)
        w2t[...] = w2[slot].reshape(ft, d).T
        for r in range(nr):
            middle(r)
            if r + 1 < nr:
                front(r + 1)
            if r >= 1:
                back(r - 1)
            if r == 0:
                pick_w1(at_most(j + 1, nt - 1), nslot)
            if r == 1:
                w3_out[slot] = w3_in[slot].T
            if r == nr - 2:
                e_out[slot] = e_in[slot].T
        back(nr - 1)
        zstore(j).start()
        w3store(j).start()
        @pl.when(j < tr)
        def _():
            estore(j).start()
        return 0
    lax.fori_loop(0, nt, tile, 0)
    xt_store.wait()

    def finish(r, _):
        block = aligned(r, rb)
        xt[:, block] = uacc[:, block].astype(BF16)
        pltpu.make_async_copy(xt.at[:, block], ut_hbm.at[:, block], osem.at[2, 1]).start()
        return 0
    lax.fori_loop(0, nr, finish, 0)
    ut_store = pltpu.make_async_copy(xt, ut_hbm, osem.at[2, 1])
    for j in (nt - 2, nt - 1):
        zstore(j).wait()
        w3store(j).wait()
        if j < tr:
            estore(j).wait()
    for r in range(nt, tr):
        ecopy(r).start()
        ecopy(r).wait()
        e_out[r % 2] = e_in[r % 2].T
        estore(r).start()
        estore(r).wait()
    ut_store.wait()


def forward_one(x, e, w1, w3, w2r):
    t, d = x.shape
    nd, nt, rows2, _ = w2r.shape
    ft, nr, tr = nd * rows2, BLOCKS, TURNS
    rb, tb = t // nr, t // tr
    V, D = pltpu.VMEM, pltpu.SemaphoreType.DMA
    S = jax.ShapeDtypeStruct
    return pl.pallas_call(
        functools.partial(kernel_a, (nt, nr, rb, tr, tb, ft, d, nd)),
        out_shape=(S((nt, ft, t), F32), S((d, t), BF16), S((d, t), BF16), S((d, t), BF16), S((nt * ft, d), BF16)),
        in_specs=[HBM] * 5, out_specs=(HBM,) * 5,
        scratch_shapes=[
            V((d, t), BF16), V((d, t), F32), V((PAIR, ft, t), F32), V((nt * ft, d), BF16), V((RING, LANES, nt * ft), BF16), V((RING, tb, d), BF16),
            V((PAIR, ft, d), BF16), V((PAIR, nd, rows2, d), BF16), V((d, ft), BF16), V((PAIR, d, ft), BF16), V((PAIR, ft, d), BF16),
            V((PAIR, tb, d), BF16), V((PAIR, d, tb), BF16), V((ft, rb), BF16), V((ft, rb), BF16),
            D((RING,)), D((RING,)), D((PAIR,)), D((PAIR, PAIR)), D((PAIR,)), D((3, 2))],
        compiler_params=pltpu.CompilerParams(vmem_limit_bytes=VMEM_MAX),
        name="forward_one",
    )(x, e, w1, w3, w2r)


MESH = pl.DeviceIdType.MESH

def gelu_pair(pre):
    normal_cdf = 0.5 * (1.0 + lax.erf(pre * ROOT_HALF))
    density = jnp.exp(-0.5 * pre * pre) * INV_ROOT_TAU
    return pre * normal_cdf, normal_cdf + pre * density

def flip(value, step):
    return value + step * (1 - 2 * lax.rem(lax.div(value, step), 2))

def position():
    me = lax.axis_index("data")
    chip = lax.div(me, 2)
    steps = [(1 << k) * (1 - 2 * lax.rem(lax.div(chip, 1 << k), 2)) for k in range(AXES)]
    return me, lax.rem(me, 2), chip, steps


def hop(steps, kind, place, j):
    axis = lax.rem(j + ORDERS[kind][place], AXES)
    return steps[0] * lax.div((2 - axis) * (1 - axis), 2) + steps[1] * axis * (2 - axis) + steps[2] * lax.div(axis * (axis - 1), 2)


def relative(hops, p):
    return sum((hops[place] for place in range(AXES) if (p >> (AXES - 1 - place)) & 1), 0)


AXES = 3


def when(condition, fn):
    pl.when(condition)(fn)


def meet(peers):
    barrier = pltpu.get_barrier_semaphore()
    for peer in peers:
        pl.semaphore_signal(barrier, inc=1, device_id=(peer,), device_id_type=MESH)
    pl.semaphore_wait(barrier, len(peers))


ORDERS = ((0, 2, 1), (1, 2, 0))
PARTS = 8
BACK_BLOCKS = 4
BEGUN = 2
TURN = 128
SEEN = (3, 6, 9, 12)
DEPTH = (2, 6, 6, 6)
LAST = len(SEEN) - 1
HOLD = 3

def kernel_bc(cfg, ut_hbm, et_hbm, xt_hbm, z_hbm, w3_hbm, w4_hbm, w2_hbm,
              gu_hbm, gd_hbm, nrm_ref,
              act, side, euacc, wa, wb, wat, zb0, zb1, eb0, eb1, hb0, hb1, qb0, qb1,
              gu, gt, gd, r0u, r0d, a0u, a0d, a1u, a1d, a2u, a2d, r1u, r1d, r2u, r2d, r3u, r3d, fu, fd, nu, nd_acc,
              insem, wsem, zsem, ssem, rsem, fsem):
    nt, nr, nc, t, ft, d, nd = cfg
    rb, rc = t // nr, t // nc
    total = 2 * nt
    me, core, chip, steps = position()
    partner = flip(me, 1)
    zb, eb, hb, qb = (zb0, zb1), (eb0, eb1), (hb0, hb1), (qb0, qb1)
    G, R, ACC, FIN, NRM, OUT = (gu, gd), ((r0u, r1u, r2u, r3u), (r0d, r1d, r2d, r3d)), ((a0u, a1u, a2u), (a0d, a1d, a2d)), (fu, fd), (nu, nd_acc), (gu_hbm, gd_hbm)

    loads = [pltpu.make_async_copy(ut_hbm, act, insem.at[0]), pltpu.make_async_copy(et_hbm, side, insem.at[1])]
    for c in loads:
        c.start()

    def wcopies(j, slot, back):
        second = w2_hbm if back else w4_hbm
        cps = [pltpu.make_async_copy(second.at[:, j], wb.at[slot], wsem.at[slot])]
        if not back:
            cps.append(pltpu.make_async_copy(w3_hbm.at[:, j], wa.at[slot], wsem.at[slot]))
        return cps
    for c in wcopies(0, 0, False):
        c.start()

    meet([partner] + [me + 2 * s for s in steps])

    nu[...] = jnp.zeros_like(nu)
    nd_acc[...] = jnp.zeros_like(nd_acc)
    gt[1] = jnp.zeros_like(gt[1])
    def zero(r, _):
        euacc[:, aligned(r, rb)] = jnp.zeros((d, rb), F32)
        return 0
    lax.fori_loop(0, nr, zero, 0)

    def flag_of(stage, j):
        return stage * max(DEPTH) + lax.rem(j, DEPTH[stage])

    both = (gu.at[0], r0u.at[0], r1u.at[0], r2u.at[0])

    def join(stage, j):
        sem = flag_of(stage, j)
        pltpu.make_async_remote_copy(src_ref=both[stage], dst_ref=both[stage], send_sem=ssem.at[sem], recv_sem=rsem.at[sem],
                                     device_id=(me,), device_id_type=MESH).wait()

    def send(kind, stage, j):
        depth = R[kind][stage].shape[0]
        slot = lax.rem(j, depth)
        sem = flag_of(stage, j)
        dst = R[kind][stage].at[slot]
        if stage == 0:
            src, dev = G[kind].at[lax.rem(j, G[kind].shape[0]), :, 1 - core], partner
        else:
            lo = PARTS >> stage
            src, dev = ACC[kind][stage - 1].at[lax.rem(j, HOLD), pl.ds(lo, lo)], me + 2 * hop(steps, kind, stage - 1, j)
        return pltpu.make_async_remote_copy(src_ref=src, dst_ref=dst, send_sem=ssem.at[sem], recv_sem=rsem.at[sem],
                                            device_id=(dev,), device_id_type=MESH)

    def final_copy(kind, j):
        slot = lax.rem(j, 2)
        return pltpu.make_async_copy(FIN[kind].at[slot], OUT[kind].at[j], fsem.at[kind, slot])

    def absorb(stage, j):
        place = lax.rem(j, HOLD)
        join(stage, j)
        for kind in range(2):
            slot = lax.rem(j, R[kind][stage].shape[0])
            got, acc = R[kind][stage], ACC[kind]
            if stage == 0:
                hops = [hop(steps, kind, place, j) for place in range(AXES)]
                for p in range(PARTS):
                    oc = chip + relative(hops, p)
                    acc[0][place, p] = G[kind][lax.rem(j, G[kind].shape[0]), oc, core] + got[slot, oc]
                continue
            kept = acc[stage - 1][place, 0:PARTS >> stage] + got[slot]
            if stage < LAST:
                acc[stage][place] = kept
            else:
                when(j >= 2, final_copy(kind, j - 2).wait)
                f = kept[0] * (1.0 / nd)
                FIN[kind][lax.rem(j, 2)] = f
                NRM[kind][...] += f * f
        for kind in range(2):
            (send(kind, stage + 1, j) if stage < LAST else final_copy(kind, j)).start()

    def comm(step):
        def due(j, fn):
            when(jnp.logical_and(j >= 0, j < total), fn)
        for stage in reversed(range(len(SEEN))):
            j = step - SEEN[stage]
            due(j, functools.partial(absorb, stage, j))
        def start():
            for kind in range(2):
                send(kind, 0, step - BEGUN).start()
        due(step - BEGUN, start)

    def turn(step, part):
        slot = lax.rem(step + 1, 2)
        lanes = pl.ds(part * TURN, TURN)
        gd[slot, :, :, :, lanes] = gt[slot, lanes, :].T.reshape(gd.shape[1:-1] + (TURN,))

    def add_up(step, r, value):
        slot, value = lax.rem(step, gu.shape[0]), value.reshape(gu.shape[1:])
        gu[slot] = value if r == 0 else gu[slot] + value

    def add_down(step, r, value):
        slot = lax.rem(step, 2)
        gt[slot] = value if r == 0 else gt[slot] + value

    def gates(r, width, pre):
        h, der = gelu_pair(pre)
        lanes = pl.ds(0, width)
        hb[r % 2][:, lanes] = h.astype(BF16)
        qb[r % 2][:, lanes] = (eb[r % 2][:, lanes].astype(F32) * der).astype(BF16)

    def pipeline(step, blocks, front, middle, back):
        front(0)
        for r in range(blocks):
            middle(r)
            if r + 1 < blocks:
                front(r + 1)
            if r >= 1:
                back(r - 1)
            for part in range(r, d // TURN, blocks):
                turn(step, part)
        back(blocks - 1)

    for c in loads:
        c.wait()

    def tile_b(j, _):
        slot = lax.rem(j, 2)
        comm(j)
        pltpu.make_async_copy(wa, wa, wsem.at[slot]).wait()
        @pl.when(j + 1 < nt)
        def _():
            for c in wcopies(j + 1, 1 - slot, False):
                c.start()
        def cols(r):
            return pl.ds(r * rb, rb)
        mine = pl.ds(0, rb)
        def front(r):
            zb[r % 2][...] = dot_nn(wa[slot].reshape(ft, d), act[:, cols(r)])
            eb[r % 2][:, mine] = dot_nn(wb[slot].reshape(ft, d), side[:, cols(r)]).astype(BF16)
            if r == 0:
                wat[...] = wa[slot].reshape(ft, d).T
        def middle(r):
            gates(r, rb, zb[r % 2][...])
        def back(r):
            q = qb[r % 2][:, mine]
            add_up(j, r, dot_nt(act[:, cols(r)], q))
            add_down(j, r, dot_nt(side[:, cols(r)], hb[r % 2][:, mine]))
            euacc[:, cols(r)] += dot_nn(wat[...], q)
        pipeline(j, nr, front, middle, back)
        return 0
    lax.fori_loop(0, nt, tile_b, 0)

    xt_in = pltpu.make_async_copy(xt_hbm, side, insem.at[1])
    xt_in.start()
    for c in wcopies(0, nt % 2, True):
        c.start()
    def zcopy(j, slot):
        return pltpu.make_async_copy(z_hbm.at[j], euacc.at[aligned(slot, ft), :], zsem.at[slot])
    def cast(q, _):
        rows = aligned(lax.rem(q + ft // TURN, d // TURN), TURN)
        act[rows, :] = euacc[rows, :].astype(BF16)
        return 0
    lax.fori_loop(0, ft // TURN, cast, 0)
    zcopy(0, nt % 2).start()
    lax.fori_loop(ft // TURN, d // TURN, cast, 0)
    xt_in.wait()

    def tile_c(step, _):
        j = step - nt
        slot = lax.rem(step, 2)
        comm(step)
        for c in wcopies(j, slot, True):
            c.wait()
        zcopy(j, slot).wait()
        @pl.when(j + 1 < nt)
        def _():
            for c in wcopies(j + 1, 1 - slot, True):
                c.start()
            zcopy(j + 1, 1 - slot).start()
        def cols(r):
            return pl.ds(r * rc, rc)
        mine = pl.ds(0, rc)
        def front(r):
            eb[r % 2][:, mine] = dot_nn(wb[slot].reshape(ft, d), act[:, cols(r)]).astype(BF16)
        def middle(r):
            gates(r, rc, euacc[aligned(slot, ft), cols(r)])
        def back(r):
            add_down(step, r, dot_nt(act[:, cols(r)], hb[r % 2][:, mine]))
            add_up(step, r, dot_nt(side[:, cols(r)], qb[r % 2][:, mine]))
        pipeline(step, nc, front, middle, back)
        return 0
    lax.fori_loop(nt, total, tile_c, 0)

    def drain(step, _):
        comm(step)
        @pl.when(step == total)
        def _():
            for part in range(d // TURN):
                turn(step, part)
        return 0
    lax.fori_loop(total, total + SEEN[LAST], drain, 0)
    for kind in range(2):
        for j in (total - 2, total - 1):
            final_copy(kind, j).wait()

    part = jnp.zeros((8, 128), F32)
    for ref in (nu, nd_acc):
        rows, cols = ref.shape
        for a in range(rows // 8):
            for b in range(cols // 128):
                part = part + ref[8 * a:8 * a + 8, 128 * b:128 * b + 128]
    nrm_ref[...] = part


def backward(ut, et, xt, z, w3r, w4r, w2r):
    d, t = ut.shape
    nd, nt, rows2, _ = w4r.shape
    ft, nr, nc = nd * rows2, BACK_BLOCKS, BACK_BLOCKS // 2
    rb, rc = t // nr, t // nc
    bu, bd = (d // nd, ft), (rows2, d)
    V, D = pltpu.VMEM, pltpu.SemaphoreType.DMA
    S = jax.ShapeDtypeStruct
    scratch = [V((d, t), BF16)] * 2 + [V((d, t), F32)] + [V((PAIR, nd, rows2, d), BF16)] * 2 + [V((d, ft), BF16)]
    scratch += [V((ft, rb), F32)] * 2 + [V((ft, rc), BF16)] * 6
    scratch += [V((3, PARTS, 2) + bu, F32), V((PAIR, d, ft), F32), V((PAIR, PARTS, 2) + bd, F32)]
    for n, c in [(DEPTH[0], PARTS)] + [(HOLD, PARTS >> k) for k in range(LAST)] + [(DEPTH[k], PARTS >> k) for k in range(1, LAST + 1)]:
        scratch += [V((n, c) + bu, F32), V((n, c) + bd, F32)]
    scratch += [V((PAIR,) + bu, F32), V((PAIR,) + bd, F32), V(bu, F32), V(bd, F32)]
    flags = len(SEEN) * max(DEPTH)
    scratch += [D((PAIR,)), D((PAIR,)), D((PAIR,)), D((flags,)), D((flags,)), D((PAIR, PAIR))]
    return pl.pallas_call(
        functools.partial(kernel_bc, (nt, nr, nc, t, ft, d, nd)),
        out_shape=(S((2 * nt,) + bu, F32), S((2 * nt,) + bd, F32), S((8, 128), F32)),
        in_specs=[HBM] * 7, out_specs=(HBM, HBM, pl.BlockSpec(memory_space=pltpu.VMEM)),
        scratch_shapes=scratch,
        compiler_params=pltpu.CompilerParams(collective_id=0, has_side_effects=True, vmem_limit_bytes=VMEM_MAX),
        name="backward",
    )(ut, et, xt, z, w3r, w4r, w2r)


STEP = 20
BETA_ONE = 0.9
BETA_TWO = 0.95
EPSILON = 1e-8
NORM_EPS = 1e-6
CORR_ONE = 1.0 - BETA_ONE ** STEP
CORR_TWO = 1.0 - BETA_TWO ** STEP
WIDTH = 16
LAG = 4
AHEAD = 2
EMIT = 4
UPDATE_VMEM = 19 * 1024 * 1024 + 256 * 1024
EMIT_VMEM = 17 * 1024 * 1024


def clip_scale(norm, clip):
    return jnp.minimum(1.0, clip / (norm + NORM_EPS))


def adam_rows(scale, rate, grad, master, mom, vel):
    scaled = scale * grad
    mom = BETA_ONE * mom + (1.0 - BETA_ONE) * scaled
    vel = BETA_TWO * vel + (1.0 - BETA_TWO) * scaled * scaled
    master = master - rate * (mom * (1.0 / CORR_ONE)) / (jnp.sqrt(vel * (1.0 / CORR_TWO)) + EPSILON)
    return master, mom, vel


def natural_columns(gbuf, layer, first, count, nd, nt):
    rows, per = gbuf.shape[2], LANES // WIDTH
    group = lax.broadcasted_iota(jnp.int32, (rows, LANES), 1) // WIDTH
    tiles = []
    for t in range(count):
        acc = None
        for s in range(per):
            place = per * (first + t) + s
            owner, j = lax.div(place, nt), lax.rem(place, nt)
            src = gbuf[layer, j, :, aligned(lax.div(owner, per), LANES)]
            turned = pltpu.roll(src, lax.rem(s - lax.rem(owner, per) + per, per) * WIDTH, 1)
            acc = turned if acc is None else jnp.where(group == s, turned, acc)
        tiles.append(acc)
    return jnp.concatenate(tiles, axis=1)


def state_loads(gu_hbm, gd_hbm, states, gbuf, sbuf, sem, lo, hi):
    loads = []
    for kind, src in enumerate((gu_hbm, gd_hbm)):
        nt, size = src.shape[0] // 2, src.shape[2] if kind == 0 else src.shape[1]
        part = pl.ds(lo * size, (hi - lo) * size)
        for layer in range(2):
            first, count = (lo, hi - lo) if kind else (0, nt if lo == 0 else 0)
            if count:
                loads.append(pltpu.make_async_copy(src.at[pl.ds((1 - layer) * nt + first, count)], gbuf[kind].at[layer, pl.ds(first, count)],
                                                   sem.at[kind, layer, 3]))
            for f in range(3):
                whole, mine = states[4 * f + 2 * layer + kind], sbuf[kind].at[layer, f]
                pair = (whole.at[:, part], mine.at[:, part]) if kind == 0 else (whole.at[part, :], mine.at[part, :])
                loads.append(pltpu.make_async_copy(*pair, sem.at[kind, layer, f]))
    return loads


def kernel_update(cfg, part_hbm, rate_ref, clip_ref, gu_hbm, gd_hbm, *refs):
    nd, pieces, ru, cu, rd = cfg
    states, (ou1, ou2, od1, od2, norm_ref), (su, sd, gbuf_u, gbuf_d, sbuf_u, sbuf_d, nrecv, insem, nsem, lsem, rsem, ssem, dsem) = refs[:12], refs[12:17], refs[17:]
    me, core, chip, steps = position()
    partner = flip(me, 1)
    IN, O = (su, sd), ((ou1, ou2), (od1, od2))
    layers = range(len(O[0]))
    loads = [state_loads(gu_hbm, gd_hbm, states, (gbuf_u, gbuf_d), (sbuf_u, sbuf_d), insem.at[n], *span)
             for n, span in enumerate(((0, AHEAD), (AHEAD, pieces)))]
    keep = pltpu.make_async_copy(part_hbm, nrecv.at[me], nsem.at[2])
    for c in (keep, *loads[0], *loads[1]):
        c.start()
    meet([lax.rem(me + k, nd) for k in range(1, nd)])
    for k in range(1, nd):
        pltpu.make_async_remote_copy(src_ref=part_hbm, dst_ref=nrecv.at[me], send_sem=nsem.at[0], recv_sem=nsem.at[1],
                                     device_id=(lax.rem(me + k, nd),), device_id_type=MESH).start()

    def block(kind, first, j, ref):
        if kind == 0:
            return ref.at[pl.ds(pl.multiple_of(first, 8), ru), aligned(j, cu)]
        return ref.at[pl.ds(pl.multiple_of(first + j * rd, 8), rd), :]

    height = (ru, rd * pieces)
    own = [pltpu.make_async_copy(IN[kind].at[w], O[kind][w].at[aligned(me, height[kind]), :], lsem.at[kind, w])
           for kind in range(2) for w in layers]

    def push(kind, p, j, hops, dev, send, recv):
        first = (2 * (chip + relative(hops, p)) + core) * height[kind]
        for w in layers:
            dst = block(kind, first, j, O[kind][w])
            src = dst if p else block(kind, 0, j, IN[kind].at[w])
            pltpu.make_async_remote_copy(src_ref=src, dst_ref=dst, send_sem=send, recv_sem=recv, device_id=(dev,), device_id_type=MESH).start()

    def flag(kind, stage, j):
        return rsem.at[kind, stage, lax.rem(j, AXES * LAG)]

    def spread(kind, stage, j, hops):
        dev = me + 2 * hops[AXES - 1 - stage]
        for p in range(1 << stage):
            push(kind, p, j, hops, dev, ssem.at[kind, stage], flag(kind, stage, j))

    def await_bytes(ref, sem, recv):
        cp = pltpu.make_async_remote_copy(src_ref=ref, dst_ref=ref, send_sem=sem, recv_sem=sem, device_id=(me,), device_id_type=MESH)
        if recv:
            cp.wait_recv()
        else:
            cp.wait_send()

    def arrived(kind, stage, j):
        n = 2 << stage
        part = O[kind][0].at[pl.ds(0, n * ru), pl.ds(0, cu)] if kind == 0 else O[kind][0].at[pl.ds(0, n * rd), :]
        await_bytes(part, flag(kind, stage, j), True)

    keep.wait()
    others = nrecv.at[pl.ds(0, nd - 1)]
    await_bytes(others, nsem.at[0], False)
    await_bytes(others, nsem.at[1], True)
    total_sq = nrecv[0]
    for k in range(1, nd):
        total_sq = total_sq + nrecv[k]
    norm = jnp.sqrt(jnp.sum(total_sq, keepdims=True))
    norm_ref[...] = jnp.broadcast_to(norm, norm_ref.shape)
    rate, scale = rate_ref[0], clip_scale(norm, clip_ref[0])

    def make(j):
        for w in layers:
            cols = aligned(j, cu)
            grad = natural_columns(gbuf_u, w, j * (cu // LANES), cu // LANES, nd, pieces)
            old = [sbuf_u[w, f, :, cols] for f in range(3)]
            su[w, :, cols] = adam_rows(scale, rate, grad, *old)[0].astype(BF16)
            rows = aligned(j, rd)
            old = [sbuf_d[w, f, rows, :] for f in range(3)]
            sd[w, rows, :] = adam_rows(scale, rate, gbuf_d[w, j], *old)[0].astype(BF16)

    def step(s, _):
        for stage in reversed(range(AXES + 1)):
            j = s - stage * LAG
            @pl.when(jnp.logical_and(j >= 0, j < pieces))
            def _():
                for kind in range(2):
                    hops = [hop(steps, kind, place, j) for place in range(AXES)]
                    if stage:
                        arrived(kind, stage - 1, j)
                    if stage < AXES:
                        spread(kind, stage, j, hops)
                    for p in range((1 << stage) >> 1, 1 << stage):
                        push(kind, p, j, hops, partner, dsem.at[0, kind], dsem.at[1, kind])
        @pl.when(s + AHEAD < pieces)
        def _():
            make(s + AHEAD)
        return 0
    for c in loads[0]:
        c.wait()
    for j in range(AHEAD):
        make(j)
    for c in loads[1]:
        c.wait()
    lax.fori_loop(0, pieces + AXES * LAG, step, 0)
    for c in own:
        c.start()
    for c in own:
        c.wait()
    for kind in range(2):
        full = O[kind][0]
        await_bytes(full, dsem.at[0, kind], False)
        await_bytes(full, dsem.at[1, kind], True)
        for stage in range(AXES):
            await_bytes(full.at[pl.ds(0, (2 << stage) * height[kind]), :], ssem.at[kind, stage], False)


def update(part, rate, clip, gu, gd, states, nd):
    (ru, f), (rf, d) = states[0].shape, states[1].shape
    pieces = gd.shape[0] // 2
    V, D, S = pltpu.VMEM, pltpu.SemaphoreType.DMA, jax.ShapeDtypeStruct
    anyspec, vm, sm = [pl.BlockSpec(memory_space=m) for m in (pl.ANY, pltpu.VMEM, pltpu.SMEM)]
    return pl.pallas_call(
        functools.partial(kernel_update, (nd, pieces, ru, f // pieces, rf // pieces)),
        out_shape=(S((ru * nd, f), BF16),) * 2 + (S((rf * nd, d), BF16),) * 2 + (S((8, LANES), F32),),
        in_specs=[HBM, sm, sm] + [HBM] * 14, out_specs=(anyspec,) * 4 + (vm,),
        scratch_shapes=[V((PAIR, ru, f), BF16), V((PAIR, rf, d), BF16), V((PAIR, pieces) + gu.shape[1:], F32), V((PAIR, pieces) + gd.shape[1:], F32),
                        V((PAIR, 3, ru, f), F32), V((PAIR, 3, rf, d), F32), V((nd, 8, LANES), F32),
                        D((2, 2, 2, 4)), D((3,)), D((PAIR, PAIR)), D((2, AXES, AXES * LAG)), D((2, AXES)), D((PAIR, PAIR))],
        compiler_params=pltpu.CompilerParams(collective_id=1, has_side_effects=True, vmem_limit_bytes=UPDATE_VMEM),
        name="update")(part, rate, clip, gu, gd, *states)


def kernel_emit(cfg, norm_ref, rate_ref, clip_ref, gu_hbm, gd_hbm, *refs):
    nd, nt = cfg
    weights, states, refs = refs[:4], refs[4:16], refs[16:]
    weights_out, states_out, norm_out = refs[:4], refs[4:16], refs[16]
    gbuf_u, gbuf_d, sbuf_u, sbuf_d, insem, wsem, osem = refs[17:]
    gbuf, sbuf = (gbuf_u, gbuf_d), (sbuf_u, sbuf_d)
    loads = state_loads(gu_hbm, gd_hbm, states, gbuf, sbuf, insem, 0, nt)
    for c in loads:
        c.start()
    copies = []
    for k, (src, dst) in enumerate(zip(weights, weights_out)):
        rows = src.shape[0] // EMIT
        for part in range(EMIT):
            piece = pl.ds(part * rows, rows)
            copies.append(pltpu.make_async_copy(src.at[piece, :], dst.at[piece, :], wsem.at[k, part]))
    for c in copies:
        c.start()
    norm = norm_ref[0:1, 0:1]
    norm_out[...] = norm
    rate, scale = rate_ref[0], clip_scale(norm, clip_ref[0])
    for n, c in enumerate(loads):
        c.wait()
        kind, layer = n // 8, n // 4 % 2
        if n % 4 < 3:
            continue
        def renew(rows, cols, grad):
            old = [sbuf[kind][layer, f, rows, cols] for f in range(3)]
            for f, value in enumerate(adam_rows(scale, rate, grad, *old)):
                sbuf[kind][layer, f, rows, cols] = value
        def body(j, _):
            if kind == 0:
                wide = sbuf_u.shape[3] // nt
                renew(slice(None), aligned(j, wide), natural_columns(gbuf_u, layer, j * (wide // LANES), wide // LANES, nd, nt))
            else:
                renew(aligned(j, gbuf_d.shape[2]), slice(None), gbuf_d[layer, j])
            return 0
        lax.fori_loop(0, nt, body, 0)
        for f in range(3):
            cp = pltpu.make_async_copy(sbuf[kind].at[layer, f], states_out[4 * f + 2 * layer + kind], osem.at[kind, layer, f])
            cp.start()
            copies.append(cp)
    for c in copies:
        c.wait()


def emit(norm, rate, clip, gu, gd, weights, states, nd):
    nt = gu.shape[0] // 2
    up, down = states[0].shape, states[1].shape
    V, D, S = pltpu.VMEM, pltpu.SemaphoreType.DMA, jax.ShapeDtypeStruct
    anyspec, vm, sm = [pl.BlockSpec(memory_space=m) for m in (pl.ANY, pltpu.VMEM, pltpu.SMEM)]
    return pl.pallas_call(
        functools.partial(kernel_emit, (nd, nt)),
        out_shape=[S(a.shape, a.dtype) for a in (*weights, *states)] + [S((1, 1), F32)],
        in_specs=[vm, sm, sm] + [HBM] * 2 + [anyspec] * 4 + [HBM] * 12, out_specs=[HBM] * 16 + [vm],
        scratch_shapes=[V((PAIR, nt) + gu.shape[1:], F32), V((PAIR, nt) + gd.shape[1:], F32), V((PAIR, 3) + up, F32), V((PAIR, 3) + down, F32),
                        D((2, 2, 4)), D((4, EMIT)), D((2, 2, 3))],
        compiler_params=pltpu.CompilerParams(vmem_limit_bytes=EMIT_VMEM), name="emit")(norm, rate, clip, gu, gd, *weights, *states)


def solution(mesh):
    groups = mesh.shape["data"]
    rows_spec = P("data", None)
    full_spec = P(None, None)
    scalar_spec = P()

    def shard_body(act_in, grad_out, w_up1, w_down1, w_up2, w_down2, *rest):
        states, learn_rate, clip_norm = rest[:12], rest[12], rest[13]
        ff, d = w_down1.shape
        down1_tiles = w_down1.reshape(groups, -1, 16, d)
        down2_tiles = w_down2.reshape(groups, -1, 16, d)
        pre1, mid_t, in_t, grad_t, up2_t = forward_one(act_in, grad_out, w_up1, w_up2, down1_tiles)
        up2_tiles = up2_t.reshape(down1_tiles.shape)
        grads_up, grads_down, sq = backward(mid_t, grad_t, in_t, pre1, up2_tiles, down2_tiles, down1_tiles)
        rate, clip = learn_rate.reshape(1), clip_norm.reshape(1)
        states = [pltpu.with_memory_space_constraint(x, pltpu.HBM) for x in states]
        sq, grads_up, grads_down = [pltpu.with_memory_space_constraint(x, pltpu.HBM) for x in (sq, grads_up, grads_down)]
        up1, up2, down1, down2, norm = update(sq, rate, clip, grads_up, grads_down, states, groups)
        *results, norm = emit(norm, rate, clip, grads_up, grads_down, (up1, down1, up2, down2), states, groups)
        return (*results, norm.reshape(()))

    in_specs = (rows_spec, rows_spec) + (full_spec,) * 4 + (rows_spec,) * 12 + (scalar_spec, scalar_spec)
    out_specs = (full_spec,) * 4 + (rows_spec,) * 12 + (scalar_spec,)
    return jax.shard_map(shard_body, mesh=mesh, in_specs=in_specs, out_specs=out_specs, check_vma=False)
```
